32 devices in a mesh: tm: 16 (over z, y, core), space: 2 (over x).
Axes of the slice: x: 2, y: 2, z: 4, core: 2. Of those that a mesh axis runs over, the one named last changes fastest.
Arguments:
- iterate: float32 [16, 4, 128, 64, 128], P('tm', None, 'space'), may hold values from -6 to 6
- right_side: float32 [16, 4, 128, 64, 128], P('tm', None, 'space'), may hold values from -6 to 6
- diffusivity: float32 [128, 64, 128], P('space'), may hold values from 0.5 to 2
- velocity: float32 [3], replicated, may hold values from -2 to 2
Outputs:
- next_iterate: float32 [16, 4, 128, 64, 128], P('tm', None, 'space')
The draws below stay inside these ranges and needn't reach their ends.
All inputs are finite; a program needn't handle non-finite values.
Results may differ from the reference program's by a relative error of at most 0.0003.
Values sent between devices are 32-bit elements; how exact they have to be, the bound alone decides.
No kernel may reach another device: no remote copies, remote signals or barrier semaphores. Data moves between devices by JAX's collectives and lax.ppermute only.
A program may use at most 192 MiB of HBM per device.

```python
import math
import jax
import jax.numpy as jnp
from jax import lax

NX = 128
NY = 128
NZ = 64
NODES = 4
STEPS = 16


def draw_right_side(key, part):
    rough_key = jax.random.fold_in(jax.random.fold_in(key, 17), 0)
    rough = jax.random.truncated_normal(rough_key, -6.0, 6.0, (STEPS, NODES, NX, NZ, NY), jnp.float32)
    return rough


def block_levels(key, extent, pieces, least, largest):
    def one(axis_at, shards_of):
        steps = jax.random.uniform(jax.random.fold_in(jax.random.fold_in(key, 6), axis_at), (shards_of,), jnp.float32, least / len(pieces), largest / len(pieces))
        return jnp.repeat(jnp.exp(steps), extent[axis_at] // shards_of).reshape((-1,) + (1,) * (len(extent) - axis_at - 1))

    factor_of = one(*pieces[0])
    for cut in pieces[1:]:
        factor_of = factor_of * one(*cut)
    return factor_of


def centred(own_key, shape, spread, limit, pieces=(), kind=jnp.bfloat16):
    level = block_levels(own_key, shape, pieces, -0.22, 0.18) if pieces else 1.0
    values = jax.random.normal(own_key, shape, jnp.float32) * spread * level
    return jnp.minimum(jnp.maximum(values, -limit), limit).astype(kind)


def setup_inputs(seed: int = 0) -> dict:
    streams_of = jax.random.split(jax.random.key(seed), 5)
    return {
        "iterate": centred(streams_of[0], (STEPS, NODES, NX, NZ, NY), 1.0, 6.0, ((0, 16), (2, 2)), jnp.float32),
        "right_side": draw_right_side(jax.random.fold_in(streams_of[4], 71), 0),
        "diffusivity": jnp.clip(jnp.exp(math.log(2.0) - 1.3862944 * jax.random.uniform(streams_of[2], (NX, NZ, NY), jnp.float32) ** block_levels(streams_of[2], (NX, NZ, NY), ((0, 2),), -0.2, 0.2)), 0.5, 2.0),
        "velocity": jnp.clip(jax.random.uniform(streams_of[3], (3,), jnp.float32, -2.0, 2.0), -2.0, 2.0),
    }


diffusion_number = 16.0
circulant_alpha = 0.1


def collocation_matrix():
    radau_nodes = [0.088587959512703947, 0.40946686444073471, 0.78765946176084706, 1.0]
    matrix = [[0.0] * 4 for row_index in range(4)]
    for column_index in range(4):
        coefficients = [1.0]
        for other_index in range(4):
            if other_index != column_index:
                scale_value = 1.0 / (radau_nodes[column_index] - radau_nodes[other_index])
                shifted = [0.0] + [value * scale_value for value in coefficients]
                lowered = [-radau_nodes[other_index] * scale_value * value for value in coefficients] + [0.0]
                coefficients = [left_value + right_value for left_value, right_value in zip(shifted, lowered)]
        for row_index in range(4):
            total = 0.0
            for power_index in range(len(coefficients)):
                total = total + coefficients[power_index] * radau_nodes[row_index] ** (power_index + 1) / (power_index + 1)
            matrix[row_index][column_index] = total
    return matrix


def solve_system(matrix, target):
    count = len(target)
    rows_list = [list(matrix[row_index]) + [target[row_index]] for row_index in range(count)]
    for column in range(count):
        best_row = column
        for candidate in range(column + 1, count):
            if abs(rows_list[candidate][column]) > abs(rows_list[best_row][column]):
                best_row = candidate
        saved_row = rows_list[column]
        rows_list[column] = rows_list[best_row]
        rows_list[best_row] = saved_row
        leader = rows_list[column][column]
        for other_row in range(count):
            if other_row != column:
                factor = rows_list[other_row][column] / leader
                rows_list[other_row] = [left_value - factor * right_value for left_value, right_value in zip(rows_list[other_row], rows_list[column])]
    return [rows_list[row_index][count] / rows_list[row_index][row_index] for row_index in range(count)]


def node_basis():
    matrix = collocation_matrix()
    helper = [[0.0] * 4 for row_index in range(4)]
    coefficients = [0.0, 0.0, 0.0, 0.0, 1.0]
    for order in range(1, 5):
        product = [[sum(matrix[row_index][inner] * helper[inner][column] for inner in range(4)) for column in range(4)] for row_index in range(4)]
        for row_index in range(4):
            product[row_index][row_index] = product[row_index][row_index] + coefficients[5 - order]
        helper = product
        trace_value = sum(sum(matrix[row_index][inner] * helper[inner][row_index] for inner in range(4)) for row_index in range(4))
        coefficients[4 - order] = -trace_value / order
    roots_list = [(0.4 + 0.9j) ** power_index for power_index in range(4)]
    for sweep in range(400):
        for root_index in range(4):
            current = roots_list[root_index]
            numer = 0.0
            for power_index in range(4, -1, -1):
                numer = numer * current + coefficients[power_index]
            denom = 1.0
            for other_index in range(4):
                if other_index != root_index:
                    denom = denom * (current - roots_list[other_index])
            roots_list[root_index] = current - numer / denom
    vectors = [[0.0] * 4 for row_index in range(4)]
    for root_index in range(4):
        shifted = [[matrix[row_index][column] - (roots_list[root_index] if row_index == column else 0.0) for column in range(3)] for row_index in range(3)]
        target = [-matrix[row_index][3] for row_index in range(3)]
        parts = solve_system(shifted, target) + [1.0 + 0.0j]
        for row_index in range(4):
            vectors[row_index][root_index] = parts[row_index]
    inverse = [[0.0] * 4 for row_index in range(4)]
    for column in range(4):
        unit = [1.0 if row_index == column else 0.0 for row_index in range(4)]
        parts = solve_system(vectors, unit)
        for row_index in range(4):
            inverse[row_index][column] = parts[row_index]
    weights = [sum(inverse[row_index][column] for column in range(4)) for row_index in range(4)]
    return roots_list, vectors, inverse, weights


def complex_vector(numbers):
    real_values = jnp.asarray([complex(value).real for value in numbers], jnp.float32)
    imag_values = jnp.asarray([complex(value).imag for value in numbers], jnp.float32)
    return real_values + 1j * imag_values


def complex_matrix(numbers):
    real_values = jnp.asarray([[complex(value).real for value in row] for row in numbers], jnp.float32)
    imag_values = jnp.asarray([[complex(value).imag for value in row] for row in numbers], jnp.float32)
    return real_values + 1j * imag_values


def spatial_operator(field_values, diffusivity, velocity):
    upper_x = jnp.roll(field_values, -1, axis=2)
    lower_x = jnp.roll(field_values, 1, axis=2)
    upper_z = jnp.roll(field_values, -1, axis=3)
    lower_z = jnp.roll(field_values, 1, axis=3)
    upper_y = jnp.roll(field_values, -1, axis=4)
    lower_y = jnp.roll(field_values, 1, axis=4)
    laplace = (upper_x + lower_x) + (upper_z + lower_z) + (upper_y + lower_y) - 6.0 * field_values
    transport = velocity[0] * (upper_x - lower_x) + velocity[1] * (upper_y - lower_y) + velocity[2] * (upper_z - lower_z)
    return diffusion_number * diffusivity * laplace - 0.5 * transport


def reference(iterate, right_side, diffusivity, velocity):
    collocation = jnp.asarray(collocation_matrix(), jnp.float32)
    applied = spatial_operator(iterate, diffusivity, velocity)
    coupled = jnp.einsum("mn,snxzy->smxzy", collocation, applied, precision=lax.Precision.HIGHEST)
    previous = jnp.concatenate([jnp.zeros_like(iterate[:1, 3]), iterate[:-1, 3]], axis=0)
    residual = right_side - iterate + coupled + previous[:, None]
    gamma_base = circulant_alpha ** (1.0 / STEPS)
    step_power = jnp.arange(STEPS, dtype=jnp.int32).astype(jnp.float32)
    step_scale = jnp.power(jnp.float32(gamma_base), step_power)
    spectrum = jnp.fft.rfftn(residual * step_scale[:, None, None, None, None], axes=(0, 2, 3, 4))
    theta_x = jnp.arange(NX, dtype=jnp.int32).astype(jnp.float32) * (2.0 * math.pi / NX)
    theta_z = jnp.arange(NZ, dtype=jnp.int32).astype(jnp.float32) * (2.0 * math.pi / NZ)
    theta_y = jnp.arange(NY // 2 + 1, dtype=jnp.int32).astype(jnp.float32) * (2.0 * math.pi / NY)
    symbol_real = diffusion_number * ((2.0 * jnp.cos(theta_x)[:, None, None] - 2.0) + (2.0 * jnp.cos(theta_z)[None, :, None] - 2.0) + (2.0 * jnp.cos(theta_y)[None, None, :] - 2.0))
    symbol_imag = -(velocity[0] * jnp.sin(theta_x)[:, None, None] + velocity[1] * jnp.sin(theta_y)[None, None, :] + velocity[2] * jnp.sin(theta_z)[None, :, None])
    symbol = symbol_real + 1j * symbol_imag
    values, vectors, inverse, weights = node_basis()
    eigen = complex_vector(values)
    basis = complex_matrix(vectors)
    basis_inverse = complex_matrix(inverse)
    ones_weights = complex_vector(weights)
    damping = 1.0 / (1.0 - eigen[:, None, None, None] * symbol[None])
    ones_image = jnp.einsum("pm,mxzy->pxzy", basis, ones_weights[:, None, None, None] * damping, precision=lax.Precision.HIGHEST)
    phases = jnp.arange(STEPS, dtype=jnp.int32).astype(jnp.float32) * (2.0 * math.pi / STEPS)
    shift_factors = gamma_base * (jnp.cos(phases) - 1j * jnp.sin(phases))

    def solve_one(operands):
        block, shift_factor = operands
        inner = jnp.einsum("mn,nxzy->mxzy", basis_inverse, block, precision=lax.Precision.HIGHEST) * damping
        image = jnp.einsum("pm,mxzy->pxzy", basis, inner, precision=lax.Precision.HIGHEST)
        factor = shift_factor * image[3] / (1.0 - shift_factor * ones_image[3])
        return image + ones_image * factor[None]

    solved = lax.map(solve_one, (spectrum, shift_factors))
    correction = jnp.fft.irfftn(solved, s=(STEPS, NX, NZ, NY), axes=(0, 2, 3, 4))
    unscale = jnp.power(jnp.float32(gamma_base), -step_power)
    return iterate + correction * unscale[:, None, None, None, None]
```

```python
import functools
import math

import jax
import jax.numpy as jnp
import numpy as np
from jax import lax
from jax.experimental import pallas as pl
from jax.experimental.pallas import tpu as pltpu
from jax.sharding import PartitionSpec as P

diffusion_number = 16.0
circulant_alpha = 0.1
NODES = 4
BLOCK = 8


def collocation_matrix():
    radau_nodes = [0.08858795951270394, 0.4094668644407347, 0.7876594617608471, 1.0]
    matrix = [[0.0] * 4 for row_index in range(4)]
    for column_index in range(4):
        coefficients = [1.0]
        for other_index in range(4):
            if other_index != column_index:
                scale_value = 1.0 / (radau_nodes[column_index] - radau_nodes[other_index])
                shifted = [0.0] + [value * scale_value for value in coefficients]
                lowered = [
                    -radau_nodes[other_index] * scale_value * value for value in coefficients
                ] + [0.0]
                coefficients = [
                    left_value + right_value for left_value, right_value in zip(shifted, lowered)
                ]
        for row_index in range(4):
            total = 0.0
            for power_index in range(len(coefficients)):
                total = total + coefficients[power_index] * radau_nodes[row_index] ** (
                    power_index + 1
                ) / (power_index + 1)
            matrix[row_index][column_index] = total
    return matrix


def solve_system(matrix, target):
    count = len(target)
    rows_list = [list(matrix[row_index]) + [target[row_index]] for row_index in range(count)]
    for column in range(count):
        best_row = column
        for candidate in range(column + 1, count):
            if abs(rows_list[candidate][column]) > abs(rows_list[best_row][column]):
                best_row = candidate
        saved_row = rows_list[column]
        rows_list[column] = rows_list[best_row]
        rows_list[best_row] = saved_row
        leader = rows_list[column][column]
        for other_row in range(count):
            if other_row != column:
                factor = rows_list[other_row][column] / leader
                rows_list[other_row] = [
                    left_value - factor * right_value
                    for left_value, right_value in zip(rows_list[other_row], rows_list[column])
                ]
    return [
        rows_list[row_index][count] / rows_list[row_index][row_index] for row_index in range(count)
    ]


def node_basis():
    matrix = collocation_matrix()
    helper = [[0.0] * 4 for row_index in range(4)]
    coefficients = [0.0, 0.0, 0.0, 0.0, 1.0]
    for order in range(1, 5):
        product = [
            [
                sum((matrix[row_index][inner] * helper[inner][column] for inner in range(4)))
                for column in range(4)
            ]
            for row_index in range(4)
        ]
        for row_index in range(4):
            product[row_index][row_index] = product[row_index][row_index] + coefficients[5 - order]
        helper = product
        trace_value = sum(
            (
                sum((matrix[row_index][inner] * helper[inner][row_index] for inner in range(4)))
                for row_index in range(4)
            )
        )
        coefficients[4 - order] = -trace_value / order
    roots_list = [(0.4 + 0.9j) ** power_index for power_index in range(4)]
    for sweep in range(400):
        for root_index in range(4):
            current = roots_list[root_index]
            numer = 0.0
            for power_index in range(4, -1, -1):
                numer = numer * current + coefficients[power_index]
            denom = 1.0
            for other_index in range(4):
                if other_index != root_index:
                    denom = denom * (current - roots_list[other_index])
            roots_list[root_index] = current - numer / denom
    vectors = [[0.0] * 4 for row_index in range(4)]
    for root_index in range(4):
        shifted = [
            [
                matrix[row_index][column] - (roots_list[root_index] if row_index == column else 0.0)
                for column in range(3)
            ]
            for row_index in range(3)
        ]
        target = [-matrix[row_index][3] for row_index in range(3)]
        parts = solve_system(shifted, target) + [1.0 + 0j]
        for row_index in range(4):
            vectors[row_index][root_index] = parts[row_index]
    inverse = [[0.0] * 4 for row_index in range(4)]
    for column in range(4):
        unit = [1.0 if row_index == column else 0.0 for row_index in range(4)]
        parts = solve_system(vectors, unit)
        for row_index in range(4):
            inverse[row_index][column] = parts[row_index]
    weights = [sum((inverse[row_index][column] for column in range(4))) for row_index in range(4)]
    return (roots_list, vectors, inverse, weights)


def split_table(table):
    table = jnp.asarray(np.asarray(table, np.float32))
    high = table.astype(jnp.bfloat16)
    return high, (table - high.astype(jnp.float32)).astype(jnp.bfloat16)


def split(values):
    high = values.astype(jnp.bfloat16)
    return high, (values - high.astype(jnp.float32)).astype(jnp.bfloat16)


def dot(left, right):
    return jnp.dot(left, right, preferred_element_type=jnp.float32)


def dot3_table_left(table_high, table_low, values):
    high, low = split(values)
    return dot(table_high, high) + (dot(table_high, low) + dot(table_low, high))


def dot3_table_right(values, table_high, table_low):
    high, low = split(values)
    return dot(high, table_high) + (dot(low, table_high) + dot(high, table_low))


def node_constants():
    values, vectors, inverse, weights = node_basis()
    return (
        np.array([complex(v) for v in values]),
        np.array([[complex(v) for v in row] for row in vectors]),
        np.array([[complex(v) for v in row] for row in inverse]),
        np.array([complex(v) for v in weights]),
    )


def half_rows(nz):
    kept = nz // 2 + 1
    return kept, -(-kept // 8) * 8


def forward_tables(nz, ny):
    _, _, inverse, _ = node_constants()
    kept, padded = half_rows(nz)
    wave = np.zeros((padded, nz), complex)
    wave[:kept] = np.exp(-2j * math.pi * np.outer(np.arange(kept), np.arange(nz)) / nz)
    mixed = np.zeros((NODES, 2, padded, NODES, nz))
    for m in range(NODES):
        for n in range(NODES):
            mixed[m, 0, :, n] = (inverse[m, n] * wave).real
            mixed[m, 1, :, n] = (inverse[m, n] * wave).imag
    plain = np.concatenate([wave.real, wave.imag], axis=0)
    angle = 2 * math.pi * (np.outer(np.arange(ny), np.arange(ny)) % ny) / ny
    c, s = np.cos(angle), np.sin(angle)
    along_y = np.block([[c, -s], [s, c]])
    return mixed.reshape(NODES * 2 * padded, NODES * nz), plain, along_y


def inverse_tables(nz, ny):
    _, vectors, _, _ = node_constants()
    kept, padded = half_rows(nz)
    weight = np.where((np.arange(kept) == 0) | (2 * np.arange(kept) == nz), 1.0, 2.0)
    wave = np.zeros((nz, padded), complex)
    wave[:, :kept] = np.exp(2j * math.pi * np.outer(np.arange(nz), np.arange(kept)) / nz) * weight / nz
    mixed = np.zeros((NODES, nz, NODES, 2, padded))
    for n in range(NODES):
        for m in range(NODES):
            mixed[n, :, m, 0] = (vectors[n, m] * wave).real
            mixed[n, :, m, 1] = -(vectors[n, m] * wave).imag
    angle = 2 * math.pi * (np.outer(np.arange(ny), np.arange(ny)) % ny) / ny
    c, s = np.cos(angle) / ny, np.sin(angle) / ny
    along_y = np.block([[c, s], [-s, c]])
    return mixed.reshape(NODES * nz, NODES * 2 * padded), along_y


def x_tables(nx):
    angle = 2 * math.pi * (np.outer(np.arange(nx), np.arange(nx)) % nx) / nx
    c, s = np.cos(angle), np.sin(angle)
    return np.concatenate([c, -s], axis=0), np.block([[c, -s], [s, c]]) / nx


def c_mul(a, b):
    return a[0] * b[0] - a[1] * b[1], a[0] * b[1] + a[1] * b[0]


def c_div(a, b):
    size = b[0] * b[0] + b[1] * b[1]
    return (a[0] * b[0] + a[1] * b[1]) / size, (a[1] * b[0] - a[0] * b[1]) / size


def c_power(a, count):
    result = None
    while count:
        if count & 1:
            result = a if result is None else c_mul(result, a)
        count >>= 1
        if count:
            a = c_mul(a, a)
    return result


def c_sqrt(a):
    size = jnp.sqrt(a[0] * a[0] + a[1] * a[1])
    large = jnp.sqrt(0.5 * (size + jnp.abs(a[0])))
    small = a[1] / (2.0 * large)
    flip = a[0] < 0.0
    return (
        jnp.where(flip, jnp.abs(small), large),
        jnp.where(flip, jnp.where(a[1] < 0.0, -large, large), small),
    )


def line_tables(velocity, nz, ny):
    values, _, _, weights = node_constants()
    _, padded = half_rows(nz)
    theta_z = jnp.arange(padded, dtype=jnp.int32).astype(jnp.float32) * (2.0 * math.pi / nz)
    theta_y = jnp.arange(ny, dtype=jnp.int32).astype(jnp.float32) * (2.0 * math.pi / ny)
    real = diffusion_number * (
        (2.0 * jnp.cos(theta_z)[:, None] - 2.0) + (2.0 * jnp.cos(theta_y)[None, :] - 2.0)
    )
    imag = -(velocity[1] * jnp.sin(theta_y)[None, :] + velocity[2] * jnp.sin(theta_z)[:, None])
    real, imag = real[None], imag[None]
    mu = (
        jnp.asarray(values.real, jnp.float32)[:, None, None],
        jnp.asarray(values.imag, jnp.float32)[:, None, None],
    )
    part = c_mul(mu, (real - 2.0 * diffusion_number, imag))
    diagonal = (1.0 - part[0], -part[1])
    from_low = diffusion_number + 0.5 * velocity[0]
    from_high = diffusion_number - 0.5 * velocity[0]
    mu2 = c_mul(mu, mu)
    square = c_mul(diagonal, diagonal)
    product = 4.0 * from_low * from_high
    root = c_sqrt((square[0] - product * mu2[0], square[1] - product * mu2[1]))
    turn = diagonal[0] * root[0] + diagonal[1] * root[1] < 0.0
    root = (jnp.where(turn, -root[0], root[0]), jnp.where(turn, -root[1], root[1]))
    kappa = (0.5 * (diagonal[0] + root[0]), 0.5 * (diagonal[1] + root[1]))
    ratio = c_div(mu, kappa)
    one = jnp.ones_like(root[0])
    gain = c_div((one, jnp.zeros_like(one)), root)
    beta = c_mul(
        gain,
        (
            jnp.asarray(weights.real, jnp.float32)[:, None, None],
            jnp.asarray(weights.imag, jnp.float32)[:, None, None],
        ),
    )
    low = (from_low * ratio[0], from_low * ratio[1])
    high = (from_high * ratio[0], from_high * ratio[1])
    return (
        jnp.stack(low, axis=1),
        jnp.stack(high, axis=1),
        jnp.stack(gain, axis=1),
        jnp.stack(beta, axis=1),
    )


def forward_kernel(
    block_ref,
    prev_ref,
    next_ref,
    halo_low_ref,
    halo_high_ref,
    right_ref,
    diffusivity_ref,
    zh_ref,
    zl_ref,
    ph_ref,
    pl_ref,
    yh_ref,
    yl_ref,
    low_ref,
    high_ref,
    gain_ref,
    out_ref,
    plain_ref,
    ends_ref,
    planes,
    power,
    *,
    padded,
):
    step = pl.program_id(0)
    steps = pl.num_programs(0)
    nz, ny = block_ref.shape[3], block_ref.shape[4]
    matrix = collocation_matrix()

    @pl.when(step == 0)
    def _():
        ends_ref[...] = jnp.zeros_like(ends_ref)
        planes[0] = halo_low_ref[0, :, 0]
        for m in range(NODES):
            power[m, 0] = jnp.ones_like(power[m, 0])
            power[m, 1] = jnp.zeros_like(power[m, 1])

    @pl.when(step > 0)
    def _():
        planes[0] = prev_ref[0, :, 0]

    @pl.when(step == steps - 1)
    def _():
        planes[BLOCK + 1] = halo_high_ref[0, :, 0]

    @pl.when(step < steps - 1)
    def _():
        planes[BLOCK + 1] = next_ref[0, :, 0]

    for j in range(BLOCK):
        planes[j + 1] = block_ref[0, :, j]

    def pair(index, carry):
        columns = []
        plains = []
        for half in range(2):
            j = 2 * index + half
            factor = diffusion_number * (diffusivity_ref[j] - 1.0)
            spread = []
            for n in range(NODES):
                f = planes[j + 1, n]
                lap = (
                    (planes[j, n] + planes[j + 2, n])
                    + (pltpu.roll(f, 1, 0) + pltpu.roll(f, nz - 1, 0))
                    + (pltpu.roll(f, 1, 1) + pltpu.roll(f, ny - 1, 1))
                    - 6.0 * f
                )
                spread.append(factor * lap)
            mixed = []
            for m in range(NODES):
                total = right_ref[0, m, j]
                for n in range(NODES):
                    total = total + matrix[m][n] * spread[n]
                mixed.append(total)
            columns.append(jnp.concatenate(mixed, axis=0))
            plains.append(planes[j + 1, NODES - 1])
        spectrum_z = dot3_table_left(zh_ref[...], zl_ref[...], jnp.concatenate(columns, axis=1))
        plain_z = dot3_table_left(ph_ref[...], pl_ref[...], jnp.concatenate(plains, axis=1))
        rows = []
        for half in range(2):
            lanes = slice(half * ny, (half + 1) * ny)
            for m in range(NODES):
                base = 2 * m * padded
                rows.append(
                    jnp.concatenate(
                        [
                            spectrum_z[base : base + padded, lanes],
                            spectrum_z[base + padded : base + 2 * padded, lanes],
                        ],
                        axis=1,
                    )
                )
            rows.append(
                jnp.concatenate([plain_z[:padded, lanes], plain_z[padded:, lanes]], axis=1)
            )
        spectrum = dot3_table_right(jnp.concatenate(rows, axis=0), yh_ref[...], yl_ref[...])
        for half in range(2):
            j = 2 * index + half
            for m in range(NODES):
                base = (half * (NODES + 1) + m) * padded
                value = (spectrum[base : base + padded, :ny], spectrum[base : base + padded, ny:])
                value = c_mul(value, (gain_ref[m, 0], gain_ref[m, 1]))
                out_ref[j, m, 0] = value[0]
                out_ref[j, m, 1] = value[1]
                moved = c_mul((ends_ref[0, m, 0], ends_ref[0, m, 1]), (low_ref[m, 0], low_ref[m, 1]))
                ends_ref[0, m, 0] = moved[0] + value[0]
                ends_ref[0, m, 1] = moved[1] + value[1]
                scale = (power[m, 0], power[m, 1])
                added = c_mul(scale, value)
                ends_ref[1, m, 0] = ends_ref[1, m, 0] + added[0]
                ends_ref[1, m, 1] = ends_ref[1, m, 1] + added[1]
                scale = c_mul(scale, (high_ref[m, 0], high_ref[m, 1]))
                power[m, 0] = scale[0]
                power[m, 1] = scale[1]
            base = (half * (NODES + 1) + NODES) * padded
            plain_ref[j, 0] = spectrum[base : base + padded, :ny]
            plain_ref[j, 1] = spectrum[base : base + padded, ny:]
        return carry

    lax.fori_loop(0, BLOCK // 2, pair, 0)


def full(shape):
    zeros = (0,) * len(shape)
    return pl.BlockSpec(shape, lambda *_: zeros)


def forward_stage(iterate, right_side, diffusivity, halos, lines):
    _, _, count, nz, ny = iterate.shape
    _, padded = half_rows(nz)
    blocks = count // BLOCK
    mixed, plain, along_y = forward_tables(nz, ny)
    tables = [*split_table(mixed), *split_table(plain), *split_table(along_y), *lines[:3]]
    plane = (1, NODES, 1, nz, ny)
    return pl.pallas_call(
        functools.partial(forward_kernel, padded=padded),
        grid=(blocks,),
        in_specs=[
            pl.BlockSpec((1, NODES, BLOCK, nz, ny), lambda b: (0, 0, b, 0, 0)),
            pl.BlockSpec(plane, lambda b: (0, 0, jnp.maximum(b * BLOCK - 1, 0), 0, 0)),
            pl.BlockSpec(plane, lambda b: (0, 0, jnp.minimum((b + 1) * BLOCK, count - 1), 0, 0)),
            full(plane),
            full(plane),
            pl.BlockSpec((1, NODES, BLOCK, nz, ny), lambda b: (0, 0, b, 0, 0)),
            pl.BlockSpec((BLOCK, nz, ny), lambda b: (b, 0, 0)),
            *[full(t.shape) for t in tables],
        ],
        out_specs=[
            pl.BlockSpec((BLOCK, NODES, 2, padded, ny), lambda b: (b, 0, 0, 0, 0)),
            pl.BlockSpec((BLOCK, 2, padded, ny), lambda b: (b, 0, 0, 0)),
            full((2, NODES, 2, padded, ny)),
        ],
        out_shape=[
            jax.ShapeDtypeStruct((count, NODES, 2, padded, ny), jnp.float32),
            jax.ShapeDtypeStruct((count, 2, padded, ny), jnp.float32),
            jax.ShapeDtypeStruct((2, NODES, 2, padded, ny), jnp.float32),
        ],
        scratch_shapes=[
            pltpu.VMEM((BLOCK + 2, NODES, nz, ny), jnp.float32),
            pltpu.VMEM((NODES, 2, padded, ny), jnp.float32),
        ],
        compiler_params=pltpu.CompilerParams(
            dimension_semantics=("arbitrary",), vmem_limit_bytes=60 * 1024 * 1024
        ),
    )(iterate, iterate, iterate, *halos, right_side, diffusivity, *tables)


def node_kernel(c_ref, plain_ref, states_ref, low_ref, high_ref, out_ref, partial, state, *, half):
    phase = pl.program_id(0)
    step = pl.program_id(1)
    blocks = pl.num_programs(1)
    padded, ny = c_ref.shape[3], c_ref.shape[4]
    _, vectors, _, _ = node_constants()
    last = [complex(v) for v in vectors[NODES - 1]]

    @pl.when((phase == 0) & (step == 0))
    def _():
        state[...] = states_ref[0]

    @pl.when((phase == 1) & (step == 0))
    def _():
        state[...] = states_ref[1]

    @pl.when(phase == 0)
    def _():
        def plane(j, carry):
            total = None
            for m in range(NODES):
                moved = c_mul((state[m, 0], state[m, 1]), (low_ref[m, 0], low_ref[m, 1]))
                moved = (moved[0] + c_ref[j, m, 0], moved[1] + c_ref[j, m, 1])
                state[m, 0] = moved[0]
                state[m, 1] = moved[1]
                added = (
                    last[m].real * moved[0] - last[m].imag * moved[1],
                    last[m].real * moved[1] + last[m].imag * moved[0],
                )
                total = added if total is None else (total[0] + added[0], total[1] + added[1])
            partial[step * BLOCK + j, 0] = total[0]
            partial[step * BLOCK + j, 1] = total[1]
            return carry

        lax.fori_loop(0, BLOCK, plane, 0)

    @pl.when(phase == 1)
    def _():
        lane = lax.broadcasted_iota(jnp.int32, (1, ny), 1)

        def plane(i, carry):
            j = BLOCK - 1 - i
            row = (blocks - 1 - step) * BLOCK + j
            total = (partial[row, 0] - plain_ref[j, 0], partial[row, 1] - plain_ref[j, 1])
            for m in range(NODES):
                moved = c_mul((state[m, 0], state[m, 1]), (high_ref[m, 0], high_ref[m, 1]))
                total = (
                    total[0] + (last[m].real * moved[0] - last[m].imag * moved[1]),
                    total[1] + (last[m].real * moved[1] + last[m].imag * moved[0]),
                )
                state[m, 0] = moved[0] + c_ref[j, m, 0]
                state[m, 1] = moved[1] + c_ref[j, m, 1]
            folded = []
            for part in range(2):
                value = total[part]
                turned = pltpu.roll(value[half : half + 8], ny // 2, 1)[:1]
                first = jnp.where(lane <= ny // 2, value[:1], turned)
                if part == 1:
                    first = jnp.where(lane % (ny // 2) == 0, total[0][half : half + 1], first)
                folded.append(first)
            for part in range(2):
                out_ref[j, part] = total[part][:half]
                out_ref[j, part, 0:1] = folded[part]
            return carry

        lax.fori_loop(0, BLOCK, plane, 0)


def node_stage(c, plain, states, lines, nz):
    count, _, _, padded, ny = c.shape
    blocks = count // BLOCK
    half = nz // 2

    def both(phase, b):
        return jnp.where(phase == 0, b, blocks - 1 - b)

    def late(phase, b):
        return jnp.where(phase == 0, blocks - 1, blocks - 1 - b)

    return pl.pallas_call(
        functools.partial(node_kernel, half=half),
        grid=(2, blocks),
        in_specs=[
            pl.BlockSpec((BLOCK, NODES, 2, padded, ny), lambda a, b: (both(a, b), 0, 0, 0, 0)),
            pl.BlockSpec((BLOCK, 2, padded, ny), lambda a, b: (late(a, b), 0, 0, 0)),
            full(states.shape),
            full(lines[0].shape),
            full(lines[1].shape),
        ],
        out_specs=pl.BlockSpec((BLOCK, 2, half, ny), lambda a, b: (late(a, b), 0, 0, 0)),
        out_shape=jax.ShapeDtypeStruct((count, 2, half, ny), jnp.float32),
        scratch_shapes=[
            pltpu.VMEM((count, 2, padded, ny), jnp.float32),
            pltpu.VMEM((NODES, 2, padded, ny), jnp.float32),
        ],
        compiler_params=pltpu.CompilerParams(
            dimension_semantics=("arbitrary", "arbitrary"), vmem_limit_bytes=60 * 1024 * 1024
        ),
    )(c, plain, states, lines[0], lines[1])


def couple_kernel(q_ref, th_ref, tl_ref, ih_ref, il_ref, grow_ref, close_ref, out_ref, work):
    steps, slabs, _, count, width = q_ref.shape
    nx = slabs * count

    def ahead(s, carry):
        for part in range(2):
            line = jnp.concatenate([q_ref[s, p, part] for p in range(slabs)], axis=0)
            waves = dot3_table_left(th_ref[...], tl_ref[...], line)
            work[s, part, 0] = waves[:nx]
            work[s, part, 1] = waves[nx:]
        return carry

    lax.fori_loop(0, steps, ahead, 0)
    for part in range(2):
        grow = (grow_ref[part, 0], grow_ref[part, 1])

        def gather(s, carry):
            moved = c_mul(grow, carry)
            return moved[0] + work[s, part, 0], moved[1] + work[s, part, 1]

        zero = jnp.zeros((nx, width), jnp.float32)
        last = lax.fori_loop(0, steps, gather, (zero, zero))
        first = c_mul(last, (close_ref[part, 0], close_ref[part, 1]))

        def spread(s, carry):
            moved = c_mul(grow, carry)
            following = (moved[0] + work[s, part, 0], moved[1] + work[s, part, 1])
            work[s, part, 0] = carry[0]
            work[s, part, 1] = carry[1]
            return following

        lax.fori_loop(0, steps, spread, first)

    def back(s, carry):
        joined = jnp.concatenate(
            [work[s, 0, 0] - work[s, 1, 1], work[s, 0, 1] + work[s, 1, 0]], axis=0
        )
        lines = dot3_table_left(ih_ref[...], il_ref[...], joined)
        for part in range(2):
            for p in range(slabs):
                base = part * nx + p * count
                out_ref[s, p, part] = lines[base : base + count]
        return carry

    lax.fori_loop(0, steps, back, 0)


def couple_stage(q, velocity, first_mode, nz, ny):
    steps, slabs, _, count, width = q.shape
    nx = slabs * count
    forward, backward = x_tables(nx)
    values, vectors, _, weights = node_constants()
    mode = first_mode + jnp.arange(width, dtype=jnp.int32)
    row, lane = mode // ny, mode % ny
    edge = row == 0
    corner = edge & (lane % (ny // 2) == 0)
    wave_z = jnp.where(edge & (lane > ny // 2), nz // 2, row)
    wave_y = jnp.where(edge & (lane > ny // 2), lane - ny // 2, lane)
    wave_z = jnp.stack([wave_z, jnp.where(corner, nz // 2, wave_z)])[:, None, :]
    theta_z = wave_z.astype(jnp.float32) * (2.0 * math.pi / nz)
    theta_y = wave_y.astype(jnp.float32)[None, None, :] * (2.0 * math.pi / ny)
    theta_x = jnp.arange(nx, dtype=jnp.int32).astype(jnp.float32)[None, :, None] * (2.0 * math.pi / nx)
    real = diffusion_number * (
        (2.0 * jnp.cos(theta_x) - 2.0)
        + (2.0 * jnp.cos(theta_z) - 2.0)
        + (2.0 * jnp.cos(theta_y) - 2.0)
    )
    imag = -(
        velocity[0] * jnp.sin(theta_x)
        + velocity[1] * jnp.sin(theta_y)
        + velocity[2] * jnp.sin(theta_z)
    )
    grow = None
    for m in range(NODES):
        mu = complex(values[m])
        below = (1.0 - (mu.real * real - mu.imag * imag), -(mu.real * imag + mu.imag * real))
        above = complex(vectors[NODES - 1, m] * weights[m])
        added = c_div((above.real, above.imag), below)
        grow = added if grow is None else (grow[0] + added[0], grow[1] + added[1])
    whole = c_power(grow, steps)
    close = c_div(
        (circulant_alpha, 0.0), (1.0 - circulant_alpha * whole[0], -circulant_alpha * whole[1])
    )
    return pl.pallas_call(
        couple_kernel,
        out_shape=jax.ShapeDtypeStruct(q.shape, jnp.float32),
        scratch_shapes=[pltpu.VMEM((steps, 2, 2, nx, width), jnp.float32)],
        compiler_params=pltpu.CompilerParams(vmem_limit_bytes=60 * 1024 * 1024),
    )(
        q,
        *split_table(forward),
        *split_table(backward),
        jnp.stack(grow, axis=1),
        jnp.stack(close, axis=1),
    )


def unfolded(b_ref, j, part, padded):
    half, ny = b_ref.shape[2], b_ref.shape[3]
    lane = lax.broadcasted_iota(jnp.int32, (8, ny), 1)
    sub = lax.broadcasted_iota(jnp.int32, (8, ny), 0)
    top = b_ref[j, part, 0:8]
    kept = jnp.where(lane % (ny // 2) == 0, 1.0, jnp.where(lane < ny // 2, 2.0, 0.0))
    inside = lane % (ny // 2) != 0
    other = b_ref[j, 1, 0:8]
    turned = pltpu.roll(top, ny // 2, 1)
    if part == 0:
        edge = jnp.where(inside, turned, other)
        first = top
    else:
        edge = jnp.where(inside, turned, 0.0)
        first = jnp.where(inside, top, 0.0)
    head = jnp.where(sub == 0, first * kept, top)
    tail = jnp.where(sub == 0, edge * kept, 0.0)
    pieces = [head, b_ref[j, part, 8:half], tail] if half > 8 else [head, tail]
    return jnp.concatenate(pieces, axis=0)


def edge_kernel(b_ref, low_ref, high_ref, beta_ref, out_ref, *, padded):
    count = b_ref.shape[0]
    out_ref[...] = jnp.zeros_like(out_ref)

    def plane(i, carry):
        for side, j in ((0, i), (1, count - 1 - i)):
            value = [unfolded(b_ref, j, part, padded) for part in range(2)]
            table = low_ref if side == 0 else high_ref
            for m in range(NODES):
                moved = c_mul((out_ref[side, m, 0], out_ref[side, m, 1]), (table[m, 0], table[m, 1]))
                out_ref[side, m, 0] = moved[0] + value[0]
                out_ref[side, m, 1] = moved[1] + value[1]
        return carry

    lax.fori_loop(0, count, plane, 0)
    for side in range(2):
        for m in range(NODES):
            value = c_mul((out_ref[side, m, 0], out_ref[side, m, 1]), (beta_ref[m, 0], beta_ref[m, 1]))
            out_ref[side, m, 0] = value[0]
            out_ref[side, m, 1] = value[1]


def edge_stage(b, lines):
    padded, ny = lines[0].shape[2:]
    return pl.pallas_call(
        functools.partial(edge_kernel, padded=padded),
        out_shape=jax.ShapeDtypeStruct((2, NODES, 2, padded, ny), jnp.float32),
        compiler_params=pltpu.CompilerParams(vmem_limit_bytes=60 * 1024 * 1024),
    )(b, lines[0], lines[1], lines[3])


def inverse_kernel(
    c_ref,
    b_ref,
    states_ref,
    low_ref,
    high_ref,
    beta_ref,
    yh_ref,
    yl_ref,
    zh_ref,
    zl_ref,
    out_ref,
    ahead,
    state,
):
    phase = pl.program_id(0)
    step = pl.program_id(1)
    blocks = pl.num_programs(1)
    padded, ny = c_ref.shape[3], c_ref.shape[4]
    nz = out_ref.shape[3]

    @pl.when((phase == 0) & (step == 0))
    def _():
        state[...] = states_ref[0]

    @pl.when((phase == 1) & (step == 0))
    def _():
        state[...] = states_ref[1]

    def source(j):
        value = [unfolded(b_ref, j, part, padded) for part in range(2)]
        result = []
        for m in range(NODES):
            added = c_mul(value, (beta_ref[m, 0], beta_ref[m, 1]))
            result.append((c_ref[j, m, 0] + added[0], c_ref[j, m, 1] + added[1]))
        return result

    @pl.when(phase == 0)
    def _():
        def plane(j, carry):
            values = source(j)
            for m in range(NODES):
                moved = c_mul((state[m, 0], state[m, 1]), (low_ref[m, 0], low_ref[m, 1]))
                for part in range(2):
                    total = moved[part] + values[m][part]
                    state[m, part] = total
                    ahead[step * BLOCK + j, m, part] = total
            return carry

        lax.fori_loop(0, BLOCK, plane, 0)

    @pl.when(phase == 1)
    def _():
        def pair(i, carry):
            rows = [None] * (2 * NODES)
            for half in range(2):
                j = BLOCK - 1 - (2 * i + half)
                row = (blocks - 1 - step) * BLOCK + j
                values = source(j)
                for m in range(NODES):
                    moved = c_mul((state[m, 0], state[m, 1]), (high_ref[m, 0], high_ref[m, 1]))
                    state[m, 0] = moved[0] + values[m][0]
                    state[m, 1] = moved[1] + values[m][1]
                    rows[half * NODES + m] = jnp.concatenate(
                        [ahead[row, m, 0] + moved[0], ahead[row, m, 1] + moved[1]], axis=1
                    )
            lines = dot3_table_right(jnp.concatenate(rows, axis=0), yh_ref[...], yl_ref[...])
            columns = []
            for half in range(2):
                stacked = []
                for m in range(NODES):
                    base = (half * NODES + m) * padded
                    stacked.append(lines[base : base + padded, :ny])
                    stacked.append(lines[base : base + padded, ny:])
                columns.append(jnp.concatenate(stacked, axis=0))
            grid = dot3_table_left(zh_ref[...], zl_ref[...], jnp.concatenate(columns, axis=1))
            for half in range(2):
                j = BLOCK - 1 - (2 * i + half)
                for n in range(NODES):
                    out_ref[0, n, j] = grid[n * nz : (n + 1) * nz, half * ny : (half + 1) * ny]
            return carry

        lax.fori_loop(0, BLOCK // 2, pair, 0)


def inverse_stage(c, b, states, lines, nz):
    count, _, _, padded, ny = c.shape
    blocks = count // BLOCK
    half = nz // 2
    mixed, along_y = inverse_tables(nz, ny)
    tables = [lines[0], lines[1], lines[3], *split_table(along_y), *split_table(mixed)]

    def both(phase, b):
        return jnp.where(phase == 0, b, blocks - 1 - b)

    def late(phase, b):
        return jnp.where(phase == 0, blocks - 1, blocks - 1 - b)

    return pl.pallas_call(
        inverse_kernel,
        grid=(2, blocks),
        in_specs=[
            pl.BlockSpec((BLOCK, NODES, 2, padded, ny), lambda a, b: (both(a, b), 0, 0, 0, 0)),
            pl.BlockSpec((BLOCK, 2, half, ny), lambda a, b: (both(a, b), 0, 0, 0)),
            full(states.shape),
            *[full(t.shape) for t in tables],
        ],
        out_specs=pl.BlockSpec((1, NODES, BLOCK, nz, ny), lambda a, b: (0, 0, late(a, b), 0, 0)),
        out_shape=jax.ShapeDtypeStruct((1, NODES, count, nz, ny), jnp.float32),
        scratch_shapes=[
            pltpu.VMEM((count, NODES, 2, padded, ny), jnp.float32),
            pltpu.VMEM((NODES, 2, padded, ny), jnp.float32),
        ],
        compiler_params=pltpu.CompilerParams(
            dimension_semantics=("arbitrary", "arbitrary"), vmem_limit_bytes=60 * 1024 * 1024
        ),
    )(c, b, states, *tables)


def ring_states(ends, lines, count, slabs):
    result = []
    for side in range(2):
        decay = c_power((lines[side][:, 0], lines[side][:, 1]), count)
        total = None
        for distance in range(slabs, 0, -1):
            if distance == slabs:
                moved = ends[side]
            else:
                shift = distance if side == 0 else -distance
                moved = lax.ppermute(
                    ends[side], "space", [(i, (i + shift) % slabs) for i in range(slabs)]
                )
            moved = (moved[:, 0], moved[:, 1])
            if total is None:
                total = moved
            else:
                total = c_mul(total, decay)
                total = (total[0] + moved[0], total[1] + moved[1])
        whole = c_power(decay, slabs)
        total = c_div(total, (1.0 - whole[0], -whole[1]))
        result.append(jnp.stack(total, axis=1))
    return jnp.stack(result)


def to_modes(q, devices):
    count, _, half, ny = q.shape
    pieces = devices // half
    q = jnp.transpose(q, (2, 1, 0, 3)).reshape(half, 2, count, pieces, ny // pieces)
    return jnp.transpose(q, (0, 3, 1, 2, 4)).reshape(devices, 2, count, ny // pieces)


def from_modes(b, half):
    devices, _, count, width = b.shape
    pieces = devices // half
    b = jnp.transpose(b.reshape(half, pieces, 2, count, width), (0, 2, 3, 1, 4))
    return jnp.transpose(b.reshape(half, 2, count, pieces * width), (2, 1, 0, 3))


def shards(iterate, right_side, diffusivity, velocity):
    steps, slabs = lax.axis_size("tm"), lax.axis_size("space")
    devices = steps * slabs
    _, _, count, nz, ny = iterate.shape
    up = [(i, (i + 1) % slabs) for i in range(slabs)]
    down = [(target, source) for source, target in up]
    halos = (
        lax.ppermute(iterate[:, :, count - 1 :], "space", up),
        lax.ppermute(iterate[:, :, :1], "space", down),
    )
    lines = line_tables(velocity, nz, ny)
    c, plain, ends = forward_stage(iterate, right_side, diffusivity, halos, lines)
    states = ring_states(ends, lines, count, slabs)
    step = lax.axis_index("tm")
    plain = plain * jnp.where(step == steps - 1, 1.0, 0.0)
    q = node_stage(c, plain, states, lines, nz)
    q = lax.all_to_all(to_modes(q, devices), ("tm", "space"), 0, 0, tiled=True)
    width = q.shape[3]
    first_mode = (step * slabs + lax.axis_index("space")) * width
    b = couple_stage(q.reshape(steps, slabs, 2, count, width), velocity, first_mode, nz, ny)
    b = lax.all_to_all(b.reshape(devices, 2, count, width), ("tm", "space"), 0, 0, tiled=True)
    b = from_modes(b, nz // 2)
    states = states + ring_states(edge_stage(b, lines), lines, count, slabs)
    return inverse_stage(c, b, states, lines, nz)


def solution(mesh):
    placed = (
        P("tm", None, "space", None, None),
        P("tm", None, "space", None, None),
        P("space", None, None),
        P(),
    )
    return jax.shard_map(
        shards,
        mesh=mesh,
        in_specs=placed,
        out_specs=P("tm", None, "space", None, None),
        check_vma=False,
    )
```

```python
import functools
import math

import jax
import jax.numpy as jnp
import numpy as np
from jax import lax
from jax.experimental import pallas as pl
from jax.experimental.pallas import tpu as pltpu
from jax.sharding import PartitionSpec as P

diffusion_number = 16.0
circulant_alpha = 0.1
NODES = 4
GROUP = 8


def collocation_matrix():
    radau_nodes = [0.08858795951270394, 0.4094668644407347, 0.7876594617608471, 1.0]
    matrix = [[0.0] * 4 for row_index in range(4)]
    for column_index in range(4):
        coefficients = [1.0]
        for other_index in range(4):
            if other_index != column_index:
                scale_value = 1.0 / (radau_nodes[column_index] - radau_nodes[other_index])
                shifted = [0.0] + [value * scale_value for value in coefficients]
                lowered = [
                    -radau_nodes[other_index] * scale_value * value for value in coefficients
                ] + [0.0]
                coefficients = [
                    left_value + right_value for left_value, right_value in zip(shifted, lowered)
                ]
        for row_index in range(4):
            total = 0.0
            for power_index in range(len(coefficients)):
                total = total + coefficients[power_index] * radau_nodes[row_index] ** (
                    power_index + 1
                ) / (power_index + 1)
            matrix[row_index][column_index] = total
    return matrix


def solve_system(matrix, target):
    count = len(target)
    rows_list = [list(matrix[row_index]) + [target[row_index]] for row_index in range(count)]
    for column in range(count):
        best_row = column
        for candidate in range(column + 1, count):
            if abs(rows_list[candidate][column]) > abs(rows_list[best_row][column]):
                best_row = candidate
        saved_row = rows_list[column]
        rows_list[column] = rows_list[best_row]
        rows_list[best_row] = saved_row
        leader = rows_list[column][column]
        for other_row in range(count):
            if other_row != column:
                factor = rows_list[other_row][column] / leader
                rows_list[other_row] = [
                    left_value - factor * right_value
                    for left_value, right_value in zip(rows_list[other_row], rows_list[column])
                ]
    return [
        rows_list[row_index][count] / rows_list[row_index][row_index] for row_index in range(count)
    ]


def node_basis():
    matrix = collocation_matrix()
    helper = [[0.0] * 4 for row_index in range(4)]
    coefficients = [0.0, 0.0, 0.0, 0.0, 1.0]
    for order in range(1, 5):
        product = [
            [
                sum((matrix[row_index][inner] * helper[inner][column] for inner in range(4)))
                for column in range(4)
            ]
            for row_index in range(4)
        ]
        for row_index in range(4):
            product[row_index][row_index] = product[row_index][row_index] + coefficients[5 - order]
        helper = product
        trace_value = sum(
            (
                sum((matrix[row_index][inner] * helper[inner][row_index] for inner in range(4)))
                for row_index in range(4)
            )
        )
        coefficients[4 - order] = -trace_value / order
    roots_list = [(0.4 + 0.9j) ** power_index for power_index in range(4)]
    for sweep in range(400):
        for root_index in range(4):
            current = roots_list[root_index]
            numer = 0.0
            for power_index in range(4, -1, -1):
                numer = numer * current + coefficients[power_index]
            denom = 1.0
            for other_index in range(4):
                if other_index != root_index:
                    denom = denom * (current - roots_list[other_index])
            roots_list[root_index] = current - numer / denom
    vectors = [[0.0] * 4 for row_index in range(4)]
    for root_index in range(4):
        shifted = [
            [
                matrix[row_index][column] - (roots_list[root_index] if row_index == column else 0.0)
                for column in range(3)
            ]
            for row_index in range(3)
        ]
        target = [-matrix[row_index][3] for row_index in range(3)]
        parts = solve_system(shifted, target) + [1.0 + 0j]
        for row_index in range(4):
            vectors[row_index][root_index] = parts[row_index]
    inverse = [[0.0] * 4 for row_index in range(4)]
    for column in range(4):
        unit = [1.0 if row_index == column else 0.0 for row_index in range(4)]
        parts = solve_system(vectors, unit)
        for row_index in range(4):
            inverse[row_index][column] = parts[row_index]
    weights = [sum((inverse[row_index][column] for column in range(4))) for row_index in range(4)]
    return (roots_list, vectors, inverse, weights)


def split_table(table):
    table = jnp.asarray(np.asarray(table, np.float32))
    high = table.astype(jnp.bfloat16)
    return high, (table - high.astype(jnp.float32)).astype(jnp.bfloat16)


def split(values):
    high = values.astype(jnp.bfloat16)
    return high, (values - high.astype(jnp.float32)).astype(jnp.bfloat16)


def dot(left, right):
    return jnp.dot(left, right, preferred_element_type=jnp.float32)


def dot3_table_left(table_high, table_low, values):
    high, low = split(values)
    return dot(table_high, high) + (dot(table_high, low) + dot(table_low, high))


def dot3_table_right(values, table_high, table_low):
    high, low = split(values)
    return dot(high, table_high) + (dot(low, table_high) + dot(high, table_low))


def node_constants():
    values, vectors, inverse, weights = node_basis()
    return (
        np.array([complex(v) for v in values]),
        np.array([[complex(v) for v in row] for row in vectors]),
        np.array([[complex(v) for v in row] for row in inverse]),
        np.array([complex(v) for v in weights]),
    )


def half_rows(nz):
    kept = nz // 2 + 1
    return kept, -(-kept // 8) * 8


def forward_tables(nz, ny):
    _, _, inverse, _ = node_constants()
    kept, padded = half_rows(nz)
    wave = np.zeros((padded, nz), complex)
    wave[:kept] = np.exp(-2j * math.pi * np.outer(np.arange(kept), np.arange(nz)) / nz)
    mixed = np.zeros((NODES, 2, padded, NODES, nz))
    for m in range(NODES):
        for n in range(NODES):
            mixed[m, 0, :, n] = (inverse[m, n] * wave).real
            mixed[m, 1, :, n] = (inverse[m, n] * wave).imag
    plain = np.concatenate([wave.real, wave.imag], axis=0)
    angle = 2 * math.pi * (np.outer(np.arange(ny), np.arange(ny)) % ny) / ny
    c, s = np.cos(angle), np.sin(angle)
    along_y = np.block([[c, -s], [s, c]])
    return mixed.reshape(NODES * 2 * padded, NODES * nz), plain, along_y


def inverse_tables(nz, ny):
    _, vectors, _, _ = node_constants()
    kept, padded = half_rows(nz)
    weight = np.where((np.arange(kept) == 0) | (2 * np.arange(kept) == nz), 1.0, 2.0)
    wave = np.zeros((nz, padded), complex)
    wave[:, :kept] = np.exp(2j * math.pi * np.outer(np.arange(nz), np.arange(kept)) / nz) * weight / nz
    mixed = np.zeros((NODES, nz, NODES, 2, padded))
    for n in range(NODES):
        for m in range(NODES):
            mixed[n, :, m, 0] = (vectors[n, m] * wave).real
            mixed[n, :, m, 1] = -(vectors[n, m] * wave).imag
    angle = 2 * math.pi * (np.outer(np.arange(ny), np.arange(ny)) % ny) / ny
    c, s = np.cos(angle) / ny, np.sin(angle) / ny
    along_y = np.block([[c, s], [-s, c]])
    return mixed.reshape(NODES * nz, NODES * 2 * padded), along_y


def x_tables(nx):
    angle = 2 * math.pi * (np.outer(np.arange(nx), np.arange(nx)) % nx) / nx
    c, s = np.cos(angle), np.sin(angle)
    return np.concatenate([c, -s], axis=0), np.block([[c, -s], [s, c]]) / nx


def c_mul(a, b):
    return a[0] * b[0] - a[1] * b[1], a[0] * b[1] + a[1] * b[0]


def c_add(a, b):
    return a[0] + b[0], a[1] + b[1]


def c_div(a, b):
    size = b[0] * b[0] + b[1] * b[1]
    return (a[0] * b[0] + a[1] * b[1]) / size, (a[1] * b[0] - a[0] * b[1]) / size


def c_power(a, count):
    result = None
    while count:
        if count & 1:
            result = a if result is None else c_mul(result, a)
        count >>= 1
        if count:
            a = c_mul(a, a)
    return result


def c_sqrt(a):
    size = jnp.sqrt(a[0] * a[0] + a[1] * a[1])
    large = jnp.sqrt(0.5 * (size + jnp.abs(a[0])))
    small = a[1] / (2.0 * large)
    flip = a[0] < 0.0
    return (
        jnp.where(flip, jnp.abs(small), large),
        jnp.where(flip, jnp.where(a[1] < 0.0, -large, large), small),
    )


def line_tables(velocity, nz, ny):
    values, _, _, weights = node_constants()
    _, padded = half_rows(nz)
    theta_z = jnp.arange(padded, dtype=jnp.int32).astype(jnp.float32) * (2.0 * math.pi / nz)
    theta_y = jnp.arange(ny, dtype=jnp.int32).astype(jnp.float32) * (2.0 * math.pi / ny)
    real = diffusion_number * (
        (2.0 * jnp.cos(theta_z)[:, None] - 2.0) + (2.0 * jnp.cos(theta_y)[None, :] - 2.0)
    )
    imag = -(velocity[1] * jnp.sin(theta_y)[None, :] + velocity[2] * jnp.sin(theta_z)[:, None])
    real, imag = real[None], imag[None]
    mu = (
        jnp.asarray(values.real, jnp.float32)[:, None, None],
        jnp.asarray(values.imag, jnp.float32)[:, None, None],
    )
    part = c_mul(mu, (real - 2.0 * diffusion_number, imag))
    diagonal = (1.0 - part[0], -part[1])
    from_low = diffusion_number + 0.5 * velocity[0]
    from_high = diffusion_number - 0.5 * velocity[0]
    mu2 = c_mul(mu, mu)
    square = c_mul(diagonal, diagonal)
    product = 4.0 * from_low * from_high
    root = c_sqrt((square[0] - product * mu2[0], square[1] - product * mu2[1]))
    turn = diagonal[0] * root[0] + diagonal[1] * root[1] < 0.0
    root = (jnp.where(turn, -root[0], root[0]), jnp.where(turn, -root[1], root[1]))
    kappa = (0.5 * (diagonal[0] + root[0]), 0.5 * (diagonal[1] + root[1]))
    ratio = c_div(mu, kappa)
    one = jnp.ones_like(root[0])
    gain = c_div((one, jnp.zeros_like(one)), kappa)
    close = c_div(kappa, root)
    beta = c_mul(
        gain,
        (
            jnp.asarray(weights.real, jnp.float32)[:, None, None],
            jnp.asarray(weights.imag, jnp.float32)[:, None, None],
        ),
    )
    low = (from_low * ratio[0], from_low * ratio[1])
    high = (from_high * ratio[0], from_high * ratio[1])
    return [jnp.stack(table, axis=1) for table in (low, high, gain, beta, close)]


def block_of(count):
    return 16 if count % 16 == 0 else GROUP


def unrolled(count, body):
    def turn(i, carry):
        body(2 * i, carry)
        return body(2 * i + 1, carry)

    lax.fori_loop(0, count // 2, turn, 0)


def forward_kernel(
    block_ref,
    prev_ref,
    next_ref,
    halo_low_ref,
    halo_high_ref,
    right_ref,
    diffusivity_ref,
    zh_ref,
    zl_ref,
    ph_ref,
    pl_ref,
    yh_ref,
    yl_ref,
    low_ref,
    high_ref,
    gain_ref,
    out_ref,
    plain_ref,
    ends_ref,
    planes,
    power,
    *,
    padded,
):
    step = pl.program_id(0)
    steps = pl.num_programs(0)
    block, nz, ny = block_ref.shape[2:]
    matrix = collocation_matrix()

    @pl.when(step == 0)
    def _():
        ends_ref[...] = jnp.zeros_like(ends_ref)
        planes[0] = halo_low_ref[0, :, 0]
        for m in range(NODES):
            power[m, 0] = jnp.ones_like(power[m, 0])
            power[m, 1] = jnp.zeros_like(power[m, 1])

    @pl.when(step > 0)
    def _():
        planes[0] = prev_ref[0, :, 0]

    @pl.when(step == steps - 1)
    def _():
        planes[block + 1] = halo_high_ref[0, :, 0]

    @pl.when(step < steps - 1)
    def _():
        planes[block + 1] = next_ref[0, :, 0]

    for j in range(block):
        planes[j + 1] = block_ref[0, :, j]

    def pair(index, carry):
        columns = []
        plains = []
        for half in range(2):
            j = 2 * index + half
            factor = diffusion_number * (diffusivity_ref[j] - 1.0)
            spread = []
            for n in range(NODES):
                f = planes[j + 1, n]
                lap = (
                    (planes[j, n] + planes[j + 2, n])
                    + (pltpu.roll(f, 1, 0) + pltpu.roll(f, nz - 1, 0))
                    + (pltpu.roll(f, 1, 1) + pltpu.roll(f, ny - 1, 1))
                    - 6.0 * f
                )
                spread.append(factor * lap)
            mixed = []
            for m in range(NODES):
                total = right_ref[0, m, j]
                for n in range(NODES):
                    total = total + matrix[m][n] * spread[n]
                mixed.append(total)
            columns.append(jnp.concatenate(mixed, axis=0))
            plains.append(planes[j + 1, NODES - 1])
        spectrum_z = dot3_table_left(zh_ref[...], zl_ref[...], jnp.concatenate(columns, axis=1))
        plain_z = dot3_table_left(ph_ref[...], pl_ref[...], jnp.concatenate(plains, axis=1))
        rows = []
        for half in range(2):
            lanes = slice(half * ny, (half + 1) * ny)
            for m in range(NODES):
                base = 2 * m * padded
                rows.append(
                    jnp.concatenate(
                        [
                            spectrum_z[base : base + padded, lanes],
                            spectrum_z[base + padded : base + 2 * padded, lanes],
                        ],
                        axis=1,
                    )
                )
            rows.append(
                jnp.concatenate([plain_z[:padded, lanes], plain_z[padded:, lanes]], axis=1)
            )
        spectrum = dot3_table_right(jnp.concatenate(rows, axis=0), yh_ref[...], yl_ref[...])
        for half in range(2):
            j = 2 * index + half
            for m in range(NODES):
                base = (half * (NODES + 1) + m) * padded
                value = (spectrum[base : base + padded, :ny], spectrum[base : base + padded, ny:])
                value = c_mul(value, (gain_ref[m, 0], gain_ref[m, 1]))
                out_ref[j, m, 0] = value[0]
                out_ref[j, m, 1] = value[1]
            base = (half * (NODES + 1) + NODES) * padded
            plain_ref[j, 0] = spectrum[base : base + padded, :ny]
            plain_ref[j, 1] = spectrum[base : base + padded, ny:]
        return carry

    unrolled(block // 2, pair)

    def tile(t, carry):
        rows = pl.ds(t * 8, 8)
        for m in range(NODES):
            low = (low_ref[m, 0, rows], low_ref[m, 1, rows])
            high = (high_ref[m, 0, rows], high_ref[m, 1, rows])
            reach = c_power(high, GROUP)
            ahead = (ends_ref[0, m, 0, rows], ends_ref[0, m, 1, rows])
            behind = (ends_ref[1, m, 0, rows], ends_ref[1, m, 1, rows])
            scale = (power[m, 0, rows], power[m, 1, rows])
            for base in range(0, block, GROUP):
                values = [
                    (out_ref[base + j, m, 0, rows], out_ref[base + j, m, 1, rows])
                    for j in range(GROUP)
                ]
                for value in values:
                    ahead = c_add(c_mul(ahead, low), value)
                back = values[-1]
                for value in values[-2::-1]:
                    back = c_add(c_mul(back, high), value)
                behind = c_add(behind, c_mul(scale, back))
                scale = c_mul(scale, reach)
            for part in range(2):
                ends_ref[0, m, part, rows] = ahead[part]
                ends_ref[1, m, part, rows] = behind[part]
                power[m, part, rows] = scale[part]
        return carry

    lax.fori_loop(0, padded // 8, tile, 0)


def full(shape):
    zeros = (0,) * len(shape)
    return pl.BlockSpec(shape, lambda *_: zeros)


def forward_stage(iterate, right_side, diffusivity, halos, lines):
    _, _, count, nz, ny = iterate.shape
    _, padded = half_rows(nz)
    block = GROUP
    blocks = count // block
    mixed, plain, along_y = forward_tables(nz, ny)
    tables = [*split_table(mixed), *split_table(plain), *split_table(along_y), *lines[:3]]
    plane = (1, NODES, 1, nz, ny)
    return pl.pallas_call(
        functools.partial(forward_kernel, padded=padded),
        grid=(blocks,),
        in_specs=[
            pl.BlockSpec((1, NODES, block, nz, ny), lambda b: (0, 0, b, 0, 0)),
            pl.BlockSpec(plane, lambda b: (0, 0, jnp.maximum(b * block - 1, 0), 0, 0)),
            pl.BlockSpec(plane, lambda b: (0, 0, jnp.minimum((b + 1) * block, count - 1), 0, 0)),
            full(plane),
            full(plane),
            pl.BlockSpec((1, NODES, block, nz, ny), lambda b: (0, 0, b, 0, 0)),
            pl.BlockSpec((block, nz, ny), lambda b: (b, 0, 0)),
            *[full(t.shape) for t in tables],
        ],
        out_specs=[
            pl.BlockSpec((block, NODES, 2, padded, ny), lambda b: (b, 0, 0, 0, 0)),
            pl.BlockSpec((block, 2, padded, ny), lambda b: (b, 0, 0, 0)),
            full((2, NODES, 2, padded, ny)),
        ],
        out_shape=[
            jax.ShapeDtypeStruct((count, NODES, 2, padded, ny), jnp.float32),
            jax.ShapeDtypeStruct((count, 2, padded, ny), jnp.float32),
            jax.ShapeDtypeStruct((2, NODES, 2, padded, ny), jnp.float32),
        ],
        scratch_shapes=[
            pltpu.VMEM((block + 2, NODES, nz, ny), jnp.float32),
            pltpu.VMEM((NODES, 2, padded, ny), jnp.float32),
        ],
        compiler_params=pltpu.CompilerParams(
            dimension_semantics=("arbitrary",), vmem_limit_bytes=60 * 1024 * 1024
        ),
    )(iterate, iterate, iterate, *halos, right_side, diffusivity, *tables)


def enter_back(state, states_ref, low_ref, close_ref):
    for m in range(NODES):
        value = c_mul((state[m, 0], state[m, 1]), (low_ref[m, 0], low_ref[m, 1]))
        value = c_add(value, (states_ref[1, m, 0], states_ref[1, m, 1]))
        value = c_mul(value, (close_ref[m, 0], close_ref[m, 1]))
        state[m, 0] = value[0]
        state[m, 1] = value[1]


def node_kernel(
    mask_ref, c_ref, plain_ref, states_ref, low_ref, high_ref, close_ref, out_ref, ahead, state, *, half
):
    phase = pl.program_id(0)
    step = pl.program_id(1)
    blocks = pl.num_programs(1)
    block, _, _, padded, ny = c_ref.shape
    _, vectors, _, _ = node_constants()
    last = [complex(v) for v in vectors[NODES - 1]]

    @pl.when((phase == 0) & (step == 0))
    def _():
        state[...] = states_ref[0]

    @pl.when((phase == 1) & (step == 0))
    def _():
        enter_back(state, states_ref, low_ref, close_ref)

    @pl.when(phase == 0)
    def _():
        def tile(t, carry):
            rows = pl.ds(t * 8, 8)
            for m in range(NODES):
                low = (low_ref[m, 0, rows], low_ref[m, 1, rows])
                value = (state[m, 0, rows], state[m, 1, rows])
                for j in range(block):
                    value = c_add(c_mul(value, low), (c_ref[j, m, 0, rows], c_ref[j, m, 1, rows]))
                    ahead[step * block + j, m, 0, rows] = value[0]
                    ahead[step * block + j, m, 1, rows] = value[1]
                state[m, 0, rows] = value[0]
                state[m, 1, rows] = value[1]
            return carry

        lax.fori_loop(0, padded // 8, tile, 0)

    @pl.when(phase == 1)
    def _():
        lane = lax.broadcasted_iota(jnp.int32, (GROUP, ny), 1)
        mask = mask_ref[0]

        def totals(start, base):
            rows = pl.ds(start, 8)
            first = (blocks - 1 - step) * block + base
            total = [
                [-mask * plain_ref[base + j, part, rows] for part in range(2)] for j in range(GROUP)
            ]
            for m in range(NODES):
                high = (high_ref[m, 0, rows], high_ref[m, 1, rows])
                value = (state[m, 0, rows], state[m, 1, rows])
                for j in reversed(range(GROUP)):
                    value = c_add(
                        c_mul(value, high), (ahead[first + j, m, 0, rows], ahead[first + j, m, 1, rows])
                    )
                    total[j][0] += last[m].real * value[0] - last[m].imag * value[1]
                    total[j][1] += last[m].real * value[1] + last[m].imag * value[0]
                state[m, 0, rows] = value[0]
                state[m, 1, rows] = value[1]
            return [
                jnp.swapaxes(jnp.stack([total[j][part] for j in range(GROUP)]), 0, 1)
                for part in range(2)
            ]

        for base in reversed(range(0, block, GROUP)):
            edge = [value[0] for value in totals(half, base)]
            top = totals(0, base)
            turned = [pltpu.roll(value, ny // 2, 1) for value in edge]
            folded = [jnp.where(lane <= ny // 2, top[part][0], turned[part]) for part in range(2)]
            folded[1] = jnp.where(lane % (ny // 2) == 0, edge[0], folded[1])
            for part in range(2):
                out_ref[0, part, base : base + GROUP] = folded[part]
                out_ref[1:8, part, base : base + GROUP] = top[part][1:]

            def tile(t, carry):
                start = pl.multiple_of(t * 8, 8)
                value = totals(start, base)
                for part in range(2):
                    out_ref[pl.ds(start, 8), part, base : base + GROUP] = value[part]
                return carry

            lax.fori_loop(1, half // 8, tile, 0)


def node_stage(c, plain, mask, states, lines, nz):
    count, _, _, padded, ny = c.shape
    block = block_of(count)
    blocks = count // block
    half = nz // 2

    def early(phase, b):
        return jnp.where(phase == 0, b, blocks - 1)

    def late(phase, b):
        return jnp.where(phase == 0, blocks - 1, blocks - 1 - b)

    tables = [lines[0], lines[1], lines[4]]
    return pl.pallas_call(
        functools.partial(node_kernel, half=half),
        grid=(2, blocks),
        in_specs=[
            pl.BlockSpec(memory_space=pltpu.SMEM),
            pl.BlockSpec((block, NODES, 2, padded, ny), lambda a, b: (early(a, b), 0, 0, 0, 0)),
            pl.BlockSpec((block, 2, padded, ny), lambda a, b: (late(a, b), 0, 0, 0)),
            full(states.shape),
            *[full(t.shape) for t in tables],
        ],
        out_specs=pl.BlockSpec((half, 2, block, ny), lambda a, b: (0, 0, late(a, b), 0)),
        out_shape=jax.ShapeDtypeStruct((half, 2, count, ny), jnp.float32),
        scratch_shapes=[
            pltpu.VMEM((count, NODES, 2, padded, ny), jnp.float32),
            pltpu.VMEM((NODES, 2, padded, ny), jnp.float32),
        ],
        compiler_params=pltpu.CompilerParams(
            dimension_semantics=("arbitrary", "arbitrary"), vmem_limit_bytes=60 * 1024 * 1024
        ),
    )(mask, c, plain, states, *tables)


def couple_kernel(q_ref, th_ref, tl_ref, ih_ref, il_ref, grow_ref, close_ref, out_ref, work):
    steps, slabs, _, count, width = q_ref.shape
    nx = slabs * count
    joined = width % 128 == 0

    def side_by_side(table_high, table_low, values):
        if not joined:
            return [dot3_table_left(table_high, table_low, value) for value in values]
        wide = dot3_table_left(table_high, table_low, jnp.concatenate(values, axis=1))
        return [wide[:, i * width : (i + 1) * width] for i in range(len(values))]

    def ahead(s, carry):
        lines = [
            jnp.concatenate([q_ref[s, p, part] for p in range(slabs)], axis=0) for part in range(2)
        ]
        for part, waves in enumerate(side_by_side(th_ref[...], tl_ref[...], lines)):
            work[s, part, 0] = waves[:nx]
            work[s, part, 1] = waves[nx:]
        return carry

    lax.fori_loop(0, steps, ahead, 0)

    def tile(t, carry):
        rows = pl.ds(t * 8, 8)
        for part in range(2):
            grow = (grow_ref[part, 0, rows], grow_ref[part, 1, rows])
            values = [(work[s, part, 0, rows], work[s, part, 1, rows]) for s in range(steps)]
            value = values[0]
            for s in range(1, steps):
                value = c_add(c_mul(grow, value), values[s])
            value = c_mul(value, (close_ref[part, 0, rows], close_ref[part, 1, rows]))
            for s in range(steps):
                work[s, part, 0, rows] = value[0]
                work[s, part, 1, rows] = value[1]
                if s + 1 < steps:
                    value = c_add(c_mul(grow, value), values[s])
        return carry

    lax.fori_loop(0, nx // 8, tile, 0)

    def back(i, carry):
        pair = [2 * i, 2 * i + 1]
        lines = [
            jnp.concatenate(
                [work[s, 0, 0] - work[s, 1, 1], work[s, 0, 1] + work[s, 1, 0]], axis=0
            )
            for s in pair
        ]
        for s, value in zip(pair, side_by_side(ih_ref[...], il_ref[...], lines)):
            for part in range(2):
                for p in range(slabs):
                    base = part * nx + p * count
                    out_ref[s, p, part] = value[base : base + count]
        return carry

    lax.fori_loop(0, steps // 2, back, 0)


def couple_stage(q, velocity, first_mode, nz, ny):
    steps, slabs, _, count, width = q.shape
    nx = slabs * count
    forward, backward = x_tables(nx)
    values, vectors, _, weights = node_constants()
    mode = first_mode + jnp.arange(width, dtype=jnp.int32)
    row, lane = mode // ny, mode % ny
    edge = row == 0
    corner = edge & (lane % (ny // 2) == 0)
    wave_z = jnp.where(edge & (lane > ny // 2), nz // 2, row)
    wave_y = jnp.where(edge & (lane > ny // 2), lane - ny // 2, lane)
    wave_z = jnp.stack([wave_z, jnp.where(corner, nz // 2, wave_z)])[:, None, :]
    theta_z = wave_z.astype(jnp.float32) * (2.0 * math.pi / nz)
    theta_y = wave_y.astype(jnp.float32)[None, None, :] * (2.0 * math.pi / ny)
    theta_x = jnp.arange(nx, dtype=jnp.int32).astype(jnp.float32)[None, :, None] * (2.0 * math.pi / nx)
    real = diffusion_number * (
        (2.0 * jnp.cos(theta_x) - 2.0)
        + (2.0 * jnp.cos(theta_z) - 2.0)
        + (2.0 * jnp.cos(theta_y) - 2.0)
    )
    imag = -(
        velocity[0] * jnp.sin(theta_x)
        + velocity[1] * jnp.sin(theta_y)
        + velocity[2] * jnp.sin(theta_z)
    )
    grow = None
    for m in range(NODES):
        mu = complex(values[m])
        below = (1.0 - (mu.real * real - mu.imag * imag), -(mu.real * imag + mu.imag * real))
        above = complex(vectors[NODES - 1, m] * weights[m])
        added = c_div((above.real, above.imag), below)
        grow = added if grow is None else (grow[0] + added[0], grow[1] + added[1])
    whole = c_power(grow, steps)
    close = c_div(
        (circulant_alpha, 0.0), (1.0 - circulant_alpha * whole[0], -circulant_alpha * whole[1])
    )
    return pl.pallas_call(
        couple_kernel,
        out_shape=jax.ShapeDtypeStruct(q.shape, jnp.float32),
        scratch_shapes=[pltpu.VMEM((steps, 2, 2, nx, width), jnp.float32)],
        compiler_params=pltpu.CompilerParams(vmem_limit_bytes=60 * 1024 * 1024),
    )(
        q,
        *split_table(forward),
        *split_table(backward),
        jnp.stack(grow, axis=1),
        jnp.stack(close, axis=1),
    )


def edge_kernel(b_ref, low_ref, high_ref, beta_ref, wide_ref, out_ref):
    half, _, count, ny = b_ref.shape
    padded = wide_ref.shape[2]
    lane = lax.broadcasted_iota(jnp.int32, (GROUP, ny), 1)
    inside = lane % (ny // 2) != 0
    kept = jnp.where(inside, jnp.where(lane < ny // 2, 2.0, 0.0), 1.0)
    zero = jnp.zeros((GROUP, ny), jnp.float32)

    def unfold(g, carry):
        base = pl.multiple_of(g * GROUP, GROUP)
        planes = pl.ds(base, GROUP)
        top = [b_ref[0, part, planes] for part in range(2)]
        turned = [pltpu.roll(value, ny // 2, 1) for value in top]
        first = (top[0], jnp.where(inside, top[1], 0.0))
        edge = (jnp.where(inside, turned[0], top[1]), jnp.where(inside, turned[1], 0.0))
        for part in range(2):
            for start in range(0, half, 8):
                rows = [b_ref[start + r, part, planes] for r in range(8)]
                if start == 0:
                    rows[0] = first[part] * kept
                wide_ref[planes, part, start : start + 8] = jnp.swapaxes(jnp.stack(rows), 0, 1)
            rows = [edge[part] * kept] + [zero] * 7
            wide_ref[planes, part, half : half + 8] = jnp.swapaxes(jnp.stack(rows), 0, 1)
        return carry

    lax.fori_loop(0, count // GROUP, unfold, 0)

    def tile(t, carry):
        rows = pl.ds(pl.multiple_of(t * 8, 8), 8)
        for side, table in enumerate((low_ref, high_ref)):
            decay = [(table[m, 0, rows], table[m, 1, rows]) for m in range(NODES)]

            def group(g, values):
                for i in range(GROUP):
                    j = g * GROUP + i
                    j = j if side == 0 else count - 1 - j
                    plane = (wide_ref[j, 0, rows], wide_ref[j, 1, rows])
                    values = [c_add(c_mul(v, d), plane) for v, d in zip(values, decay)]
                return values

            values = lax.fori_loop(0, count // GROUP, group, [(zero, zero)] * NODES)
            for m in range(NODES):
                value = c_mul(values[m], (beta_ref[m, 0, rows], beta_ref[m, 1, rows]))
                out_ref[side, m, 0, rows] = value[0]
                out_ref[side, m, 1, rows] = value[1]
        return carry

    lax.fori_loop(0, padded // 8, tile, 0)


def edge_stage(b, lines):
    count = b.shape[2]
    padded, ny = lines[0].shape[2:]
    return pl.pallas_call(
        edge_kernel,
        out_shape=[
            jax.ShapeDtypeStruct((count, 2, padded, ny), jnp.float32),
            jax.ShapeDtypeStruct((2, NODES, 2, padded, ny), jnp.float32),
        ],
        compiler_params=pltpu.CompilerParams(vmem_limit_bytes=60 * 1024 * 1024),
    )(b, lines[0], lines[1], lines[3])


def inverse_kernel(
    c_ref,
    b_ref,
    states_ref,
    low_ref,
    high_ref,
    beta_ref,
    close_ref,
    yh_ref,
    yl_ref,
    zh_ref,
    zl_ref,
    out_ref,
    ahead,
    state,
):
    phase = pl.program_id(0)
    step = pl.program_id(1)
    blocks = pl.num_programs(1)
    block, _, _, padded, ny = c_ref.shape
    nz = out_ref.shape[3]

    @pl.when((phase == 0) & (step == 0))
    def _():
        state[...] = states_ref[0]

    @pl.when((phase == 1) & (step == 0))
    def _():
        enter_back(state, states_ref, low_ref, close_ref)

    @pl.when(phase == 0)
    def _():
        def tile(t, carry):
            rows = pl.ds(pl.multiple_of(t * 8, 8), 8)
            for base in range(0, block, GROUP):
                planes = [
                    (b_ref[base + j, 0, rows], b_ref[base + j, 1, rows]) for j in range(GROUP)
                ]
                for m in range(NODES):
                    low = (low_ref[m, 0, rows], low_ref[m, 1, rows])
                    beta = (beta_ref[m, 0, rows], beta_ref[m, 1, rows])
                    value = (state[m, 0, rows], state[m, 1, rows])
                    for j in range(GROUP):
                        source = c_add(
                            c_mul(planes[j], beta),
                            (c_ref[base + j, m, 0, rows], c_ref[base + j, m, 1, rows]),
                        )
                        value = c_add(c_mul(value, low), source)
                        ahead[step * block + base + j, m, 0, rows] = value[0]
                        ahead[step * block + base + j, m, 1, rows] = value[1]
                    state[m, 0, rows] = value[0]
                    state[m, 1, rows] = value[1]
            return carry

        lax.fori_loop(0, padded // 8, tile, 0)

    @pl.when(phase == 1)
    def _():
        first = (blocks - 1 - step) * block

        def tile(t, carry):
            rows = pl.ds(pl.multiple_of(t * 8, 8), 8)
            for m in range(NODES):
                high = (high_ref[m, 0, rows], high_ref[m, 1, rows])
                value = (state[m, 0, rows], state[m, 1, rows])
                for j in reversed(range(block)):
                    value = c_add(
                        c_mul(value, high), (ahead[first + j, m, 0, rows], ahead[first + j, m, 1, rows])
                    )
                    ahead[first + j, m, 0, rows] = value[0]
                    ahead[first + j, m, 1, rows] = value[1]
                state[m, 0, rows] = value[0]
                state[m, 1, rows] = value[1]
            return carry

        lax.fori_loop(0, padded // 8, tile, 0)

        def pair(i, carry):
            rows = []
            for half in range(2):
                row = first + 2 * i + half
                for m in range(NODES):
                    rows.append(jnp.concatenate([ahead[row, m, 0], ahead[row, m, 1]], axis=1))
            lines = dot3_table_right(jnp.concatenate(rows, axis=0), yh_ref[...], yl_ref[...])
            columns = []
            for half in range(2):
                stacked = []
                for m in range(NODES):
                    base = (half * NODES + m) * padded
                    stacked.append(lines[base : base + padded, :ny])
                    stacked.append(lines[base : base + padded, ny:])
                columns.append(jnp.concatenate(stacked, axis=0))
            grid = dot3_table_left(zh_ref[...], zl_ref[...], jnp.concatenate(columns, axis=1))
            for half in range(2):
                for n in range(NODES):
                    out_ref[0, n, 2 * i + half] = grid[
                        n * nz : (n + 1) * nz, half * ny : (half + 1) * ny
                    ]
            return carry

        unrolled(block // 2, pair)


def inverse_stage(c, b, states, lines, nz):
    count, _, _, padded, ny = c.shape
    block = block_of(count)
    blocks = count // block
    mixed, along_y = inverse_tables(nz, ny)
    tables = [lines[0], lines[1], lines[3], lines[4], *split_table(along_y), *split_table(mixed)]

    def early(phase, b):
        return jnp.where(phase == 0, b, blocks - 1)

    def late(phase, b):
        return jnp.where(phase == 0, blocks - 1, blocks - 1 - b)

    return pl.pallas_call(
        inverse_kernel,
        grid=(2, blocks),
        in_specs=[
            pl.BlockSpec((block, NODES, 2, padded, ny), lambda a, b: (early(a, b), 0, 0, 0, 0)),
            pl.BlockSpec((block, 2, padded, ny), lambda a, b: (early(a, b), 0, 0, 0)),
            full(states.shape),
            *[full(t.shape) for t in tables],
        ],
        out_specs=pl.BlockSpec((1, NODES, block, nz, ny), lambda a, b: (0, 0, late(a, b), 0, 0)),
        out_shape=jax.ShapeDtypeStruct((1, NODES, count, nz, ny), jnp.float32),
        scratch_shapes=[
            pltpu.VMEM((count, NODES, 2, padded, ny), jnp.float32),
            pltpu.VMEM((NODES, 2, padded, ny), jnp.float32),
        ],
        compiler_params=pltpu.CompilerParams(
            dimension_semantics=("arbitrary", "arbitrary"), vmem_limit_bytes=60 * 1024 * 1024
        ),
    )(c, b, states, *tables)


def ring_states(ends, lines, count, slabs):
    result = []
    for side in range(2):
        decay = c_power((lines[side][:, 0], lines[side][:, 1]), count)
        total = None
        for distance in range(slabs, 0, -1):
            if distance == slabs:
                moved = ends[side]
            else:
                shift = distance if side == 0 else -distance
                moved = lax.ppermute(
                    ends[side], "space", [(i, (i + shift) % slabs) for i in range(slabs)]
                )
            moved = (moved[:, 0], moved[:, 1])
            if total is None:
                total = moved
            else:
                total = c_mul(total, decay)
                total = (total[0] + moved[0], total[1] + moved[1])
        whole = c_power(decay, slabs)
        total = c_div(total, (1.0 - whole[0], -whole[1]))
        result.append(jnp.stack(total, axis=1))
    return jnp.stack(result)


def to_modes(q, devices):
    half, _, count, ny = q.shape
    pieces = devices // half
    if pieces > 1:
        q = q.reshape(half, 2 * count, pieces, ny // pieces)
        q = jnp.transpose(q, (0, 2, 1, 3))
    return q.reshape(devices, 2 * count, ny // pieces)


def from_modes(b, half):
    devices, lines, width = b.shape
    pieces = devices // half
    if pieces > 1:
        b = jnp.transpose(b.reshape(half, pieces, lines, width), (0, 2, 1, 3))
    return b.reshape(half, 2, lines // 2, pieces * width)


def shards(iterate, right_side, diffusivity, velocity):
    steps, slabs = lax.axis_size("tm"), lax.axis_size("space")
    devices = steps * slabs
    _, _, count, nz, ny = iterate.shape
    up = [(i, (i + 1) % slabs) for i in range(slabs)]
    down = [(target, source) for source, target in up]
    halos = (
        lax.ppermute(iterate[:, :, count - 1 :], "space", up),
        lax.ppermute(iterate[:, :, :1], "space", down),
    )
    lines = line_tables(velocity, nz, ny)
    c, plain, ends = forward_stage(iterate, right_side, diffusivity, halos, lines)
    states = ring_states(ends, lines, count, slabs)
    step = lax.axis_index("tm")
    mask = jnp.where(step == steps - 1, 1.0, 0.0).astype(jnp.float32)[None]
    q = node_stage(c, plain, mask, states, lines, nz)
    q = lax.all_to_all(to_modes(q, devices), ("tm", "space"), 0, 0, tiled=True)
    width = q.shape[2]
    first_mode = (step * slabs + lax.axis_index("space")) * width
    b = couple_stage(q.reshape(steps, slabs, 2, count, width), velocity, first_mode, nz, ny)
    b = lax.all_to_all(b.reshape(devices, 2 * count, width), ("tm", "space"), 0, 0, tiled=True)
    b, ends = edge_stage(from_modes(b, nz // 2), lines)
    states = states + ring_states(ends, lines, count, slabs)
    return inverse_stage(c, b, states, lines, nz)


def solution(mesh):
    placed = (
        P("tm", None, "space", None, None),
        P("tm", None, "space", None, None),
        P("space", None, None),
        P(),
    )
    return jax.shard_map(
        shards,
        mesh=mesh,
        in_specs=placed,
        out_specs=P("tm", None, "space", None, None),
        check_vma=False,
    )
```

```python
import functools
import math

import jax
import jax.numpy as jnp
import numpy as np
from jax import lax
from jax.experimental import pallas as pl
from jax.experimental.pallas import tpu as pltpu
from jax.sharding import PartitionSpec as P

diffusion_number = 16.0
circulant_alpha = 0.1
NODES = 4
GROUP = 8


def collocation_matrix():
    radau_nodes = [0.08858795951270394, 0.4094668644407347, 0.7876594617608471, 1.0]
    matrix = [[0.0] * 4 for row_index in range(4)]
    for column_index in range(4):
        coefficients = [1.0]
        for other_index in range(4):
            if other_index != column_index:
                scale_value = 1.0 / (radau_nodes[column_index] - radau_nodes[other_index])
                shifted = [0.0] + [value * scale_value for value in coefficients]
                lowered = [
                    -radau_nodes[other_index] * scale_value * value for value in coefficients
                ] + [0.0]
                coefficients = [
                    left_value + right_value for left_value, right_value in zip(shifted, lowered)
                ]
        for row_index in range(4):
            total = 0.0
            for power_index in range(len(coefficients)):
                total = total + coefficients[power_index] * radau_nodes[row_index] ** (
                    power_index + 1
                ) / (power_index + 1)
            matrix[row_index][column_index] = total
    return matrix


def solve_system(matrix, target):
    count = len(target)
    rows_list = [list(matrix[row_index]) + [target[row_index]] for row_index in range(count)]
    for column in range(count):
        best_row = column
        for candidate in range(column + 1, count):
            if abs(rows_list[candidate][column]) > abs(rows_list[best_row][column]):
                best_row = candidate
        saved_row = rows_list[column]
        rows_list[column] = rows_list[best_row]
        rows_list[best_row] = saved_row
        leader = rows_list[column][column]
        for other_row in range(count):
            if other_row != column:
                factor = rows_list[other_row][column] / leader
                rows_list[other_row] = [
                    left_value - factor * right_value
                    for left_value, right_value in zip(rows_list[other_row], rows_list[column])
                ]
    return [
        rows_list[row_index][count] / rows_list[row_index][row_index] for row_index in range(count)
    ]


def node_basis():
    matrix = collocation_matrix()
    helper = [[0.0] * 4 for row_index in range(4)]
    coefficients = [0.0, 0.0, 0.0, 0.0, 1.0]
    for order in range(1, 5):
        product = [
            [
                sum((matrix[row_index][inner] * helper[inner][column] for inner in range(4)))
                for column in range(4)
            ]
            for row_index in range(4)
        ]
        for row_index in range(4):
            product[row_index][row_index] = product[row_index][row_index] + coefficients[5 - order]
        helper = product
        trace_value = sum(
            (
                sum((matrix[row_index][inner] * helper[inner][row_index] for inner in range(4)))
                for row_index in range(4)
            )
        )
        coefficients[4 - order] = -trace_value / order
    roots_list = [(0.4 + 0.9j) ** power_index for power_index in range(4)]
    for sweep in range(400):
        for root_index in range(4):
            current = roots_list[root_index]
            numer = 0.0
            for power_index in range(4, -1, -1):
                numer = numer * current + coefficients[power_index]
            denom = 1.0
            for other_index in range(4):
                if other_index != root_index:
                    denom = denom * (current - roots_list[other_index])
            roots_list[root_index] = current - numer / denom
    vectors = [[0.0] * 4 for row_index in range(4)]
    for root_index in range(4):
        shifted = [
            [
                matrix[row_index][column] - (roots_list[root_index] if row_index == column else 0.0)
                for column in range(3)
            ]
            for row_index in range(3)
        ]
        target = [-matrix[row_index][3] for row_index in range(3)]
        parts = solve_system(shifted, target) + [1.0 + 0j]
        for row_index in range(4):
            vectors[row_index][root_index] = parts[row_index]
    inverse = [[0.0] * 4 for row_index in range(4)]
    for column in range(4):
        unit = [1.0 if row_index == column else 0.0 for row_index in range(4)]
        parts = solve_system(vectors, unit)
        for row_index in range(4):
            inverse[row_index][column] = parts[row_index]
    weights = [sum((inverse[row_index][column] for column in range(4))) for row_index in range(4)]
    return (roots_list, vectors, inverse, weights)


def split_table(table):
    table = jnp.asarray(np.asarray(table, np.float32))
    high = table.astype(jnp.bfloat16)
    return high, (table - high.astype(jnp.float32)).astype(jnp.bfloat16)


def split(values):
    high = values.astype(jnp.bfloat16)
    return high, (values - high.astype(jnp.float32)).astype(jnp.bfloat16)


def dot(left, right):
    return jnp.dot(left, right, preferred_element_type=jnp.float32)


def dot3_table_left(table_high, table_low, values):
    high, low = split(values)
    return dot(table_high, high) + (dot(table_high, low) + dot(table_low, high))


def dot3_table_right(values, table_high, table_low):
    high, low = split(values)
    return dot(high, table_high) + (dot(low, table_high) + dot(high, table_low))


def node_constants():
    values, vectors, inverse, weights = node_basis()
    return (
        np.array([complex(v) for v in values]),
        np.array([[complex(v) for v in row] for row in vectors]),
        np.array([[complex(v) for v in row] for row in inverse]),
        np.array([complex(v) for v in weights]),
    )


def half_rows(nz):
    kept = nz // 2 + 1
    return kept, -(-kept // 8) * 8


def forward_tables(nz, ny):
    _, _, inverse, _ = node_constants()
    kept, padded = half_rows(nz)
    wave = np.zeros((padded, nz), complex)
    wave[:kept] = np.exp(-2j * math.pi * np.outer(np.arange(kept), np.arange(nz)) / nz)
    mixed = np.zeros((NODES, 2, padded, NODES, nz))
    for m in range(NODES):
        for n in range(NODES):
            mixed[m, 0, :, n] = (inverse[m, n] * wave).real
            mixed[m, 1, :, n] = (inverse[m, n] * wave).imag
    plain = np.concatenate([wave.real, wave.imag], axis=0)
    angle = 2 * math.pi * (np.outer(np.arange(ny), np.arange(ny)) % ny) / ny
    c, s = np.cos(angle), np.sin(angle)
    along_y = np.block([[c, -s], [s, c]])
    return mixed.reshape(NODES * 2 * padded, NODES * nz), plain, along_y


def inverse_tables(nz, ny):
    _, vectors, _, _ = node_constants()
    kept, padded = half_rows(nz)
    weight = np.where((np.arange(kept) == 0) | (2 * np.arange(kept) == nz), 1.0, 2.0)
    wave = np.zeros((nz, padded), complex)
    wave[:, :kept] = np.exp(2j * math.pi * np.outer(np.arange(nz), np.arange(kept)) / nz) * weight / nz
    mixed = np.zeros((NODES, nz, NODES, 2, padded))
    for n in range(NODES):
        for m in range(NODES):
            mixed[n, :, m, 0] = (vectors[n, m] * wave).real
            mixed[n, :, m, 1] = -(vectors[n, m] * wave).imag
    angle = 2 * math.pi * (np.outer(np.arange(ny), np.arange(ny)) % ny) / ny
    c, s = np.cos(angle) / ny, np.sin(angle) / ny
    along_y = np.block([[c, s], [-s, c]])
    return mixed.reshape(NODES * nz, NODES * 2 * padded), along_y


def x_tables(nx):
    angle = 2 * math.pi * (np.outer(np.arange(nx), np.arange(nx)) % nx) / nx
    c, s = np.cos(angle), np.sin(angle)
    return np.concatenate([c, -s], axis=0), np.block([[c, -s], [s, c]]) / nx


def c_mul(a, b):
    return a[0] * b[0] - a[1] * b[1], a[0] * b[1] + a[1] * b[0]


def c_add(a, b):
    return a[0] + b[0], a[1] + b[1]


def c_div(a, b):
    size = b[0] * b[0] + b[1] * b[1]
    return (a[0] * b[0] + a[1] * b[1]) / size, (a[1] * b[0] - a[0] * b[1]) / size


def c_power(a, count):
    result = None
    while count:
        if count & 1:
            result = a if result is None else c_mul(result, a)
        count >>= 1
        if count:
            a = c_mul(a, a)
    return result


def c_sqrt(a):
    size = jnp.sqrt(a[0] * a[0] + a[1] * a[1])
    large = jnp.sqrt(0.5 * (size + jnp.abs(a[0])))
    small = a[1] / (2.0 * large)
    flip = a[0] < 0.0
    return (
        jnp.where(flip, jnp.abs(small), large),
        jnp.where(flip, jnp.where(a[1] < 0.0, -large, large), small),
    )


def line_tables(velocity, nz, ny):
    values, _, _, weights = node_constants()
    _, padded = half_rows(nz)
    theta_z = jnp.arange(padded, dtype=jnp.int32).astype(jnp.float32) * (2.0 * math.pi / nz)
    theta_y = jnp.arange(ny, dtype=jnp.int32).astype(jnp.float32) * (2.0 * math.pi / ny)
    real = diffusion_number * (
        (2.0 * jnp.cos(theta_z)[:, None] - 2.0) + (2.0 * jnp.cos(theta_y)[None, :] - 2.0)
    )
    imag = -(velocity[1] * jnp.sin(theta_y)[None, :] + velocity[2] * jnp.sin(theta_z)[:, None])
    real, imag = real[None], imag[None]
    mu = (
        jnp.asarray(values.real, jnp.float32)[:, None, None],
        jnp.asarray(values.imag, jnp.float32)[:, None, None],
    )
    part = c_mul(mu, (real - 2.0 * diffusion_number, imag))
    diagonal = (1.0 - part[0], -part[1])
    from_low = diffusion_number + 0.5 * velocity[0]
    from_high = diffusion_number - 0.5 * velocity[0]
    mu2 = c_mul(mu, mu)
    square = c_mul(diagonal, diagonal)
    product = 4.0 * from_low * from_high
    root = c_sqrt((square[0] - product * mu2[0], square[1] - product * mu2[1]))
    turn = diagonal[0] * root[0] + diagonal[1] * root[1] < 0.0
    root = (jnp.where(turn, -root[0], root[0]), jnp.where(turn, -root[1], root[1]))
    kappa = (0.5 * (diagonal[0] + root[0]), 0.5 * (diagonal[1] + root[1]))
    ratio = c_div(mu, kappa)
    one = jnp.ones_like(root[0])
    gain = c_div((one, jnp.zeros_like(one)), kappa)
    close = c_div(kappa, root)
    beta = c_mul(
        gain,
        (
            jnp.asarray(weights.real, jnp.float32)[:, None, None],
            jnp.asarray(weights.imag, jnp.float32)[:, None, None],
        ),
    )
    low = (from_low * ratio[0], from_low * ratio[1])
    high = (from_high * ratio[0], from_high * ratio[1])
    return [jnp.stack(table, axis=1) for table in (low, high, gain, beta, close)]


def block_of(count):
    return 16 if count % 16 == 0 else GROUP


def unrolled(count, body, most=8):
    each = math.gcd(count, most)

    def turn(i, carry):
        for k in range(each):
            body(i * each + k, carry)
        return carry

    lax.fori_loop(0, count // each, turn, 0)


def forward_kernel(
    block_ref,
    prev_ref,
    next_ref,
    halo_low_ref,
    halo_high_ref,
    right_ref,
    diffusivity_ref,
    zh_ref,
    zl_ref,
    ph_ref,
    pl_ref,
    yh_ref,
    yl_ref,
    low_ref,
    high_ref,
    gain_ref,
    out_ref,
    plain_ref,
    ends_ref,
    planes,
    power,
    *,
    padded,
):
    step = pl.program_id(0)
    steps = pl.num_programs(0)
    block, nz, ny = block_ref.shape[2:]
    matrix = collocation_matrix()

    @pl.when(step == 0)
    def _():
        ends_ref[...] = jnp.zeros_like(ends_ref)
        planes[0] = halo_low_ref[0, :, 0]
        for m in range(NODES):
            power[m, 0] = jnp.ones_like(power[m, 0])
            power[m, 1] = jnp.zeros_like(power[m, 1])

    @pl.when(step > 0)
    def _():
        planes[0] = prev_ref[0, :, 0]

    @pl.when(step == steps - 1)
    def _():
        planes[block + 1] = halo_high_ref[0, :, 0]

    @pl.when(step < steps - 1)
    def _():
        planes[block + 1] = next_ref[0, :, 0]

    for j in range(block):
        planes[j + 1] = block_ref[0, :, j]

    def pair(index, carry):
        columns = []
        plains = []
        for half in range(2):
            j = 2 * index + half
            factor = diffusion_number * (diffusivity_ref[j] - 1.0)
            spread = []
            for n in range(NODES):
                f = planes[j + 1, n]
                lap = (
                    (planes[j, n] + planes[j + 2, n])
                    + (pltpu.roll(f, 1, 0) + pltpu.roll(f, nz - 1, 0))
                    + (pltpu.roll(f, 1, 1) + pltpu.roll(f, ny - 1, 1))
                    - 6.0 * f
                )
                spread.append(factor * lap)
            mixed = []
            for m in range(NODES):
                total = right_ref[0, m, j]
                for n in range(NODES):
                    total = total + matrix[m][n] * spread[n]
                mixed.append(total)
            columns.append(jnp.concatenate(mixed, axis=0))
            plains.append(planes[j + 1, NODES - 1])
        spectrum_z = dot3_table_left(zh_ref[...], zl_ref[...], jnp.concatenate(columns, axis=1))
        plain_z = dot3_table_left(ph_ref[...], pl_ref[...], jnp.concatenate(plains, axis=1))
        rows = []
        for half in range(2):
            lanes = slice(half * ny, (half + 1) * ny)
            for m in range(NODES):
                base = 2 * m * padded
                rows.append(
                    jnp.concatenate(
                        [
                            spectrum_z[base : base + padded, lanes],
                            spectrum_z[base + padded : base + 2 * padded, lanes],
                        ],
                        axis=1,
                    )
                )
            rows.append(
                jnp.concatenate([plain_z[:padded, lanes], plain_z[padded:, lanes]], axis=1)
            )
        spectrum = dot3_table_right(jnp.concatenate(rows, axis=0), yh_ref[...], yl_ref[...])
        for half in range(2):
            j = 2 * index + half
            for m in range(NODES):
                base = (half * (NODES + 1) + m) * padded
                value = (spectrum[base : base + padded, :ny], spectrum[base : base + padded, ny:])
                value = c_mul(value, (gain_ref[m, 0], gain_ref[m, 1]))
                out_ref[j, m, 0] = value[0]
                out_ref[j, m, 1] = value[1]
            base = (half * (NODES + 1) + NODES) * padded
            plain_ref[j, 0] = spectrum[base : base + padded, :ny]
            plain_ref[j, 1] = spectrum[base : base + padded, ny:]
        return carry

    unrolled(block // 2, pair)

    def tile(t, carry):
        rows = pl.ds(t * 8, 8)
        for m in range(NODES):
            low = (low_ref[m, 0, rows], low_ref[m, 1, rows])
            high = (high_ref[m, 0, rows], high_ref[m, 1, rows])
            reach = c_power(high, GROUP)
            ahead = (ends_ref[0, m, 0, rows], ends_ref[0, m, 1, rows])
            behind = (ends_ref[1, m, 0, rows], ends_ref[1, m, 1, rows])
            scale = (power[m, 0, rows], power[m, 1, rows])
            for base in range(0, block, GROUP):
                values = [
                    (out_ref[base + j, m, 0, rows], out_ref[base + j, m, 1, rows])
                    for j in range(GROUP)
                ]
                for value in values:
                    ahead = c_add(c_mul(ahead, low), value)
                back = values[-1]
                for value in values[-2::-1]:
                    back = c_add(c_mul(back, high), value)
                behind = c_add(behind, c_mul(scale, back))
                scale = c_mul(scale, reach)
            for part in range(2):
                ends_ref[0, m, part, rows] = ahead[part]
                ends_ref[1, m, part, rows] = behind[part]
                power[m, part, rows] = scale[part]
        return carry

    lax.fori_loop(0, padded // 8, tile, 0)


def full(shape):
    zeros = (0,) * len(shape)
    return pl.BlockSpec(shape, lambda *_: zeros)


def forward_stage(iterate, right_side, diffusivity, halos, lines):
    _, _, count, nz, ny = iterate.shape
    _, padded = half_rows(nz)
    block = block_of(count)
    blocks = count // block
    mixed, plain, along_y = forward_tables(nz, ny)
    tables = [*split_table(mixed), *split_table(plain), *split_table(along_y), *lines[:3]]
    plane = (1, NODES, 1, nz, ny)
    return pl.pallas_call(
        functools.partial(forward_kernel, padded=padded),
        grid=(blocks,),
        in_specs=[
            pl.BlockSpec((1, NODES, block, nz, ny), lambda b: (0, 0, b, 0, 0)),
            pl.BlockSpec(plane, lambda b: (0, 0, jnp.maximum(b * block - 1, 0), 0, 0)),
            pl.BlockSpec(plane, lambda b: (0, 0, jnp.minimum((b + 1) * block, count - 1), 0, 0)),
            full(plane),
            full(plane),
            pl.BlockSpec((1, NODES, block, nz, ny), lambda b: (0, 0, b, 0, 0)),
            pl.BlockSpec((block, nz, ny), lambda b: (b, 0, 0)),
            *[full(t.shape) for t in tables],
        ],
        out_specs=[
            pl.BlockSpec((block, NODES, 2, padded, ny), lambda b: (b, 0, 0, 0, 0)),
            pl.BlockSpec((block, 2, padded, ny), lambda b: (b, 0, 0, 0)),
            full((2, NODES, 2, padded, ny)),
        ],
        out_shape=[
            jax.ShapeDtypeStruct((count, NODES, 2, padded, ny), jnp.float32),
            jax.ShapeDtypeStruct((count, 2, padded, ny), jnp.float32),
            jax.ShapeDtypeStruct((2, NODES, 2, padded, ny), jnp.float32),
        ],
        scratch_shapes=[
            pltpu.VMEM((block + 2, NODES, nz, ny), jnp.float32),
            pltpu.VMEM((NODES, 2, padded, ny), jnp.float32),
        ],
        compiler_params=pltpu.CompilerParams(
            dimension_semantics=("arbitrary",), vmem_limit_bytes=60 * 1024 * 1024
        ),
    )(iterate, iterate, iterate, *halos, right_side, diffusivity, *tables)


def enter_back(state, states_ref, low_ref, close_ref):
    for m in range(NODES):
        value = c_mul((state[m, 0], state[m, 1]), (low_ref[m, 0], low_ref[m, 1]))
        value = c_add(value, (states_ref[1, m, 0], states_ref[1, m, 1]))
        value = c_mul(value, (close_ref[m, 0], close_ref[m, 1]))
        state[m, 0] = value[0]
        state[m, 1] = value[1]


def node_kernel(
    mask_ref, c_ref, plain_ref, states_ref, low_ref, high_ref, close_ref, out_ref, ahead, state, *, half
):
    phase = pl.program_id(0)
    step = pl.program_id(1)
    blocks = pl.num_programs(1)
    block, _, _, padded, ny = c_ref.shape
    _, vectors, _, _ = node_constants()
    last = [complex(v) for v in vectors[NODES - 1]]

    @pl.when((phase == 0) & (step == 0))
    def _():
        state[...] = states_ref[0]

    @pl.when((phase == 1) & (step == 0))
    def _():
        enter_back(state, states_ref, low_ref, close_ref)

    @pl.when(phase == 0)
    def _():
        def tile(t, carry):
            rows = pl.ds(t * 8, 8)
            for m in range(NODES):
                low = (low_ref[m, 0, rows], low_ref[m, 1, rows])
                value = (state[m, 0, rows], state[m, 1, rows])
                for j in range(block):
                    value = c_add(c_mul(value, low), (c_ref[j, m, 0, rows], c_ref[j, m, 1, rows]))
                    ahead[step * block + j, m, 0, rows] = value[0]
                    ahead[step * block + j, m, 1, rows] = value[1]
                state[m, 0, rows] = value[0]
                state[m, 1, rows] = value[1]
            return carry

        lax.fori_loop(0, padded // 8, tile, 0)

    @pl.when(phase == 1)
    def _():
        lane = lax.broadcasted_iota(jnp.int32, (GROUP, ny), 1)
        mask = mask_ref[0]

        def totals(start, base):
            rows = pl.ds(start, 8)
            first = (blocks - 1 - step) * block + base
            total = [
                [-mask * plain_ref[base + j, part, rows] for part in range(2)] for j in range(GROUP)
            ]
            for m in range(NODES):
                high = (high_ref[m, 0, rows], high_ref[m, 1, rows])
                value = (state[m, 0, rows], state[m, 1, rows])
                for j in reversed(range(GROUP)):
                    value = c_add(
                        c_mul(value, high), (ahead[first + j, m, 0, rows], ahead[first + j, m, 1, rows])
                    )
                    total[j][0] += last[m].real * value[0] - last[m].imag * value[1]
                    total[j][1] += last[m].real * value[1] + last[m].imag * value[0]
                state[m, 0, rows] = value[0]
                state[m, 1, rows] = value[1]
            return [
                jnp.swapaxes(jnp.stack([total[j][part] for j in range(GROUP)]), 0, 1)
                for part in range(2)
            ]

        for base in reversed(range(0, block, GROUP)):
            edge = [value[0] for value in totals(half, base)]
            top = totals(0, base)
            turned = [pltpu.roll(value, ny // 2, 1) for value in edge]
            folded = [jnp.where(lane <= ny // 2, top[part][0], turned[part]) for part in range(2)]
            folded[1] = jnp.where(lane % (ny // 2) == 0, edge[0], folded[1])
            for part in range(2):
                out_ref[0, part, base : base + GROUP] = folded[part]
                out_ref[1:8, part, base : base + GROUP] = top[part][1:]

            def tile(t, carry):
                start = pl.multiple_of(t * 8, 8)
                value = totals(start, base)
                for part in range(2):
                    out_ref[pl.ds(start, 8), part, base : base + GROUP] = value[part]
                return carry

            lax.fori_loop(1, half // 8, tile, 0)


def node_stage(c, plain, mask, states, lines, nz):
    count, _, _, padded, ny = c.shape
    block = block_of(count)
    blocks = count // block
    half = nz // 2

    def early(phase, b):
        return jnp.where(phase == 0, b, blocks - 1)

    def late(phase, b):
        return jnp.where(phase == 0, blocks - 1, blocks - 1 - b)

    tables = [lines[0], lines[1], lines[4]]
    return pl.pallas_call(
        functools.partial(node_kernel, half=half),
        grid=(2, blocks),
        in_specs=[
            pl.BlockSpec(memory_space=pltpu.SMEM),
            pl.BlockSpec((block, NODES, 2, padded, ny), lambda a, b: (early(a, b), 0, 0, 0, 0)),
            pl.BlockSpec((block, 2, padded, ny), lambda a, b: (late(a, b), 0, 0, 0)),
            full(states.shape),
            *[full(t.shape) for t in tables],
        ],
        out_specs=pl.BlockSpec((half, 2, block, ny), lambda a, b: (0, 0, late(a, b), 0)),
        out_shape=jax.ShapeDtypeStruct((half, 2, count, ny), jnp.float32),
        scratch_shapes=[
            pltpu.VMEM((count, NODES, 2, padded, ny), jnp.float32),
            pltpu.VMEM((NODES, 2, padded, ny), jnp.float32),
        ],
        compiler_params=pltpu.CompilerParams(
            dimension_semantics=("arbitrary", "arbitrary"), vmem_limit_bytes=60 * 1024 * 1024
        ),
    )(mask, c, plain, states, *tables)


def couple_kernel(q_ref, th_ref, tl_ref, ih_ref, il_ref, grow_ref, close_ref, out_ref, work):
    steps, slabs, _, count, width = q_ref.shape
    nx = slabs * count
    joined = width % 128 == 0

    def side_by_side(table_high, table_low, values):
        if not joined:
            return [dot3_table_left(table_high, table_low, value) for value in values]
        wide = dot3_table_left(table_high, table_low, jnp.concatenate(values, axis=1))
        return [wide[:, i * width : (i + 1) * width] for i in range(len(values))]

    def ahead(s, carry):
        lines = [
            jnp.concatenate([q_ref[s, p, part] for p in range(slabs)], axis=0) for part in range(2)
        ]
        for part, waves in enumerate(side_by_side(th_ref[...], tl_ref[...], lines)):
            work[s, part, 0] = waves[:nx]
            work[s, part, 1] = waves[nx:]
        return carry

    unrolled(steps, ahead)

    def tile(t, carry):
        rows = pl.ds(t * 8, 8)
        for part in range(2):
            grow = (grow_ref[part, 0, rows], grow_ref[part, 1, rows])
            values = [(work[s, part, 0, rows], work[s, part, 1, rows]) for s in range(steps)]
            value = values[0]
            for s in range(1, steps):
                value = c_add(c_mul(grow, value), values[s])
            value = c_mul(value, (close_ref[part, 0, rows], close_ref[part, 1, rows]))
            for s in range(steps):
                work[s, part, 0, rows] = value[0]
                work[s, part, 1, rows] = value[1]
                if s + 1 < steps:
                    value = c_add(c_mul(grow, value), values[s])
        return carry

    lax.fori_loop(0, nx // 8, tile, 0)

    def back(i, carry):
        pair = [2 * i, 2 * i + 1]
        lines = [
            jnp.concatenate(
                [work[s, 0, 0] - work[s, 1, 1], work[s, 0, 1] + work[s, 1, 0]], axis=0
            )
            for s in pair
        ]
        for s, value in zip(pair, side_by_side(ih_ref[...], il_ref[...], lines)):
            for part in range(2):
                for p in range(slabs):
                    base = part * nx + p * count
                    out_ref[s, p, part] = value[base : base + count]
        return carry

    unrolled(steps // 2, back)


def couple_stage(q, velocity, first_mode, nz, ny):
    steps, slabs, _, count, width = q.shape
    nx = slabs * count
    forward, backward = x_tables(nx)
    values, vectors, _, weights = node_constants()
    mode = first_mode + jnp.arange(width, dtype=jnp.int32)
    row, lane = mode // ny, mode % ny
    edge = row == 0
    corner = edge & (lane % (ny // 2) == 0)
    wave_z = jnp.where(edge & (lane > ny // 2), nz // 2, row)
    wave_y = jnp.where(edge & (lane > ny // 2), lane - ny // 2, lane)
    wave_z = jnp.stack([wave_z, jnp.where(corner, nz // 2, wave_z)])[:, None, :]
    theta_z = wave_z.astype(jnp.float32) * (2.0 * math.pi / nz)
    theta_y = wave_y.astype(jnp.float32)[None, None, :] * (2.0 * math.pi / ny)
    theta_x = jnp.arange(nx, dtype=jnp.int32).astype(jnp.float32)[None, :, None] * (2.0 * math.pi / nx)
    real = diffusion_number * (
        (2.0 * jnp.cos(theta_x) - 2.0)
        + (2.0 * jnp.cos(theta_z) - 2.0)
        + (2.0 * jnp.cos(theta_y) - 2.0)
    )
    imag = -(
        velocity[0] * jnp.sin(theta_x)
        + velocity[1] * jnp.sin(theta_y)
        + velocity[2] * jnp.sin(theta_z)
    )
    grow = None
    for m in range(NODES):
        mu = complex(values[m])
        below = (1.0 - (mu.real * real - mu.imag * imag), -(mu.real * imag + mu.imag * real))
        above = complex(vectors[NODES - 1, m] * weights[m])
        added = c_div((above.real, above.imag), below)
        grow = added if grow is None else (grow[0] + added[0], grow[1] + added[1])
    whole = c_power(grow, steps)
    close = c_div(
        (circulant_alpha, 0.0), (1.0 - circulant_alpha * whole[0], -circulant_alpha * whole[1])
    )
    return pl.pallas_call(
        couple_kernel,
        out_shape=jax.ShapeDtypeStruct(q.shape, jnp.float32),
        scratch_shapes=[pltpu.VMEM((steps, 2, 2, nx, width), jnp.float32)],
        compiler_params=pltpu.CompilerParams(vmem_limit_bytes=60 * 1024 * 1024),
    )(
        q,
        *split_table(forward),
        *split_table(backward),
        jnp.stack(grow, axis=1),
        jnp.stack(close, axis=1),
    )


def edge_kernel(b_ref, low_ref, high_ref, beta_ref, wide_ref, out_ref):
    half, _, count, ny = b_ref.shape
    padded = wide_ref.shape[2]
    lane = lax.broadcasted_iota(jnp.int32, (GROUP, ny), 1)
    inside = lane % (ny // 2) != 0
    kept = jnp.where(inside, jnp.where(lane < ny // 2, 2.0, 0.0), 1.0)
    zero = jnp.zeros((GROUP, ny), jnp.float32)

    def unfold(g, carry):
        base = pl.multiple_of(g * GROUP, GROUP)
        planes = pl.ds(base, GROUP)
        top = [b_ref[0, part, planes] for part in range(2)]
        turned = [pltpu.roll(value, ny // 2, 1) for value in top]
        first = (top[0], jnp.where(inside, top[1], 0.0))
        edge = (jnp.where(inside, turned[0], top[1]), jnp.where(inside, turned[1], 0.0))
        for part in range(2):
            for start in range(0, half, 8):
                rows = [b_ref[start + r, part, planes] for r in range(8)]
                if start == 0:
                    rows[0] = first[part] * kept
                wide_ref[planes, part, start : start + 8] = jnp.swapaxes(jnp.stack(rows), 0, 1)
            rows = [edge[part] * kept] + [zero] * 7
            wide_ref[planes, part, half : half + 8] = jnp.swapaxes(jnp.stack(rows), 0, 1)
        return carry

    lax.fori_loop(0, count // GROUP, unfold, 0)

    def tile(t, carry):
        rows = pl.ds(pl.multiple_of(t * 8, 8), 8)
        for side, table in enumerate((low_ref, high_ref)):
            decay = [(table[m, 0, rows], table[m, 1, rows]) for m in range(NODES)]

            def group(g, values):
                for i in range(GROUP):
                    j = g * GROUP + i
                    j = j if side == 0 else count - 1 - j
                    plane = (wide_ref[j, 0, rows], wide_ref[j, 1, rows])
                    values = [c_add(c_mul(v, d), plane) for v, d in zip(values, decay)]
                return values

            values = lax.fori_loop(0, count // GROUP, group, [(zero, zero)] * NODES)
            for m in range(NODES):
                value = c_mul(values[m], (beta_ref[m, 0, rows], beta_ref[m, 1, rows]))
                out_ref[side, m, 0, rows] = value[0]
                out_ref[side, m, 1, rows] = value[1]
        return carry

    lax.fori_loop(0, padded // 8, tile, 0)


def edge_stage(b, lines):
    count = b.shape[2]
    padded, ny = lines[0].shape[2:]
    return pl.pallas_call(
        edge_kernel,
        out_shape=[
            jax.ShapeDtypeStruct((count, 2, padded, ny), jnp.float32),
            jax.ShapeDtypeStruct((2, NODES, 2, padded, ny), jnp.float32),
        ],
        compiler_params=pltpu.CompilerParams(vmem_limit_bytes=60 * 1024 * 1024),
    )(b, lines[0], lines[1], lines[3])


def inverse_kernel(
    c_ref,
    b_ref,
    states_ref,
    low_ref,
    high_ref,
    beta_ref,
    close_ref,
    yh_ref,
    yl_ref,
    zh_ref,
    zl_ref,
    out_ref,
    ahead,
    state,
):
    phase = pl.program_id(0)
    step = pl.program_id(1)
    blocks = pl.num_programs(1)
    block, _, _, padded, ny = c_ref.shape
    nz = out_ref.shape[3]

    @pl.when((phase == 0) & (step == 0))
    def _():
        state[...] = states_ref[0]

    @pl.when((phase == 1) & (step == 0))
    def _():
        enter_back(state, states_ref, low_ref, close_ref)

    @pl.when(phase == 0)
    def _():
        def tile(t, carry):
            rows = pl.ds(pl.multiple_of(t * 8, 8), 8)
            for base in range(0, block, GROUP):
                planes = [
                    (b_ref[base + j, 0, rows], b_ref[base + j, 1, rows]) for j in range(GROUP)
                ]
                for m in range(NODES):
                    low = (low_ref[m, 0, rows], low_ref[m, 1, rows])
                    beta = (beta_ref[m, 0, rows], beta_ref[m, 1, rows])
                    value = (state[m, 0, rows], state[m, 1, rows])
                    for j in range(GROUP):
                        source = c_add(
                            c_mul(planes[j], beta),
                            (c_ref[base + j, m, 0, rows], c_ref[base + j, m, 1, rows]),
                        )
                        value = c_add(c_mul(value, low), source)
                        ahead[step * block + base + j, m, 0, rows] = value[0]
                        ahead[step * block + base + j, m, 1, rows] = value[1]
                    state[m, 0, rows] = value[0]
                    state[m, 1, rows] = value[1]
            return carry

        lax.fori_loop(0, padded // 8, tile, 0)

    @pl.when(phase == 1)
    def _():
        first = (blocks - 1 - step) * block

        def tile(t, carry):
            rows = pl.ds(pl.multiple_of(t * 8, 8), 8)
            for m in range(NODES):
                high = (high_ref[m, 0, rows], high_ref[m, 1, rows])
                value = (state[m, 0, rows], state[m, 1, rows])
                for j in reversed(range(block)):
                    value = c_add(
                        c_mul(value, high), (ahead[first + j, m, 0, rows], ahead[first + j, m, 1, rows])
                    )
                    ahead[first + j, m, 0, rows] = value[0]
                    ahead[first + j, m, 1, rows] = value[1]
                state[m, 0, rows] = value[0]
                state[m, 1, rows] = value[1]
            return carry

        lax.fori_loop(0, padded // 8, tile, 0)

        def pair(i, carry):
            rows = []
            for half in range(2):
                row = first + 2 * i + half
                for m in range(NODES):
                    rows.append(jnp.concatenate([ahead[row, m, 0], ahead[row, m, 1]], axis=1))
            lines = dot3_table_right(jnp.concatenate(rows, axis=0), yh_ref[...], yl_ref[...])
            columns = []
            for half in range(2):
                stacked = []
                for m in range(NODES):
                    base = (half * NODES + m) * padded
                    stacked.append(lines[base : base + padded, :ny])
                    stacked.append(lines[base : base + padded, ny:])
                columns.append(jnp.concatenate(stacked, axis=0))
            grid = dot3_table_left(zh_ref[...], zl_ref[...], jnp.concatenate(columns, axis=1))
            for half in range(2):
                for n in range(NODES):
                    out_ref[0, n, 2 * i + half] = grid[
                        n * nz : (n + 1) * nz, half * ny : (half + 1) * ny
                    ]
            return carry

        unrolled(block // 2, pair)


def inverse_stage(c, b, states, lines, nz):
    count, _, _, padded, ny = c.shape
    block = block_of(count)
    blocks = count // block
    mixed, along_y = inverse_tables(nz, ny)
    tables = [lines[0], lines[1], lines[3], lines[4], *split_table(along_y), *split_table(mixed)]

    def early(phase, b):
        return jnp.where(phase == 0, b, blocks - 1)

    def late(phase, b):
        return jnp.where(phase == 0, blocks - 1, blocks - 1 - b)

    return pl.pallas_call(
        inverse_kernel,
        grid=(2, blocks),
        in_specs=[
            pl.BlockSpec((block, NODES, 2, padded, ny), lambda a, b: (early(a, b), 0, 0, 0, 0)),
            pl.BlockSpec((block, 2, padded, ny), lambda a, b: (early(a, b), 0, 0, 0)),
            full(states.shape),
            *[full(t.shape) for t in tables],
        ],
        out_specs=pl.BlockSpec((1, NODES, block, nz, ny), lambda a, b: (0, 0, late(a, b), 0, 0)),
        out_shape=jax.ShapeDtypeStruct((1, NODES, count, nz, ny), jnp.float32),
        scratch_shapes=[
            pltpu.VMEM((count, NODES, 2, padded, ny), jnp.float32),
            pltpu.VMEM((NODES, 2, padded, ny), jnp.float32),
        ],
        compiler_params=pltpu.CompilerParams(
            dimension_semantics=("arbitrary", "arbitrary"), vmem_limit_bytes=60 * 1024 * 1024
        ),
    )(c, b, states, *tables)


def ring_states(ends, lines, count, slabs):
    decay = jnp.stack([lines[0], lines[1]])
    decay = c_power((decay[:, :, 0], decay[:, :, 1]), count)
    total = None
    for distance in range(slabs, 0, -1):
        if distance == slabs:
            moved = ends
        elif 2 * distance == slabs:
            moved = lax.ppermute(ends, "space", [(i, (i + distance) % slabs) for i in range(slabs)])
        else:
            moved = jnp.stack(
                [
                    lax.ppermute(
                        ends[side], "space", [(i, (i + shift) % slabs) for i in range(slabs)]
                    )
                    for side, shift in enumerate((distance, -distance))
                ]
            )
        moved = (moved[:, :, 0], moved[:, :, 1])
        total = moved if total is None else c_add(c_mul(total, decay), moved)
    whole = c_power(decay, slabs)
    total = c_div(total, (1.0 - whole[0], -whole[1]))
    return jnp.stack(total, axis=2)


def to_modes(q, devices):
    half, _, count, ny = q.shape
    pieces = devices // half
    if pieces > 1:
        q = q.reshape(half, 2 * count, pieces, ny // pieces)
        q = jnp.transpose(q, (0, 2, 1, 3))
    return q.reshape(devices, 2 * count, ny // pieces)


def from_modes(b, half):
    devices, lines, width = b.shape
    pieces = devices // half
    if pieces > 1:
        b = jnp.transpose(b.reshape(half, pieces, lines, width), (0, 2, 1, 3))
    return b.reshape(half, 2, lines // 2, pieces * width)


def shards(iterate, right_side, diffusivity, velocity):
    steps, slabs = lax.axis_size("tm"), lax.axis_size("space")
    devices = steps * slabs
    _, _, count, nz, ny = iterate.shape
    up = [(i, (i + 1) % slabs) for i in range(slabs)]
    down = [(target, source) for source, target in up]
    halos = (
        lax.ppermute(iterate[:, :, count - 1 :], "space", up),
        lax.ppermute(iterate[:, :, :1], "space", down),
    )
    lines = line_tables(velocity, nz, ny)
    c, plain, ends = forward_stage(iterate, right_side, diffusivity, halos, lines)
    states = ring_states(ends, lines, count, slabs)
    step = lax.axis_index("tm")
    mask = jnp.where(step == steps - 1, 1.0, 0.0).astype(jnp.float32)[None]
    q = node_stage(c, plain, mask, states, lines, nz)
    q = lax.all_to_all(to_modes(q, devices), ("tm", "space"), 0, 0, tiled=True)
    width = q.shape[2]
    first_mode = (step * slabs + lax.axis_index("space")) * width
    b = couple_stage(q.reshape(steps, slabs, 2, count, width), velocity, first_mode, nz, ny)
    b = lax.all_to_all(b.reshape(devices, 2 * count, width), ("tm", "space"), 0, 0, tiled=True)
    b, ends = edge_stage(from_modes(b, nz // 2), lines)
    states = states + ring_states(ends, lines, count, slabs)
    return inverse_stage(c, b, states, lines, nz)


def solution(mesh):
    placed = (
        P("tm", None, "space", None, None),
        P("tm", None, "space", None, None),
        P("space", None, None),
        P(),
    )
    return jax.shard_map(
        shards,
        mesh=mesh,
        in_specs=placed,
        out_specs=P("tm", None, "space", None, None),
        check_vma=False,
    )
```

```python
import functools
import math

import jax
import jax.numpy as jnp
import numpy as np
from jax import lax
from jax.experimental import pallas as pl
from jax.experimental.pallas import tpu as pltpu
from jax.sharding import PartitionSpec as P

diffusion_number = 16.0
circulant_alpha = 0.1
NODES = 4
GROUP = 8


def collocation_matrix():
    radau_nodes = [0.08858795951270394, 0.4094668644407347, 0.7876594617608471, 1.0]
    matrix = [[0.0] * 4 for row_index in range(4)]
    for column_index in range(4):
        coefficients = [1.0]
        for other_index in range(4):
            if other_index != column_index:
                scale_value = 1.0 / (radau_nodes[column_index] - radau_nodes[other_index])
                shifted = [0.0] + [value * scale_value for value in coefficients]
                lowered = [
                    -radau_nodes[other_index] * scale_value * value for value in coefficients
                ] + [0.0]
                coefficients = [
                    left_value + right_value for left_value, right_value in zip(shifted, lowered)
                ]
        for row_index in range(4):
            total = 0.0
            for power_index in range(len(coefficients)):
                total = total + coefficients[power_index] * radau_nodes[row_index] ** (
                    power_index + 1
                ) / (power_index + 1)
            matrix[row_index][column_index] = total
    return matrix


def solve_system(matrix, target):
    count = len(target)
    rows_list = [list(matrix[row_index]) + [target[row_index]] for row_index in range(count)]
    for column in range(count):
        best_row = column
        for candidate in range(column + 1, count):
            if abs(rows_list[candidate][column]) > abs(rows_list[best_row][column]):
                best_row = candidate
        saved_row = rows_list[column]
        rows_list[column] = rows_list[best_row]
        rows_list[best_row] = saved_row
        leader = rows_list[column][column]
        for other_row in range(count):
            if other_row != column:
                factor = rows_list[other_row][column] / leader
                rows_list[other_row] = [
                    left_value - factor * right_value
                    for left_value, right_value in zip(rows_list[other_row], rows_list[column])
                ]
    return [
        rows_list[row_index][count] / rows_list[row_index][row_index] for row_index in range(count)
    ]


def node_basis():
    matrix = collocation_matrix()
    helper = [[0.0] * 4 for row_index in range(4)]
    coefficients = [0.0, 0.0, 0.0, 0.0, 1.0]
    for order in range(1, 5):
        product = [
            [
                sum((matrix[row_index][inner] * helper[inner][column] for inner in range(4)))
                for column in range(4)
            ]
            for row_index in range(4)
        ]
        for row_index in range(4):
            product[row_index][row_index] = product[row_index][row_index] + coefficients[5 - order]
        helper = product
        trace_value = sum(
            (
                sum((matrix[row_index][inner] * helper[inner][row_index] for inner in range(4)))
                for row_index in range(4)
            )
        )
        coefficients[4 - order] = -trace_value / order
    roots_list = [(0.4 + 0.9j) ** power_index for power_index in range(4)]
    for sweep in range(400):
        for root_index in range(4):
            current = roots_list[root_index]
            numer = 0.0
            for power_index in range(4, -1, -1):
                numer = numer * current + coefficients[power_index]
            denom = 1.0
            for other_index in range(4):
                if other_index != root_index:
                    denom = denom * (current - roots_list[other_index])
            roots_list[root_index] = current - numer / denom
    vectors = [[0.0] * 4 for row_index in range(4)]
    for root_index in range(4):
        shifted = [
            [
                matrix[row_index][column] - (roots_list[root_index] if row_index == column else 0.0)
                for column in range(3)
            ]
            for row_index in range(3)
        ]
        target = [-matrix[row_index][3] for row_index in range(3)]
        parts = solve_system(shifted, target) + [1.0 + 0j]
        for row_index in range(4):
            vectors[row_index][root_index] = parts[row_index]
    inverse = [[0.0] * 4 for row_index in range(4)]
    for column in range(4):
        unit = [1.0 if row_index == column else 0.0 for row_index in range(4)]
        parts = solve_system(vectors, unit)
        for row_index in range(4):
            inverse[row_index][column] = parts[row_index]
    weights = [sum((inverse[row_index][column] for column in range(4))) for row_index in range(4)]
    return (roots_list, vectors, inverse, weights)


def split_table(table):
    table = jnp.asarray(np.asarray(table, np.float32))
    high = table.astype(jnp.bfloat16)
    return high, (table - high.astype(jnp.float32)).astype(jnp.bfloat16)


def split(values):
    high = values.astype(jnp.bfloat16)
    return high, (values - high.astype(jnp.float32)).astype(jnp.bfloat16)


def dot(left, right):
    return jnp.dot(left, right, preferred_element_type=jnp.float32)


def dot3_table_left(table_high, table_low, values):
    high, low = split(values)
    return dot(table_high, high) + (dot(table_high, low) + dot(table_low, high))


def dot3_table_right(values, table_high, table_low):
    high, low = split(values)
    return dot(high, table_high) + (dot(low, table_high) + dot(high, table_low))


def node_constants():
    values, vectors, inverse, weights = node_basis()
    return (
        np.array([complex(v) for v in values]),
        np.array([[complex(v) for v in row] for row in vectors]),
        np.array([[complex(v) for v in row] for row in inverse]),
        np.array([complex(v) for v in weights]),
    )


def half_rows(nz):
    kept = nz // 2 + 1
    return kept, -(-kept // 8) * 8


def forward_tables(nz, ny):
    _, _, inverse, _ = node_constants()
    kept, padded = half_rows(nz)
    wave = np.zeros((padded, nz), complex)
    wave[:kept] = np.exp(-2j * math.pi * np.outer(np.arange(kept), np.arange(nz)) / nz)
    mixed = np.zeros((NODES, 2, padded, NODES, nz))
    for m in range(NODES):
        for n in range(NODES):
            mixed[m, 0, :, n] = (inverse[m, n] * wave).real
            mixed[m, 1, :, n] = (inverse[m, n] * wave).imag
    plain = np.concatenate([wave.real, wave.imag], axis=0)
    angle = 2 * math.pi * (np.outer(np.arange(ny), np.arange(ny)) % ny) / ny
    c, s = np.cos(angle), np.sin(angle)
    along_y = np.block([[c, -s], [s, c]])
    return mixed.reshape(NODES * 2 * padded, NODES * nz), plain, along_y


def inverse_tables(nz, ny):
    _, vectors, _, _ = node_constants()
    kept, padded = half_rows(nz)
    weight = np.where((np.arange(kept) == 0) | (2 * np.arange(kept) == nz), 1.0, 2.0)
    wave = np.zeros((nz, padded), complex)
    wave[:, :kept] = np.exp(2j * math.pi * np.outer(np.arange(nz), np.arange(kept)) / nz) * weight / nz
    mixed = np.zeros((NODES, nz, NODES, 2, padded))
    for n in range(NODES):
        for m in range(NODES):
            mixed[n, :, m, 0] = (vectors[n, m] * wave).real
            mixed[n, :, m, 1] = -(vectors[n, m] * wave).imag
    angle = 2 * math.pi * (np.outer(np.arange(ny), np.arange(ny)) % ny) / ny
    c, s = np.cos(angle) / ny, np.sin(angle) / ny
    along_y = np.block([[c, s], [-s, c]])
    return mixed.reshape(NODES * nz, NODES * 2 * padded), along_y


def x_tables(nx):
    angle = 2 * math.pi * (np.outer(np.arange(nx), np.arange(nx)) % nx) / nx
    c, s = np.cos(angle), np.sin(angle)
    return np.concatenate([c, -s], axis=0), np.block([[c, -s], [s, c]]) / nx


def c_mul(a, b):
    return a[0] * b[0] - a[1] * b[1], a[0] * b[1] + a[1] * b[0]


def c_add(a, b):
    return a[0] + b[0], a[1] + b[1]


def c_div(a, b):
    size = b[0] * b[0] + b[1] * b[1]
    return (a[0] * b[0] + a[1] * b[1]) / size, (a[1] * b[0] - a[0] * b[1]) / size


def c_power(a, count):
    result = None
    while count:
        if count & 1:
            result = a if result is None else c_mul(result, a)
        count >>= 1
        if count:
            a = c_mul(a, a)
    return result


def c_sqrt(a):
    size = jnp.sqrt(a[0] * a[0] + a[1] * a[1])
    large = jnp.sqrt(0.5 * (size + jnp.abs(a[0])))
    small = a[1] / (2.0 * large)
    flip = a[0] < 0.0
    return (
        jnp.where(flip, jnp.abs(small), large),
        jnp.where(flip, jnp.where(a[1] < 0.0, -large, large), small),
    )


def line_kernel(velocity_ref, real_ref, sin_z_ref, sin_y_ref, *out_refs, count, slabs):
    values, _, _, weights = node_constants()
    real = real_ref[...] - 2.0 * diffusion_number
    imag = -(velocity_ref[1] * sin_y_ref[...] + velocity_ref[2] * sin_z_ref[...])
    one, zero = jnp.ones_like(real), jnp.zeros_like(real)
    from_low = diffusion_number + 0.5 * velocity_ref[0]
    from_high = diffusion_number - 0.5 * velocity_ref[0]
    product = 4.0 * from_low * from_high
    for m in range(NODES):
        mu = complex(values[m])
        mu2 = mu * mu
        diagonal = (1.0 - (mu.real * real - mu.imag * imag), -(mu.real * imag + mu.imag * real))
        square = c_mul(diagonal, diagonal)
        root = c_sqrt((square[0] - product * mu2.real, square[1] - product * mu2.imag))
        turn = diagonal[0] * root[0] + diagonal[1] * root[1] < 0.0
        root = (jnp.where(turn, -root[0], root[0]), jnp.where(turn, -root[1], root[1]))
        kappa = (0.5 * (diagonal[0] + root[0]), 0.5 * (diagonal[1] + root[1]))
        gain = c_div((one, zero), kappa)
        ratio = (mu.real * gain[0] - mu.imag * gain[1], mu.real * gain[1] + mu.imag * gain[0])
        weight = complex(weights[m])
        beta = (
            weight.real * gain[0] - weight.imag * gain[1],
            weight.real * gain[1] + weight.imag * gain[0],
        )
        sides = [(factor * ratio[0], factor * ratio[1]) for factor in (from_low, from_high)]
        tables = [*sides, gain, beta, c_div(kappa, root)]
        for table, out_ref in zip(tables, out_refs):
            out_ref[m, 0] = table[0]
            out_ref[m, 1] = table[1]
        for side in range(2):
            decay = c_power(sides[side], count)
            whole = c_power(decay, slabs)
            around = c_div((one, zero), (1.0 - whole[0], -whole[1]))
            for part in range(2):
                out_refs[5][side, m, part] = decay[part]
                out_refs[6][side, m, part] = around[part]


def line_tables(velocity, nz, ny, count, slabs):
    _, padded = half_rows(nz)
    theta_z = 2 * math.pi * np.arange(padded)[:, None] / nz
    theta_y = 2 * math.pi * np.arange(ny)[None, :] / ny
    real = diffusion_number * ((2 * np.cos(theta_z) - 2) + (2 * np.cos(theta_y) - 2))
    waves = [real, np.sin(theta_z) + 0 * theta_y, np.sin(theta_y) + 0 * theta_z]
    one = jax.ShapeDtypeStruct((NODES, 2, padded, ny), jnp.float32)
    two = jax.ShapeDtypeStruct((2, NODES, 2, padded, ny), jnp.float32)
    return pl.pallas_call(
        functools.partial(line_kernel, count=count, slabs=slabs),
        in_specs=[
            pl.BlockSpec(memory_space=pltpu.SMEM),
            *[pl.BlockSpec(memory_space=pltpu.VMEM)] * 3,
        ],
        out_shape=[one] * 5 + [two] * 2,
    )(velocity, *[jnp.asarray(wave, jnp.float32) for wave in waves])


def block_of(count):
    return 16 if count % 16 == 0 else GROUP


def unrolled(count, body, most=8):
    each = math.gcd(count, most)

    def turn(i, carry):
        for k in range(each):
            body(i * each + k, carry)
        return carry

    lax.fori_loop(0, count // each, turn, 0)


def forward_kernel(
    block_ref,
    prev_ref,
    next_ref,
    halo_ref,
    right_ref,
    diffusivity_ref,
    zh_ref,
    zl_ref,
    yh_ref,
    yl_ref,
    low_ref,
    high_ref,
    gain_ref,
    out_ref,
    ends_ref,
    planes,
    power,
    *,
    padded,
):
    step = pl.program_id(0)
    steps = pl.num_programs(0)
    block, nz, ny = block_ref.shape[2:]
    matrix = collocation_matrix()

    @pl.when(step == 0)
    def _():
        ends_ref[...] = jnp.zeros_like(ends_ref)
        planes[0] = halo_ref[0]
        for m in range(NODES):
            power[m, 0] = jnp.ones_like(power[m, 0])
            power[m, 1] = jnp.zeros_like(power[m, 1])

    @pl.when(step > 0)
    def _():
        planes[0] = prev_ref[0, :, 0]

    @pl.when(step == steps - 1)
    def _():
        planes[block + 1] = halo_ref[1]

    @pl.when(step < steps - 1)
    def _():
        planes[block + 1] = next_ref[0, :, 0]

    for j in range(block):
        planes[j + 1] = block_ref[0, :, j]

    def pair(index, carry):
        columns = []
        for half in range(2):
            j = 2 * index + half
            factor = diffusion_number * (diffusivity_ref[j] - 1.0)
            spread = []
            for n in range(NODES):
                f = planes[j + 1, n]
                lap = (
                    (planes[j, n] + planes[j + 2, n])
                    + (pltpu.roll(f, 1, 0) + pltpu.roll(f, nz - 1, 0))
                    + (pltpu.roll(f, 1, 1) + pltpu.roll(f, ny - 1, 1))
                    - 6.0 * f
                )
                spread.append(factor * lap)
            mixed = []
            for m in range(NODES):
                total = right_ref[0, m, j]
                for n in range(NODES):
                    total = total + matrix[m][n] * spread[n]
                mixed.append(total)
            columns.append(jnp.concatenate(mixed, axis=0))
        spectrum_z = dot3_table_left(zh_ref[...], zl_ref[...], jnp.concatenate(columns, axis=1))
        rows = []
        for half in range(2):
            lanes = slice(half * ny, (half + 1) * ny)
            for m in range(NODES):
                base = 2 * m * padded
                rows.append(
                    jnp.concatenate(
                        [
                            spectrum_z[base : base + padded, lanes],
                            spectrum_z[base + padded : base + 2 * padded, lanes],
                        ],
                        axis=1,
                    )
                )
        spectrum = dot3_table_right(jnp.concatenate(rows, axis=0), yh_ref[...], yl_ref[...])
        for half in range(2):
            j = 2 * index + half
            for m in range(NODES):
                base = (half * NODES + m) * padded
                value = (spectrum[base : base + padded, :ny], spectrum[base : base + padded, ny:])
                value = c_mul(value, (gain_ref[m, 0], gain_ref[m, 1]))
                out_ref[j, m, 0] = value[0]
                out_ref[j, m, 1] = value[1]
        return carry

    unrolled(block // 2, pair)

    def tile(t, carry):
        rows = pl.ds(pl.multiple_of(t * 8, 8), 8)
        nodes = range(NODES)
        low = [(low_ref[m, 0, rows], low_ref[m, 1, rows]) for m in nodes]
        high = [(high_ref[m, 0, rows], high_ref[m, 1, rows]) for m in nodes]
        ahead = [(ends_ref[0, m, 0, rows], ends_ref[0, m, 1, rows]) for m in nodes]
        back = [(out_ref[block - 1, m, 0, rows], out_ref[block - 1, m, 1, rows]) for m in nodes]
        for j in range(block):
            k = block - 1 - j
            for m in nodes:
                value = (out_ref[j, m, 0, rows], out_ref[j, m, 1, rows])
                ahead[m] = c_add(c_mul(ahead[m], low[m]), value)
                if j:
                    value = (out_ref[k, m, 0, rows], out_ref[k, m, 1, rows])
                    back[m] = c_add(c_mul(back[m], high[m]), value)
        for m in nodes:
            scale = (power[m, 0, rows], power[m, 1, rows])
            added = c_mul(scale, back[m])
            scale = c_mul(scale, c_power(high[m], block))
            for part in range(2):
                ends_ref[0, m, part, rows] = ahead[m][part]
                ends_ref[1, m, part, rows] = ends_ref[1, m, part, rows] + added[part]
                power[m, part, rows] = scale[part]
        return carry

    lax.fori_loop(0, padded // 8, tile, 0)


def full(shape):
    zeros = (0,) * len(shape)
    return pl.BlockSpec(shape, lambda *_: zeros)


def forward_stage(iterate, right_side, diffusivity, halo, lines):
    _, _, count, nz, ny = iterate.shape
    _, padded = half_rows(nz)
    block = block_of(count)
    blocks = count // block
    mixed, _, along_y = forward_tables(nz, ny)
    tables = [*split_table(mixed), *split_table(along_y), *lines[:3]]
    plane = (1, NODES, 1, nz, ny)
    return pl.pallas_call(
        functools.partial(forward_kernel, padded=padded),
        grid=(blocks,),
        in_specs=[
            pl.BlockSpec((1, NODES, block, nz, ny), lambda b: (0, 0, b, 0, 0)),
            pl.BlockSpec(plane, lambda b: (0, 0, jnp.maximum(b * block - 1, 0), 0, 0)),
            pl.BlockSpec(plane, lambda b: (0, 0, jnp.minimum((b + 1) * block, count - 1), 0, 0)),
            full(halo.shape),
            pl.BlockSpec((1, NODES, block, nz, ny), lambda b: (0, 0, b, 0, 0)),
            pl.BlockSpec((block, nz, ny), lambda b: (b, 0, 0)),
            *[full(t.shape) for t in tables],
        ],
        out_specs=[
            pl.BlockSpec((block, NODES, 2, padded, ny), lambda b: (b, 0, 0, 0, 0)),
            full((2, NODES, 2, padded, ny)),
        ],
        out_shape=[
            jax.ShapeDtypeStruct((count, NODES, 2, padded, ny), jnp.float32),
            jax.ShapeDtypeStruct((2, NODES, 2, padded, ny), jnp.float32),
        ],
        scratch_shapes=[
            pltpu.VMEM((block + 2, NODES, nz, ny), jnp.float32),
            pltpu.VMEM((NODES, 2, padded, ny), jnp.float32),
        ],
        compiler_params=pltpu.CompilerParams(
            dimension_semantics=("arbitrary",), vmem_limit_bytes=60 * 1024 * 1024
        ),
    )(iterate, iterate, iterate, halo, right_side, diffusivity, *tables)


def plain_kernel(field_ref, after_ref, zh_ref, zl_ref, yh_ref, yl_ref, out_ref):
    del after_ref
    block, nz, ny = field_ref.shape[2:]
    padded = out_ref.shape[2]

    def pair(index, carry):
        planes = [field_ref[0, 0, 2 * index + half] for half in range(2)]
        waves = dot3_table_left(zh_ref[...], zl_ref[...], jnp.concatenate(planes, axis=1))
        rows = []
        for half in range(2):
            lanes = slice(half * ny, (half + 1) * ny)
            rows.append(jnp.concatenate([waves[:padded, lanes], waves[padded:, lanes]], axis=1))
        spectrum = dot3_table_right(jnp.concatenate(rows, axis=0), yh_ref[...], yl_ref[...])
        for half in range(2):
            for part in range(2):
                out_ref[2 * index + half, part] = spectrum[
                    half * padded : (half + 1) * padded, part * ny : (part + 1) * ny
                ]
        return carry

    unrolled(block // 2, pair)


def plain_stage(iterate, after):
    _, _, count, nz, ny = iterate.shape
    _, padded = half_rows(nz)
    block = block_of(count)
    _, plain, along_y = forward_tables(nz, ny)
    tables = [*split_table(plain), *split_table(along_y)]
    return pl.pallas_call(
        plain_kernel,
        grid=(count // block,),
        in_specs=[
            pl.BlockSpec((1, 1, block, nz, ny), lambda b: (0, NODES - 1, b, 0, 0)),
            pl.BlockSpec(memory_space=pl.ANY),
            *[full(t.shape) for t in tables],
        ],
        out_specs=pl.BlockSpec((block, 2, padded, ny), lambda b: (b, 0, 0, 0)),
        out_shape=jax.ShapeDtypeStruct((count, 2, padded, ny), jnp.float32),
        compiler_params=pltpu.CompilerParams(dimension_semantics=("arbitrary",)),
        cost_estimate=pl.CostEstimate(
            flops=2 * 10**9, bytes_accessed=6 * 10**6, transcendentals=0
        ),
    )(iterate, after, *tables)


def enter(side, ends_refs, decay_ref, around_ref):
    result = []
    for m in range(NODES):
        decay = (decay_ref[side, m, 0], decay_ref[side, m, 1])
        total = None
        for ends_ref in ends_refs:
            moved = (ends_ref[side, m, 0], ends_ref[side, m, 1])
            total = moved if total is None else c_add(c_mul(total, decay), moved)
        result.append(c_mul(total, (around_ref[side, m, 0], around_ref[side, m, 1])))
    return result


def enter_low(state, ends_refs, decay_ref, around_ref):
    for m, value in enumerate(enter(0, ends_refs, decay_ref, around_ref)):
        state[m, 0] = value[0]
        state[m, 1] = value[1]


def enter_back(state, ends_refs, decay_ref, around_ref, low_ref, close_ref):
    for m, entering in enumerate(enter(1, ends_refs, decay_ref, around_ref)):
        value = c_mul((state[m, 0], state[m, 1]), (low_ref[m, 0], low_ref[m, 1]))
        value = c_mul(c_add(value, entering), (close_ref[m, 0], close_ref[m, 1]))
        state[m, 0] = value[0]
        state[m, 1] = value[1]


def node_kernel(*refs, half):
    mask_ref, c_ref, plain_ref, low_ref, high_ref, close_ref, decay_ref, around_ref = refs[:8]
    ends_refs = refs[8:-3]
    out_ref, ahead, state = refs[-3:]
    phase = pl.program_id(0)
    step = pl.program_id(1)
    blocks = pl.num_programs(1)
    block, _, _, padded, ny = c_ref.shape
    _, vectors, _, _ = node_constants()
    last = [complex(v) for v in vectors[NODES - 1]]

    @pl.when((phase == 0) & (step == 0))
    def _():
        enter_low(state, ends_refs, decay_ref, around_ref)

    @pl.when((phase == 1) & (step == 0))
    def _():
        enter_back(state, ends_refs, decay_ref, around_ref, low_ref, close_ref)

    @pl.when(phase == 0)
    def _():
        def tile(t, carry):
            rows = pl.ds(pl.multiple_of(t * 8, 8), 8)
            low = [(low_ref[m, 0, rows], low_ref[m, 1, rows]) for m in range(NODES)]
            values = [(state[m, 0, rows], state[m, 1, rows]) for m in range(NODES)]
            for j in range(block):
                for m in range(NODES):
                    value = (c_ref[j, m, 0, rows], c_ref[j, m, 1, rows])
                    values[m] = c_add(c_mul(values[m], low[m]), value)
                    ahead[step * block + j, m, 0, rows] = values[m][0]
                    ahead[step * block + j, m, 1, rows] = values[m][1]
            for m in range(NODES):
                state[m, 0, rows] = values[m][0]
                state[m, 1, rows] = values[m][1]
            return carry

        lax.fori_loop(0, padded // 8, tile, 0)

    @pl.when(phase == 1)
    def _():
        lane = lax.broadcasted_iota(jnp.int32, (GROUP, ny), 1)
        mask = mask_ref[0]

        def totals(start, base):
            rows = pl.ds(start, 8)
            first = (blocks - 1 - step) * block + base
            high = [(high_ref[m, 0, rows], high_ref[m, 1, rows]) for m in range(NODES)]
            values = [(state[m, 0, rows], state[m, 1, rows]) for m in range(NODES)]
            total = [None] * GROUP
            for j in reversed(range(GROUP)):
                real, imag = (-mask * plain_ref[base + j, part, rows] for part in range(2))
                for m in range(NODES):
                    value = (ahead[first + j, m, 0, rows], ahead[first + j, m, 1, rows])
                    value = c_add(c_mul(values[m], high[m]), value)
                    real += last[m].real * value[0] - last[m].imag * value[1]
                    imag += last[m].real * value[1] + last[m].imag * value[0]
                    values[m] = value
                total[j] = (real, imag)
            for m in range(NODES):
                state[m, 0, rows] = values[m][0]
                state[m, 1, rows] = values[m][1]
            return [
                jnp.swapaxes(jnp.stack([total[j][part] for j in range(GROUP)]), 0, 1)
                for part in range(2)
            ]

        for base in reversed(range(0, block, GROUP)):
            edge = [value[0] for value in totals(half, base)]
            top = totals(0, base)
            turned = [pltpu.roll(value, ny // 2, 1) for value in edge]
            folded = [jnp.where(lane <= ny // 2, top[part][0], turned[part]) for part in range(2)]
            folded[1] = jnp.where(lane % (ny // 2) == 0, edge[0], folded[1])
            for part in range(2):
                out_ref[0, part, base : base + GROUP] = folded[part]
                out_ref[1:8, part, base : base + GROUP] = top[part][1:]

            def tile(t, carry):
                start = pl.multiple_of(t * 8, 8)
                value = totals(start, base)
                for part in range(2):
                    out_ref[pl.ds(start, 8), part, base : base + GROUP] = value[part]
                return carry

            lax.fori_loop(1, half // 8, tile, 0)


def node_stage(c, plain, mask, ends, lines, nz):
    count, _, _, padded, ny = c.shape
    block = block_of(count)
    blocks = count // block
    half = nz // 2

    def early(phase, b):
        return jnp.where(phase == 0, b, blocks - 1)

    def late(phase, b):
        return jnp.where(phase == 0, blocks - 1, blocks - 1 - b)

    tables = [lines[0], lines[1], lines[4], lines[5], lines[6], *ends]
    return pl.pallas_call(
        functools.partial(node_kernel, half=half),
        grid=(2, blocks),
        in_specs=[
            pl.BlockSpec(memory_space=pltpu.SMEM),
            pl.BlockSpec((block, NODES, 2, padded, ny), lambda a, b: (early(a, b), 0, 0, 0, 0)),
            pl.BlockSpec((block, 2, padded, ny), lambda a, b: (late(a, b), 0, 0, 0)),
            *[full(t.shape) for t in tables],
        ],
        out_specs=pl.BlockSpec((half, 2, block, ny), lambda a, b: (0, 0, late(a, b), 0)),
        out_shape=jax.ShapeDtypeStruct((half, 2, count, ny), jnp.float32),
        scratch_shapes=[
            pltpu.VMEM((count, NODES, 2, padded, ny), jnp.float32),
            pltpu.VMEM((NODES, 2, padded, ny), jnp.float32),
        ],
        compiler_params=pltpu.CompilerParams(
            dimension_semantics=("arbitrary", "arbitrary"), vmem_limit_bytes=60 * 1024 * 1024
        ),
    )(mask, c, plain, *tables)


def couple_kernel(q_ref, th_ref, tl_ref, ih_ref, il_ref, grow_ref, close_ref, out_ref, work):
    steps, slabs, _, count, width = q_ref.shape
    nx = slabs * count
    joined = width % 128 == 0

    def side_by_side(table_high, table_low, values):
        if not joined:
            return [dot3_table_left(table_high, table_low, value) for value in values]
        wide = dot3_table_left(table_high, table_low, jnp.concatenate(values, axis=1))
        return [wide[:, i * width : (i + 1) * width] for i in range(len(values))]

    def ahead(s, carry):
        lines = [
            jnp.concatenate([q_ref[s, p, part] for p in range(slabs)], axis=0) for part in range(2)
        ]
        for part, waves in enumerate(side_by_side(th_ref[...], tl_ref[...], lines)):
            work[s, part, 0] = waves[:nx]
            work[s, part, 1] = waves[nx:]
        return carry

    unrolled(steps, ahead)

    def tile(t, carry):
        rows = pl.ds(t * 8, 8)
        for part in range(2):
            grow = (grow_ref[part, 0, rows], grow_ref[part, 1, rows])
            values = [(work[s, part, 0, rows], work[s, part, 1, rows]) for s in range(steps)]
            value = values[0]
            for s in range(1, steps):
                value = c_add(c_mul(grow, value), values[s])
            value = c_mul(value, (close_ref[part, 0, rows], close_ref[part, 1, rows]))
            for s in range(steps):
                work[s, part, 0, rows] = value[0]
                work[s, part, 1, rows] = value[1]
                if s + 1 < steps:
                    value = c_add(c_mul(grow, value), values[s])
        return carry

    lax.fori_loop(0, nx // 8, tile, 0)

    def back(i, carry):
        pair = [2 * i, 2 * i + 1]
        lines = [
            jnp.concatenate(
                [work[s, 0, 0] - work[s, 1, 1], work[s, 0, 1] + work[s, 1, 0]], axis=0
            )
            for s in pair
        ]
        for s, value in zip(pair, side_by_side(ih_ref[...], il_ref[...], lines)):
            for part in range(2):
                for p in range(slabs):
                    base = part * nx + p * count
                    out_ref[s, p, part] = value[base : base + count]
        return carry

    unrolled(steps // 2, back)


def couple_stage(q, velocity, first_mode, nz, ny):
    steps, slabs, _, count, width = q.shape
    nx = slabs * count
    forward, backward = x_tables(nx)
    values, vectors, _, weights = node_constants()
    mode = first_mode + jnp.arange(width, dtype=jnp.int32)
    row, lane = mode // ny, mode % ny
    edge = row == 0
    corner = edge & (lane % (ny // 2) == 0)
    wave_z = jnp.where(edge & (lane > ny // 2), nz // 2, row)
    wave_y = jnp.where(edge & (lane > ny // 2), lane - ny // 2, lane)
    wave_z = jnp.stack([wave_z, jnp.where(corner, nz // 2, wave_z)])[:, None, :]
    theta_z = wave_z.astype(jnp.float32) * (2.0 * math.pi / nz)
    theta_y = wave_y.astype(jnp.float32)[None, None, :] * (2.0 * math.pi / ny)
    theta_x = jnp.arange(nx, dtype=jnp.int32).astype(jnp.float32)[None, :, None] * (2.0 * math.pi / nx)
    real = diffusion_number * (
        (2.0 * jnp.cos(theta_x) - 2.0)
        + (2.0 * jnp.cos(theta_z) - 2.0)
        + (2.0 * jnp.cos(theta_y) - 2.0)
    )
    imag = -(
        velocity[0] * jnp.sin(theta_x)
        + velocity[1] * jnp.sin(theta_y)
        + velocity[2] * jnp.sin(theta_z)
    )
    grow = None
    for m in range(NODES):
        mu = complex(values[m])
        below = (1.0 - (mu.real * real - mu.imag * imag), -(mu.real * imag + mu.imag * real))
        above = complex(vectors[NODES - 1, m] * weights[m])
        added = c_div((above.real, above.imag), below)
        grow = added if grow is None else (grow[0] + added[0], grow[1] + added[1])
    whole = c_power(grow, steps)
    close = c_div(
        (circulant_alpha, 0.0), (1.0 - circulant_alpha * whole[0], -circulant_alpha * whole[1])
    )
    return pl.pallas_call(
        couple_kernel,
        out_shape=jax.ShapeDtypeStruct(q.shape, jnp.float32),
        scratch_shapes=[pltpu.VMEM((steps, 2, 2, nx, width), jnp.float32)],
        compiler_params=pltpu.CompilerParams(vmem_limit_bytes=60 * 1024 * 1024),
    )(
        q,
        *split_table(forward),
        *split_table(backward),
        jnp.stack(grow, axis=1),
        jnp.stack(close, axis=1),
    )


def edge_kernel(b_ref, ends_ref, low_ref, high_ref, beta_ref, wide_ref, out_ref):
    half, _, count, ny = b_ref.shape
    padded = wide_ref.shape[2]
    lane = lax.broadcasted_iota(jnp.int32, (GROUP, ny), 1)
    inside = lane % (ny // 2) != 0
    kept = jnp.where(inside, jnp.where(lane < ny // 2, 2.0, 0.0), 1.0)
    zero = jnp.zeros((GROUP, ny), jnp.float32)

    def unfold(g, carry):
        base = pl.multiple_of(g * GROUP, GROUP)
        planes = pl.ds(base, GROUP)
        top = [b_ref[0, part, planes] for part in range(2)]
        turned = [pltpu.roll(value, ny // 2, 1) for value in top]
        first = (top[0], jnp.where(inside, top[1], 0.0))
        edge = (jnp.where(inside, turned[0], top[1]), jnp.where(inside, turned[1], 0.0))
        for part in range(2):
            for start in range(0, half, 8):
                rows = [b_ref[start + r, part, planes] for r in range(8)]
                if start == 0:
                    rows[0] = first[part] * kept
                wide_ref[planes, part, start : start + 8] = jnp.swapaxes(jnp.stack(rows), 0, 1)
            rows = [edge[part] * kept] + [zero] * 7
            wide_ref[planes, part, half : half + 8] = jnp.swapaxes(jnp.stack(rows), 0, 1)
        return carry

    lax.fori_loop(0, count // GROUP, unfold, 0)

    def tile(t, carry):
        rows = pl.ds(pl.multiple_of(t * 8, 8), 8)
        for side, table in enumerate((low_ref, high_ref)):
            decay = [(table[m, 0, rows], table[m, 1, rows]) for m in range(NODES)]

            def group(g, values):
                for i in range(GROUP):
                    j = g * GROUP + i
                    j = j if side == 0 else count - 1 - j
                    plane = (wide_ref[j, 0, rows], wide_ref[j, 1, rows])
                    values = [c_add(c_mul(v, d), plane) for v, d in zip(values, decay)]
                return values

            values = lax.fori_loop(0, count // GROUP, group, [(zero, zero)] * NODES)
            for m in range(NODES):
                value = c_mul(values[m], (beta_ref[m, 0, rows], beta_ref[m, 1, rows]))
                for part in range(2):
                    out_ref[side, m, part, rows] = ends_ref[side, m, part, rows] + value[part]
        return carry

    lax.fori_loop(0, padded // 8, tile, 0)


def edge_stage(b, ends, lines):
    count = b.shape[2]
    padded, ny = lines[0].shape[2:]
    return pl.pallas_call(
        edge_kernel,
        out_shape=[
            jax.ShapeDtypeStruct((count, 2, padded, ny), jnp.float32),
            jax.ShapeDtypeStruct((2, NODES, 2, padded, ny), jnp.float32),
        ],
        compiler_params=pltpu.CompilerParams(vmem_limit_bytes=60 * 1024 * 1024),
    )(b, ends, lines[0], lines[1], lines[3])


def inverse_kernel(*refs):
    c_ref, b_ref, low_ref, high_ref, beta_ref, close_ref, decay_ref, around_ref = refs[:8]
    yh_ref, yl_ref, zh_ref, zl_ref = refs[8:12]
    ends_refs = refs[12:-3]
    out_ref, ahead, state = refs[-3:]
    phase = pl.program_id(0)
    step = pl.program_id(1)
    blocks = pl.num_programs(1)
    block, _, _, padded, ny = c_ref.shape
    nz = out_ref.shape[3]

    @pl.when((phase == 0) & (step == 0))
    def _():
        enter_low(state, ends_refs, decay_ref, around_ref)

    @pl.when((phase == 1) & (step == 0))
    def _():
        enter_back(state, ends_refs, decay_ref, around_ref, low_ref, close_ref)

    @pl.when(phase == 0)
    def _():
        def tile(t, carry):
            rows = pl.ds(pl.multiple_of(t * 8, 8), 8)
            nodes = range(NODES)
            low = [(low_ref[m, 0, rows], low_ref[m, 1, rows]) for m in nodes]
            beta = [(beta_ref[m, 0, rows], beta_ref[m, 1, rows]) for m in nodes]
            values = [(state[m, 0, rows], state[m, 1, rows]) for m in nodes]
            for j in range(block):
                plane = (b_ref[j, 0, rows], b_ref[j, 1, rows])
                for m in nodes:
                    source = (c_ref[j, m, 0, rows], c_ref[j, m, 1, rows])
                    source = c_add(c_mul(plane, beta[m]), source)
                    values[m] = c_add(c_mul(values[m], low[m]), source)
                    ahead[step * block + j, m, 0, rows] = values[m][0]
                    ahead[step * block + j, m, 1, rows] = values[m][1]
            for m in nodes:
                state[m, 0, rows] = values[m][0]
                state[m, 1, rows] = values[m][1]
            return carry

        lax.fori_loop(0, padded // 8, tile, 0)

    @pl.when(phase == 1)
    def _():
        first = (blocks - 1 - step) * block

        def tile(t, carry):
            rows = pl.ds(pl.multiple_of(t * 8, 8), 8)
            nodes = range(NODES)
            high = [(high_ref[m, 0, rows], high_ref[m, 1, rows]) for m in nodes]
            values = [(state[m, 0, rows], state[m, 1, rows]) for m in nodes]
            for j in reversed(range(block)):
                for m in nodes:
                    value = (ahead[first + j, m, 0, rows], ahead[first + j, m, 1, rows])
                    values[m] = c_add(c_mul(values[m], high[m]), value)
                    ahead[first + j, m, 0, rows] = values[m][0]
                    ahead[first + j, m, 1, rows] = values[m][1]
            for m in nodes:
                state[m, 0, rows] = values[m][0]
                state[m, 1, rows] = values[m][1]
            return carry

        lax.fori_loop(0, padded // 8, tile, 0)

        def pair(i, carry):
            rows = []
            for half in range(2):
                row = first + 2 * i + half
                for m in range(NODES):
                    rows.append(jnp.concatenate([ahead[row, m, 0], ahead[row, m, 1]], axis=1))
            lines = dot3_table_right(jnp.concatenate(rows, axis=0), yh_ref[...], yl_ref[...])
            columns = []
            for half in range(2):
                stacked = []
                for m in range(NODES):
                    base = (half * NODES + m) * padded
                    stacked.append(lines[base : base + padded, :ny])
                    stacked.append(lines[base : base + padded, ny:])
                columns.append(jnp.concatenate(stacked, axis=0))
            grid = dot3_table_left(zh_ref[...], zl_ref[...], jnp.concatenate(columns, axis=1))
            for half in range(2):
                for n in range(NODES):
                    out_ref[0, n, 2 * i + half] = grid[
                        n * nz : (n + 1) * nz, half * ny : (half + 1) * ny
                    ]
            return carry

        unrolled(block // 2, pair)


def inverse_stage(c, b, ends, lines, nz):
    count, _, _, padded, ny = c.shape
    block = block_of(count)
    blocks = count // block
    mixed, along_y = inverse_tables(nz, ny)
    tables = [lines[0], lines[1], *lines[3:], *split_table(along_y), *split_table(mixed), *ends]

    def early(phase, b):
        return jnp.where(phase == 0, b, blocks - 1)

    def late(phase, b):
        return jnp.where(phase == 0, blocks - 1, blocks - 1 - b)

    return pl.pallas_call(
        inverse_kernel,
        grid=(2, blocks),
        in_specs=[
            pl.BlockSpec((block, NODES, 2, padded, ny), lambda a, b: (early(a, b), 0, 0, 0, 0)),
            pl.BlockSpec((block, 2, padded, ny), lambda a, b: (early(a, b), 0, 0, 0)),
            *[full(t.shape) for t in tables],
        ],
        out_specs=pl.BlockSpec((1, NODES, block, nz, ny), lambda a, b: (0, 0, late(a, b), 0, 0)),
        out_shape=jax.ShapeDtypeStruct((1, NODES, count, nz, ny), jnp.float32),
        scratch_shapes=[
            pltpu.VMEM((count, NODES, 2, padded, ny), jnp.float32),
            pltpu.VMEM((NODES, 2, padded, ny), jnp.float32),
        ],
        compiler_params=pltpu.CompilerParams(
            dimension_semantics=("arbitrary", "arbitrary"), vmem_limit_bytes=60 * 1024 * 1024
        ),
    )(c, b, *tables)


def ring_ends(ends, slabs):
    result = [ends]
    for distance in range(slabs - 1, 0, -1):
        if 2 * distance == slabs:
            moved = lax.ppermute(ends, "space", [(i, (i + distance) % slabs) for i in range(slabs)])
        else:
            moved = jnp.stack(
                [
                    lax.ppermute(
                        ends[side], "space", [(i, (i + shift) % slabs) for i in range(slabs)]
                    )
                    for side, shift in enumerate((distance, -distance))
                ]
            )
        result.append(moved)
    return result


def to_modes(q, devices):
    half, _, count, ny = q.shape
    pieces = devices // half
    if pieces > 1:
        q = q.reshape(half, 2 * count, pieces, ny // pieces)
        q = jnp.transpose(q, (0, 2, 1, 3))
    return q.reshape(devices, 2 * count, ny // pieces)


def from_modes(b, half):
    devices, lines, width = b.shape
    pieces = devices // half
    if pieces > 1:
        b = jnp.transpose(b.reshape(half, pieces, lines, width), (0, 2, 1, 3))
    return b.reshape(half, 2, lines // 2, pieces * width)


def shards(iterate, right_side, diffusivity, velocity):
    steps, slabs = lax.axis_size("tm"), lax.axis_size("space")
    devices = steps * slabs
    _, _, count, nz, ny = iterate.shape
    up = [(i, (i + 1) % slabs) for i in range(slabs)]
    down = [(target, source) for source, target in up]
    last, first = iterate[0, :, count - 1], iterate[0, :, 0]
    if slabs == 2:
        halo = lax.ppermute(jnp.stack([last, first]), "space", up)
    else:
        halo = jnp.stack([lax.ppermute(last, "space", up), lax.ppermute(first, "space", down)])
    lines = line_tables(velocity, nz, ny, count, slabs)
    c, ends = forward_stage(iterate, right_side, diffusivity, halo, lines)
    every = ring_ends(ends, slabs)
    plain = plain_stage(iterate, ends)
    step = lax.axis_index("tm")
    mask = jnp.where(step == steps - 1, 1.0, 0.0).astype(jnp.float32)[None]
    q = node_stage(c, plain, mask, every, lines, nz)
    q = lax.all_to_all(to_modes(q, devices), ("tm", "space"), 0, 0, tiled=True)
    width = q.shape[2]
    first_mode = (step * slabs + lax.axis_index("space")) * width
    b = couple_stage(q.reshape(steps, slabs, 2, count, width), velocity, first_mode, nz, ny)
    b = lax.all_to_all(b.reshape(devices, 2 * count, width), ("tm", "space"), 0, 0, tiled=True)
    b, ends = edge_stage(from_modes(b, nz // 2), ends, lines)
    return inverse_stage(c, b, ring_ends(ends, slabs), lines, nz)


def solution(mesh):
    placed = (
        P("tm", None, "space", None, None),
        P("tm", None, "space", None, None),
        P("space", None, None),
        P(),
    )
    return jax.shard_map(
        shards,
        mesh=mesh,
        in_specs=placed,
        out_specs=P("tm", None, "space", None, None),
        check_vma=False,
    )
```

```python
import functools
import math

import jax
import jax.numpy as jnp
import numpy as np
from jax import lax
from jax.experimental import pallas as pl
from jax.experimental.pallas import tpu as pltpu
from jax.sharding import PartitionSpec as P

diffusion_number = 16.0
circulant_alpha = 0.1
NODES = 4
GROUP = 8


def collocation_matrix():
    radau_nodes = [0.08858795951270394, 0.4094668644407347, 0.7876594617608471, 1.0]
    matrix = [[0.0] * 4 for row_index in range(4)]
    for column_index in range(4):
        coefficients = [1.0]
        for other_index in range(4):
            if other_index != column_index:
                scale_value = 1.0 / (radau_nodes[column_index] - radau_nodes[other_index])
                shifted = [0.0] + [value * scale_value for value in coefficients]
                lowered = [
                    -radau_nodes[other_index] * scale_value * value for value in coefficients
                ] + [0.0]
                coefficients = [
                    left_value + right_value for left_value, right_value in zip(shifted, lowered)
                ]
        for row_index in range(4):
            total = 0.0
            for power_index in range(len(coefficients)):
                total = total + coefficients[power_index] * radau_nodes[row_index] ** (
                    power_index + 1
                ) / (power_index + 1)
            matrix[row_index][column_index] = total
    return matrix


def solve_system(matrix, target):
    count = len(target)
    rows_list = [list(matrix[row_index]) + [target[row_index]] for row_index in range(count)]
    for column in range(count):
        best_row = column
        for candidate in range(column + 1, count):
            if abs(rows_list[candidate][column]) > abs(rows_list[best_row][column]):
                best_row = candidate
        saved_row = rows_list[column]
        rows_list[column] = rows_list[best_row]
        rows_list[best_row] = saved_row
        leader = rows_list[column][column]
        for other_row in range(count):
            if other_row != column:
                factor = rows_list[other_row][column] / leader
                rows_list[other_row] = [
                    left_value - factor * right_value
                    for left_value, right_value in zip(rows_list[other_row], rows_list[column])
                ]
    return [
        rows_list[row_index][count] / rows_list[row_index][row_index] for row_index in range(count)
    ]


def node_basis():
    matrix = collocation_matrix()
    helper = [[0.0] * 4 for row_index in range(4)]
    coefficients = [0.0, 0.0, 0.0, 0.0, 1.0]
    for order in range(1, 5):
        product = [
            [
                sum((matrix[row_index][inner] * helper[inner][column] for inner in range(4)))
                for column in range(4)
            ]
            for row_index in range(4)
        ]
        for row_index in range(4):
            product[row_index][row_index] = product[row_index][row_index] + coefficients[5 - order]
        helper = product
        trace_value = sum(
            (
                sum((matrix[row_index][inner] * helper[inner][row_index] for inner in range(4)))
                for row_index in range(4)
            )
        )
        coefficients[4 - order] = -trace_value / order
    roots_list = [(0.4 + 0.9j) ** power_index for power_index in range(4)]
    for sweep in range(400):
        for root_index in range(4):
            current = roots_list[root_index]
            numer = 0.0
            for power_index in range(4, -1, -1):
                numer = numer * current + coefficients[power_index]
            denom = 1.0
            for other_index in range(4):
                if other_index != root_index:
                    denom = denom * (current - roots_list[other_index])
            roots_list[root_index] = current - numer / denom
    vectors = [[0.0] * 4 for row_index in range(4)]
    for root_index in range(4):
        shifted = [
            [
                matrix[row_index][column] - (roots_list[root_index] if row_index == column else 0.0)
                for column in range(3)
            ]
            for row_index in range(3)
        ]
        target = [-matrix[row_index][3] for row_index in range(3)]
        parts = solve_system(shifted, target) + [1.0 + 0j]
        for row_index in range(4):
            vectors[row_index][root_index] = parts[row_index]
    inverse = [[0.0] * 4 for row_index in range(4)]
    for column in range(4):
        unit = [1.0 if row_index == column else 0.0 for row_index in range(4)]
        parts = solve_system(vectors, unit)
        for row_index in range(4):
            inverse[row_index][column] = parts[row_index]
    weights = [sum((inverse[row_index][column] for column in range(4))) for row_index in range(4)]
    return (roots_list, vectors, inverse, weights)


def split_table(table):
    table = jnp.asarray(np.asarray(table, np.float32))
    high = table.astype(jnp.bfloat16)
    return high, (table - high.astype(jnp.float32)).astype(jnp.bfloat16)


def split(values):
    high = values.astype(jnp.bfloat16)
    return high, (values - high.astype(jnp.float32)).astype(jnp.bfloat16)


def dot(left, right):
    return jnp.dot(left, right, preferred_element_type=jnp.float32)


def dot3_table_left(table_high, table_low, values):
    high, low = split(values)
    return dot(table_high, high) + (dot(table_high, low) + dot(table_low, high))


def dot3_table_right(values, table_high, table_low):
    high, low = split(values)
    return dot(high, table_high) + (dot(low, table_high) + dot(high, table_low))


def node_constants():
    values, vectors, inverse, weights = node_basis()
    return (
        np.array([complex(v) for v in values]),
        np.array([[complex(v) for v in row] for row in vectors]),
        np.array([[complex(v) for v in row] for row in inverse]),
        np.array([complex(v) for v in weights]),
    )


def half_rows(nz):
    kept = nz // 2 + 1
    return kept, -(-kept // 8) * 8


def forward_tables(nz, ny):
    _, _, inverse, _ = node_constants()
    kept, padded = half_rows(nz)
    wave = np.zeros((padded, nz), complex)
    wave[:kept] = np.exp(-2j * math.pi * np.outer(np.arange(kept), np.arange(nz)) / nz)
    mixed = np.zeros((NODES, 2, padded, NODES, nz))
    for m in range(NODES):
        for n in range(NODES):
            mixed[m, 0, :, n] = (inverse[m, n] * wave).real
            mixed[m, 1, :, n] = (inverse[m, n] * wave).imag
    plain = np.concatenate([wave.real, wave.imag], axis=0)
    angle = 2 * math.pi * (np.outer(np.arange(ny), np.arange(ny)) % ny) / ny
    c, s = np.cos(angle), np.sin(angle)
    along_y = np.block([[c, -s], [s, c]])
    return mixed.reshape(NODES * 2 * padded, NODES * nz), plain, along_y


def inverse_tables(nz, ny):
    _, vectors, _, _ = node_constants()
    kept, padded = half_rows(nz)
    weight = np.where((np.arange(kept) == 0) | (2 * np.arange(kept) == nz), 1.0, 2.0)
    wave = np.zeros((nz, padded), complex)
    wave[:, :kept] = np.exp(2j * math.pi * np.outer(np.arange(nz), np.arange(kept)) / nz) * weight / nz
    mixed = np.zeros((NODES, nz, NODES, 2, padded))
    for n in range(NODES):
        for m in range(NODES):
            mixed[n, :, m, 0] = (vectors[n, m] * wave).real
            mixed[n, :, m, 1] = -(vectors[n, m] * wave).imag
    angle = 2 * math.pi * (np.outer(np.arange(ny), np.arange(ny)) % ny) / ny
    c, s = np.cos(angle) / ny, np.sin(angle) / ny
    along_y = np.block([[c, s], [-s, c]])
    return mixed.reshape(NODES * nz, NODES * 2 * padded), along_y


def x_tables(nx):
    angle = 2 * math.pi * (np.outer(np.arange(nx), np.arange(nx)) % nx) / nx
    c, s = np.cos(angle), np.sin(angle)
    return np.concatenate([c, -s], axis=0), np.block([[c, -s], [s, c]]) / nx


def c_mul(a, b):
    return a[0] * b[0] - a[1] * b[1], a[0] * b[1] + a[1] * b[0]


def c_add(a, b):
    return a[0] + b[0], a[1] + b[1]


def c_div(a, b):
    size = b[0] * b[0] + b[1] * b[1]
    return (a[0] * b[0] + a[1] * b[1]) / size, (a[1] * b[0] - a[0] * b[1]) / size


def c_power(a, count):
    result = None
    while count:
        if count & 1:
            result = a if result is None else c_mul(result, a)
        count >>= 1
        if count:
            a = c_mul(a, a)
    return result


def c_sqrt(a):
    size = jnp.sqrt(a[0] * a[0] + a[1] * a[1])
    large = jnp.sqrt(0.5 * (size + jnp.abs(a[0])))
    small = a[1] / (2.0 * large)
    flip = a[0] < 0.0
    return (
        jnp.where(flip, jnp.abs(small), large),
        jnp.where(flip, jnp.where(a[1] < 0.0, -large, large), small),
    )


def line_kernel(velocity_ref, real_ref, sin_z_ref, sin_y_ref, *out_refs, count, slabs):
    values, _, _, weights = node_constants()
    real = real_ref[...] - 2.0 * diffusion_number
    imag = -(velocity_ref[1] * sin_y_ref[...] + velocity_ref[2] * sin_z_ref[...])
    one, zero = jnp.ones_like(real), jnp.zeros_like(real)
    from_low = diffusion_number + 0.5 * velocity_ref[0]
    from_high = diffusion_number - 0.5 * velocity_ref[0]
    product = 4.0 * from_low * from_high
    for m in range(NODES):
        mu = complex(values[m])
        mu2 = mu * mu
        diagonal = (1.0 - (mu.real * real - mu.imag * imag), -(mu.real * imag + mu.imag * real))
        square = c_mul(diagonal, diagonal)
        root = c_sqrt((square[0] - product * mu2.real, square[1] - product * mu2.imag))
        turn = diagonal[0] * root[0] + diagonal[1] * root[1] < 0.0
        root = (jnp.where(turn, -root[0], root[0]), jnp.where(turn, -root[1], root[1]))
        kappa = (0.5 * (diagonal[0] + root[0]), 0.5 * (diagonal[1] + root[1]))
        gain = c_div((one, zero), kappa)
        ratio = (mu.real * gain[0] - mu.imag * gain[1], mu.real * gain[1] + mu.imag * gain[0])
        weight = complex(weights[m])
        beta = (
            weight.real * gain[0] - weight.imag * gain[1],
            weight.real * gain[1] + weight.imag * gain[0],
        )
        sides = [(factor * ratio[0], factor * ratio[1]) for factor in (from_low, from_high)]
        tables = [*sides, gain, beta, c_div(kappa, root)]
        for table, out_ref in zip(tables, out_refs):
            out_ref[m, 0] = table[0]
            out_ref[m, 1] = table[1]
        for side in range(2):
            decay = c_power(sides[side], count)
            whole = c_power(decay, slabs)
            around = c_div((one, zero), (1.0 - whole[0], -whole[1]))
            for part in range(2):
                out_refs[5][side, m, part] = decay[part]
                out_refs[6][side, m, part] = around[part]


def line_tables(velocity, nz, ny, count, slabs):
    _, padded = half_rows(nz)
    theta_z = 2 * math.pi * np.arange(padded)[:, None] / nz
    theta_y = 2 * math.pi * np.arange(ny)[None, :] / ny
    real = diffusion_number * ((2 * np.cos(theta_z) - 2) + (2 * np.cos(theta_y) - 2))
    waves = [real, np.sin(theta_z) + 0 * theta_y, np.sin(theta_y) + 0 * theta_z]
    one = jax.ShapeDtypeStruct((NODES, 2, padded, ny), jnp.float32)
    two = jax.ShapeDtypeStruct((2, NODES, 2, padded, ny), jnp.float32)
    return pl.pallas_call(
        functools.partial(line_kernel, count=count, slabs=slabs),
        in_specs=[
            pl.BlockSpec(memory_space=pltpu.SMEM),
            *[pl.BlockSpec(memory_space=pltpu.VMEM)] * 3,
        ],
        out_shape=[one] * 5 + [two] * 2,
        compiler_params=pltpu.CompilerParams(vmem_limit_bytes=60 * 1024 * 1024),
    )(velocity, *[jnp.asarray(wave, jnp.float32) for wave in waves])


def block_of(count):
    return 16 if count % 16 == 0 else GROUP


def unrolled(count, body, most=8):
    each = math.gcd(count, most)

    def turn(i, carry):
        for k in range(each):
            body(i * each + k, carry)
        return carry

    lax.fori_loop(0, count // each, turn, 0)


def forward_kernel(
    block_ref,
    prev_ref,
    next_ref,
    halo_ref,
    right_ref,
    diffusivity_ref,
    zh_ref,
    zl_ref,
    yh_ref,
    yl_ref,
    low_ref,
    high_ref,
    gain_ref,
    out_ref,
    ends_ref,
    planes,
    power,
    *,
    padded,
):
    step = pl.program_id(0)
    steps = pl.num_programs(0)
    block, nz, ny = block_ref.shape[2:]
    matrix = collocation_matrix()

    @pl.when(step == 0)
    def _():
        ends_ref[...] = jnp.zeros_like(ends_ref)
        planes[0] = halo_ref[0]
        for m in range(NODES):
            power[m, 0] = jnp.ones_like(power[m, 0])
            power[m, 1] = jnp.zeros_like(power[m, 1])

    @pl.when(step > 0)
    def _():
        planes[0] = prev_ref[0, :, 0]

    @pl.when(step == steps - 1)
    def _():
        planes[block + 1] = halo_ref[1]

    @pl.when(step < steps - 1)
    def _():
        planes[block + 1] = next_ref[0, :, 0]

    for j in range(block):
        planes[j + 1] = block_ref[0, :, j]

    def pair(index, carry):
        columns = []
        for half in range(2):
            j = 2 * index + half
            factor = diffusion_number * (diffusivity_ref[j] - 1.0)
            spread = []
            for n in range(NODES):
                f = planes[j + 1, n]
                lap = (
                    (planes[j, n] + planes[j + 2, n])
                    + (pltpu.roll(f, 1, 0) + pltpu.roll(f, nz - 1, 0))
                    + (pltpu.roll(f, 1, 1) + pltpu.roll(f, ny - 1, 1))
                    - 6.0 * f
                )
                spread.append(factor * lap)
            mixed = []
            for m in range(NODES):
                total = right_ref[0, m, j]
                for n in range(NODES):
                    total = total + matrix[m][n] * spread[n]
                mixed.append(total)
            columns.append(jnp.concatenate(mixed, axis=0))
        spectrum_z = dot3_table_left(zh_ref[...], zl_ref[...], jnp.concatenate(columns, axis=1))
        rows = []
        for half in range(2):
            lanes = slice(half * ny, (half + 1) * ny)
            for m in range(NODES):
                base = 2 * m * padded
                rows.append(
                    jnp.concatenate(
                        [
                            spectrum_z[base : base + padded, lanes],
                            spectrum_z[base + padded : base + 2 * padded, lanes],
                        ],
                        axis=1,
                    )
                )
        spectrum = dot3_table_right(jnp.concatenate(rows, axis=0), yh_ref[...], yl_ref[...])
        for half in range(2):
            j = 2 * index + half
            for m in range(NODES):
                base = (half * NODES + m) * padded
                value = (spectrum[base : base + padded, :ny], spectrum[base : base + padded, ny:])
                value = c_mul(value, (gain_ref[m, 0], gain_ref[m, 1]))
                out_ref[j, m, 0] = value[0]
                out_ref[j, m, 1] = value[1]
        return carry

    unrolled(block // 2, pair)

    def tile(t, carry):
        rows = pl.ds(pl.multiple_of(t * 8, 8), 8)
        nodes = range(NODES)
        low = [(low_ref[m, 0, rows], low_ref[m, 1, rows]) for m in nodes]
        high = [(high_ref[m, 0, rows], high_ref[m, 1, rows]) for m in nodes]
        ahead = [(ends_ref[0, m, 0, rows], ends_ref[0, m, 1, rows]) for m in nodes]
        back = [(out_ref[block - 1, m, 0, rows], out_ref[block - 1, m, 1, rows]) for m in nodes]
        for j in range(block):
            k = block - 1 - j
            for m in nodes:
                value = (out_ref[j, m, 0, rows], out_ref[j, m, 1, rows])
                ahead[m] = c_add(c_mul(ahead[m], low[m]), value)
                if j:
                    value = (out_ref[k, m, 0, rows], out_ref[k, m, 1, rows])
                    back[m] = c_add(c_mul(back[m], high[m]), value)
        for m in nodes:
            scale = (power[m, 0, rows], power[m, 1, rows])
            added = c_mul(scale, back[m])
            scale = c_mul(scale, c_power(high[m], block))
            for part in range(2):
                ends_ref[0, m, part, rows] = ahead[m][part]
                ends_ref[1, m, part, rows] = ends_ref[1, m, part, rows] + added[part]
                power[m, part, rows] = scale[part]
        return carry

    lax.fori_loop(0, padded // 8, tile, 0)


def full(shape):
    zeros = (0,) * len(shape)
    return pl.BlockSpec(shape, lambda *_: zeros)


def forward_stage(iterate, right_side, diffusivity, halo, lines):
    _, _, count, nz, ny = iterate.shape
    _, padded = half_rows(nz)
    block = block_of(count)
    blocks = count // block
    mixed, _, along_y = forward_tables(nz, ny)
    tables = [*split_table(mixed), *split_table(along_y), *lines[:3]]
    plane = (1, NODES, 1, nz, ny)
    return pl.pallas_call(
        functools.partial(forward_kernel, padded=padded),
        grid=(blocks,),
        in_specs=[
            pl.BlockSpec((1, NODES, block, nz, ny), lambda b: (0, 0, b, 0, 0)),
            pl.BlockSpec(plane, lambda b: (0, 0, jnp.maximum(b * block - 1, 0), 0, 0)),
            pl.BlockSpec(plane, lambda b: (0, 0, jnp.minimum((b + 1) * block, count - 1), 0, 0)),
            full(halo.shape),
            pl.BlockSpec((1, NODES, block, nz, ny), lambda b: (0, 0, b, 0, 0)),
            pl.BlockSpec((block, nz, ny), lambda b: (b, 0, 0)),
            *[full(t.shape) for t in tables],
        ],
        out_specs=[
            pl.BlockSpec((block, NODES, 2, padded, ny), lambda b: (b, 0, 0, 0, 0)),
            full((2, NODES, 2, padded, ny)),
        ],
        out_shape=[
            jax.ShapeDtypeStruct((count, NODES, 2, padded, ny), jnp.float32),
            jax.ShapeDtypeStruct((2, NODES, 2, padded, ny), jnp.float32),
        ],
        scratch_shapes=[
            pltpu.VMEM((block + 2, NODES, nz, ny), jnp.float32),
            pltpu.VMEM((NODES, 2, padded, ny), jnp.float32),
        ],
        compiler_params=pltpu.CompilerParams(
            dimension_semantics=("arbitrary",), vmem_limit_bytes=60 * 1024 * 1024
        ),
    )(iterate, iterate, iterate, halo, right_side, diffusivity, *tables)


def plain_kernel(field_ref, after_ref, zh_ref, zl_ref, yh_ref, yl_ref, out_ref):
    del after_ref
    block, nz, ny = field_ref.shape[2:]
    padded = out_ref.shape[2]

    def pair(index, carry):
        planes = [field_ref[0, 0, 2 * index + half] for half in range(2)]
        waves = dot3_table_left(zh_ref[...], zl_ref[...], jnp.concatenate(planes, axis=1))
        rows = []
        for half in range(2):
            lanes = slice(half * ny, (half + 1) * ny)
            rows.append(jnp.concatenate([waves[:padded, lanes], waves[padded:, lanes]], axis=1))
        spectrum = dot3_table_right(jnp.concatenate(rows, axis=0), yh_ref[...], yl_ref[...])
        for half in range(2):
            for part in range(2):
                out_ref[2 * index + half, part] = spectrum[
                    half * padded : (half + 1) * padded, part * ny : (part + 1) * ny
                ]
        return carry

    unrolled(block // 2, pair)


def plain_stage(iterate, after):
    _, _, count, nz, ny = iterate.shape
    _, padded = half_rows(nz)
    block = block_of(count)
    _, plain, along_y = forward_tables(nz, ny)
    tables = [*split_table(plain), *split_table(along_y)]
    return pl.pallas_call(
        plain_kernel,
        grid=(count // block,),
        in_specs=[
            pl.BlockSpec((1, 1, block, nz, ny), lambda b: (0, NODES - 1, b, 0, 0)),
            pl.BlockSpec(memory_space=pl.ANY),
            *[full(t.shape) for t in tables],
        ],
        out_specs=pl.BlockSpec((block, 2, padded, ny), lambda b: (b, 0, 0, 0)),
        out_shape=jax.ShapeDtypeStruct((count, 2, padded, ny), jnp.float32),
        compiler_params=pltpu.CompilerParams(
            dimension_semantics=("arbitrary",), vmem_limit_bytes=60 * 1024 * 1024
        ),
        cost_estimate=pl.CostEstimate(
            flops=2 * 10**9, bytes_accessed=6 * 10**6, transcendentals=0
        ),
    )(iterate, after, *tables)


def enter(side, ends_refs, decay_ref, around_ref):
    result = []
    for m in range(NODES):
        decay = (decay_ref[side, m, 0], decay_ref[side, m, 1])
        total = None
        for ends_ref in ends_refs:
            moved = (ends_ref[side, m, 0], ends_ref[side, m, 1])
            total = moved if total is None else c_add(c_mul(total, decay), moved)
        result.append(c_mul(total, (around_ref[side, m, 0], around_ref[side, m, 1])))
    return result


def enter_low(state, ends_refs, decay_ref, around_ref):
    for m, value in enumerate(enter(0, ends_refs, decay_ref, around_ref)):
        state[m, 0] = value[0]
        state[m, 1] = value[1]


def enter_back(state, ends_refs, decay_ref, around_ref, low_ref, close_ref):
    for m, entering in enumerate(enter(1, ends_refs, decay_ref, around_ref)):
        value = c_mul((state[m, 0], state[m, 1]), (low_ref[m, 0], low_ref[m, 1]))
        value = c_mul(c_add(value, entering), (close_ref[m, 0], close_ref[m, 1]))
        state[m, 0] = value[0]
        state[m, 1] = value[1]


def node_kernel(*refs, half):
    mask_ref, c_ref, plain_ref, low_ref, high_ref, close_ref, decay_ref, around_ref = refs[:8]
    ends_refs = refs[8:-3]
    out_ref, ahead, state = refs[-3:]
    phase = pl.program_id(0)
    step = pl.program_id(1)
    blocks = pl.num_programs(1)
    block, _, _, padded, ny = c_ref.shape
    _, vectors, _, _ = node_constants()
    last = [complex(v) for v in vectors[NODES - 1]]

    @pl.when((phase == 0) & (step == 0))
    def _():
        enter_low(state, ends_refs, decay_ref, around_ref)

    @pl.when((phase == 1) & (step == 0))
    def _():
        enter_back(state, ends_refs, decay_ref, around_ref, low_ref, close_ref)

    @pl.when(phase == 0)
    def _():
        def tile(t, carry):
            rows = pl.ds(pl.multiple_of(t * 8, 8), 8)
            low = [(low_ref[m, 0, rows], low_ref[m, 1, rows]) for m in range(NODES)]
            values = [(state[m, 0, rows], state[m, 1, rows]) for m in range(NODES)]
            for j in range(block):
                for m in range(NODES):
                    value = (c_ref[j, m, 0, rows], c_ref[j, m, 1, rows])
                    values[m] = c_add(c_mul(values[m], low[m]), value)
                    ahead[step * block + j, m, 0, rows] = values[m][0]
                    ahead[step * block + j, m, 1, rows] = values[m][1]
            for m in range(NODES):
                state[m, 0, rows] = values[m][0]
                state[m, 1, rows] = values[m][1]
            return carry

        lax.fori_loop(0, padded // 8, tile, 0)

    @pl.when(phase == 1)
    def _():
        lane = lax.broadcasted_iota(jnp.int32, (GROUP, ny), 1)
        mask = mask_ref[0]

        def totals(start, base):
            rows = pl.ds(start, 8)
            first = (blocks - 1 - step) * block + base
            high = [(high_ref[m, 0, rows], high_ref[m, 1, rows]) for m in range(NODES)]
            values = [(state[m, 0, rows], state[m, 1, rows]) for m in range(NODES)]
            total = [None] * GROUP
            for j in reversed(range(GROUP)):
                real, imag = (-mask * plain_ref[base + j, part, rows] for part in range(2))
                for m in range(NODES):
                    value = (ahead[first + j, m, 0, rows], ahead[first + j, m, 1, rows])
                    value = c_add(c_mul(values[m], high[m]), value)
                    real += last[m].real * value[0] - last[m].imag * value[1]
                    imag += last[m].real * value[1] + last[m].imag * value[0]
                    values[m] = value
                total[j] = (real, imag)
            for m in range(NODES):
                state[m, 0, rows] = values[m][0]
                state[m, 1, rows] = values[m][1]
            return [
                jnp.swapaxes(jnp.stack([total[j][part] for j in range(GROUP)]), 0, 1)
                for part in range(2)
            ]

        for base in reversed(range(0, block, GROUP)):
            edge = [value[0] for value in totals(half, base)]
            top = totals(0, base)
            turned = [pltpu.roll(value, ny // 2, 1) for value in edge]
            folded = [jnp.where(lane <= ny // 2, top[part][0], turned[part]) for part in range(2)]
            folded[1] = jnp.where(lane % (ny // 2) == 0, edge[0], folded[1])
            for part in range(2):
                out_ref[0, part, base : base + GROUP] = folded[part]
                out_ref[1:8, part, base : base + GROUP] = top[part][1:]

            def tile(t, carry):
                start = pl.multiple_of(t * 8, 8)
                value = totals(start, base)
                for part in range(2):
                    out_ref[pl.ds(start, 8), part, base : base + GROUP] = value[part]
                return carry

            lax.fori_loop(1, half // 8, tile, 0)


def node_stage(c, plain, mask, ends, lines, nz):
    count, _, _, padded, ny = c.shape
    block = block_of(count)
    blocks = count // block
    half = nz // 2

    def early(phase, b):
        return jnp.where(phase == 0, b, blocks - 1)

    def late(phase, b):
        return jnp.where(phase == 0, blocks - 1, blocks - 1 - b)

    tables = [lines[0], lines[1], lines[4], lines[5], lines[6], *ends]
    return pl.pallas_call(
        functools.partial(node_kernel, half=half),
        grid=(2, blocks),
        in_specs=[
            pl.BlockSpec(memory_space=pltpu.SMEM),
            pl.BlockSpec((block, NODES, 2, padded, ny), lambda a, b: (early(a, b), 0, 0, 0, 0)),
            pl.BlockSpec((block, 2, padded, ny), lambda a, b: (late(a, b), 0, 0, 0)),
            *[full(t.shape) for t in tables],
        ],
        out_specs=pl.BlockSpec((half, 2, block, ny), lambda a, b: (0, 0, late(a, b), 0)),
        out_shape=jax.ShapeDtypeStruct((half, 2, count, ny), jnp.float32),
        scratch_shapes=[
            pltpu.VMEM((count, NODES, 2, padded, ny), jnp.float32),
            pltpu.VMEM((NODES, 2, padded, ny), jnp.float32),
        ],
        compiler_params=pltpu.CompilerParams(
            dimension_semantics=("arbitrary", "arbitrary"), vmem_limit_bytes=60 * 1024 * 1024
        ),
    )(mask, c, plain, *tables)


def couple_kernel(q_ref, th_ref, tl_ref, ih_ref, il_ref, grow_ref, close_ref, out_ref, work):
    steps, slabs, _, count, width = q_ref.shape
    nx = slabs * count
    joined = width % 128 == 0

    def side_by_side(table_high, table_low, values):
        if not joined:
            return [dot3_table_left(table_high, table_low, value) for value in values]
        wide = dot3_table_left(table_high, table_low, jnp.concatenate(values, axis=1))
        return [wide[:, i * width : (i + 1) * width] for i in range(len(values))]

    def ahead(s, carry):
        lines = [
            jnp.concatenate([q_ref[s, p, part] for p in range(slabs)], axis=0) for part in range(2)
        ]
        for part, waves in enumerate(side_by_side(th_ref[...], tl_ref[...], lines)):
            work[s, part, 0] = waves[:nx]
            work[s, part, 1] = waves[nx:]
        return carry

    unrolled(steps, ahead)

    def tile(t, carry):
        rows = pl.ds(t * 8, 8)
        for part in range(2):
            grow = (grow_ref[part, 0, rows], grow_ref[part, 1, rows])
            values = [(work[s, part, 0, rows], work[s, part, 1, rows]) for s in range(steps)]
            value = values[0]
            for s in range(1, steps):
                value = c_add(c_mul(grow, value), values[s])
            value = c_mul(value, (close_ref[part, 0, rows], close_ref[part, 1, rows]))
            for s in range(steps):
                work[s, part, 0, rows] = value[0]
                work[s, part, 1, rows] = value[1]
                if s + 1 < steps:
                    value = c_add(c_mul(grow, value), values[s])
        return carry

    lax.fori_loop(0, nx // 8, tile, 0)

    def back(i, carry):
        pair = [2 * i, 2 * i + 1]
        lines = [
            jnp.concatenate(
                [work[s, 0, 0] - work[s, 1, 1], work[s, 0, 1] + work[s, 1, 0]], axis=0
            )
            for s in pair
        ]
        for s, value in zip(pair, side_by_side(ih_ref[...], il_ref[...], lines)):
            for part in range(2):
                for p in range(slabs):
                    base = part * nx + p * count
                    out_ref[s, p, part] = value[base : base + count]
        return carry

    unrolled(steps // 2, back)


def couple_stage(q, velocity, first_mode, nz, ny):
    steps, slabs, _, count, width = q.shape
    nx = slabs * count
    forward, backward = x_tables(nx)
    values, vectors, _, weights = node_constants()
    mode = first_mode + jnp.arange(width, dtype=jnp.int32)
    row, lane = mode // ny, mode % ny
    edge = row == 0
    corner = edge & (lane % (ny // 2) == 0)
    wave_z = jnp.where(edge & (lane > ny // 2), nz // 2, row)
    wave_y = jnp.where(edge & (lane > ny // 2), lane - ny // 2, lane)
    wave_z = jnp.stack([wave_z, jnp.where(corner, nz // 2, wave_z)])[:, None, :]
    theta_z = wave_z.astype(jnp.float32) * (2.0 * math.pi / nz)
    theta_y = wave_y.astype(jnp.float32)[None, None, :] * (2.0 * math.pi / ny)
    theta_x = jnp.arange(nx, dtype=jnp.int32).astype(jnp.float32)[None, :, None] * (2.0 * math.pi / nx)
    real = diffusion_number * (
        (2.0 * jnp.cos(theta_x) - 2.0)
        + (2.0 * jnp.cos(theta_z) - 2.0)
        + (2.0 * jnp.cos(theta_y) - 2.0)
    )
    imag = -(
        velocity[0] * jnp.sin(theta_x)
        + velocity[1] * jnp.sin(theta_y)
        + velocity[2] * jnp.sin(theta_z)
    )
    grow = None
    for m in range(NODES):
        mu = complex(values[m])
        below = (1.0 - (mu.real * real - mu.imag * imag), -(mu.real * imag + mu.imag * real))
        above = complex(vectors[NODES - 1, m] * weights[m])
        added = c_div((above.real, above.imag), below)
        grow = added if grow is None else (grow[0] + added[0], grow[1] + added[1])
    whole = c_power(grow, steps)
    close = c_div(
        (circulant_alpha, 0.0), (1.0 - circulant_alpha * whole[0], -circulant_alpha * whole[1])
    )
    return pl.pallas_call(
        couple_kernel,
        out_shape=jax.ShapeDtypeStruct(q.shape, jnp.float32),
        scratch_shapes=[pltpu.VMEM((steps, 2, 2, nx, width), jnp.float32)],
        compiler_params=pltpu.CompilerParams(vmem_limit_bytes=24 * 1024 * 1024),
    )(
        q,
        *split_table(forward),
        *split_table(backward),
        jnp.stack(grow, axis=1),
        jnp.stack(close, axis=1),
    )


def edge_kernel(b_ref, ends_ref, low_ref, high_ref, beta_ref, wide_ref, out_ref):
    half, _, count, ny = b_ref.shape
    padded = wide_ref.shape[2]
    lane = lax.broadcasted_iota(jnp.int32, (GROUP, ny), 1)
    inside = lane % (ny // 2) != 0
    kept = jnp.where(inside, jnp.where(lane < ny // 2, 2.0, 0.0), 1.0)
    zero = jnp.zeros((GROUP, ny), jnp.float32)

    def unfold(g, carry):
        base = pl.multiple_of(g * GROUP, GROUP)
        planes = pl.ds(base, GROUP)
        top = [b_ref[0, part, planes] for part in range(2)]
        turned = [pltpu.roll(value, ny // 2, 1) for value in top]
        first = (top[0], jnp.where(inside, top[1], 0.0))
        edge = (jnp.where(inside, turned[0], top[1]), jnp.where(inside, turned[1], 0.0))
        for part in range(2):
            for start in range(0, half, 8):
                rows = [b_ref[start + r, part, planes] for r in range(8)]
                if start == 0:
                    rows[0] = first[part] * kept
                wide_ref[planes, part, start : start + 8] = jnp.swapaxes(jnp.stack(rows), 0, 1)
            rows = [edge[part] * kept] + [zero] * 7
            wide_ref[planes, part, half : half + 8] = jnp.swapaxes(jnp.stack(rows), 0, 1)
        return carry

    lax.fori_loop(0, count // GROUP, unfold, 0)

    def tile(t, carry):
        rows = pl.ds(pl.multiple_of(t * 8, 8), 8)
        for side, table in enumerate((low_ref, high_ref)):
            decay = [(table[m, 0, rows], table[m, 1, rows]) for m in range(NODES)]

            def group(g, values):
                for i in range(GROUP):
                    j = g * GROUP + i
                    j = j if side == 0 else count - 1 - j
                    plane = (wide_ref[j, 0, rows], wide_ref[j, 1, rows])
                    values = [c_add(c_mul(v, d), plane) for v, d in zip(values, decay)]
                return values

            values = lax.fori_loop(0, count // GROUP, group, [(zero, zero)] * NODES)
            for m in range(NODES):
                value = c_mul(values[m], (beta_ref[m, 0, rows], beta_ref[m, 1, rows]))
                for part in range(2):
                    out_ref[side, m, part, rows] = ends_ref[side, m, part, rows] + value[part]
        return carry

    lax.fori_loop(0, padded // 8, tile, 0)


def edge_stage(b, ends, lines):
    count = b.shape[2]
    padded, ny = lines[0].shape[2:]
    return pl.pallas_call(
        edge_kernel,
        out_shape=[
            jax.ShapeDtypeStruct((count, 2, padded, ny), jnp.float32),
            jax.ShapeDtypeStruct((2, NODES, 2, padded, ny), jnp.float32),
        ],
        compiler_params=pltpu.CompilerParams(vmem_limit_bytes=16 * 1024 * 1024),
    )(b, ends, lines[0], lines[1], lines[3])


def inverse_kernel(*refs):
    c_ref, b_ref, low_ref, high_ref, beta_ref, close_ref, decay_ref, around_ref = refs[:8]
    yh_ref, yl_ref, zh_ref, zl_ref = refs[8:12]
    ends_refs = refs[12:-3]
    out_ref, ahead, state = refs[-3:]
    phase = pl.program_id(0)
    step = pl.program_id(1)
    blocks = pl.num_programs(1)
    block, _, _, padded, ny = c_ref.shape
    nz = out_ref.shape[3]

    @pl.when((phase == 0) & (step == 0))
    def _():
        enter_low(state, ends_refs, decay_ref, around_ref)

    @pl.when((phase == 1) & (step == 0))
    def _():
        enter_back(state, ends_refs, decay_ref, around_ref, low_ref, close_ref)

    @pl.when(phase == 0)
    def _():
        def tile(t, carry):
            rows = pl.ds(pl.multiple_of(t * 8, 8), 8)
            nodes = range(NODES)
            low = [(low_ref[m, 0, rows], low_ref[m, 1, rows]) for m in nodes]
            beta = [(beta_ref[m, 0, rows], beta_ref[m, 1, rows]) for m in nodes]
            values = [(state[m, 0, rows], state[m, 1, rows]) for m in nodes]
            for j in range(block):
                plane = (b_ref[j, 0, rows], b_ref[j, 1, rows])
                for m in nodes:
                    source = (c_ref[j, m, 0, rows], c_ref[j, m, 1, rows])
                    source = c_add(c_mul(plane, beta[m]), source)
                    values[m] = c_add(c_mul(values[m], low[m]), source)
                    ahead[step * block + j, m, 0, rows] = values[m][0]
                    ahead[step * block + j, m, 1, rows] = values[m][1]
            for m in nodes:
                state[m, 0, rows] = values[m][0]
                state[m, 1, rows] = values[m][1]
            return carry

        lax.fori_loop(0, padded // 8, tile, 0)

    @pl.when(phase == 1)
    def _():
        first = (blocks - 1 - step) * block

        def tile(t, carry):
            rows = pl.ds(pl.multiple_of(t * 8, 8), 8)
            nodes = range(NODES)
            high = [(high_ref[m, 0, rows], high_ref[m, 1, rows]) for m in nodes]
            values = [(state[m, 0, rows], state[m, 1, rows]) for m in nodes]
            for j in reversed(range(block)):
                for m in nodes:
                    value = (ahead[first + j, m, 0, rows], ahead[first + j, m, 1, rows])
                    values[m] = c_add(c_mul(values[m], high[m]), value)
                    ahead[first + j, m, 0, rows] = values[m][0]
                    ahead[first + j, m, 1, rows] = values[m][1]
            for m in nodes:
                state[m, 0, rows] = values[m][0]
                state[m, 1, rows] = values[m][1]
            return carry

        lax.fori_loop(0, padded // 8, tile, 0)

        def pair(i, carry):
            rows = []
            for half in range(2):
                row = first + 2 * i + half
                for m in range(NODES):
                    rows.append(jnp.concatenate([ahead[row, m, 0], ahead[row, m, 1]], axis=1))
            lines = dot3_table_right(jnp.concatenate(rows, axis=0), yh_ref[...], yl_ref[...])
            columns = []
            for half in range(2):
                stacked = []
                for m in range(NODES):
                    base = (half * NODES + m) * padded
                    stacked.append(lines[base : base + padded, :ny])
                    stacked.append(lines[base : base + padded, ny:])
                columns.append(jnp.concatenate(stacked, axis=0))
            grid = dot3_table_left(zh_ref[...], zl_ref[...], jnp.concatenate(columns, axis=1))
            for half in range(2):
                for n in range(NODES):
                    out_ref[0, n, 2 * i + half] = grid[
                        n * nz : (n + 1) * nz, half * ny : (half + 1) * ny
                    ]
            return carry

        unrolled(block // 2, pair)


def inverse_stage(c, b, ends, lines, nz):
    count, _, _, padded, ny = c.shape
    block = block_of(count)
    blocks = count // block
    mixed, along_y = inverse_tables(nz, ny)
    tables = [lines[0], lines[1], *lines[3:], *split_table(along_y), *split_table(mixed), *ends]

    def early(phase, b):
        return jnp.where(phase == 0, b, blocks - 1)

    def late(phase, b):
        return jnp.where(phase == 0, blocks - 1, blocks - 1 - b)

    return pl.pallas_call(
        inverse_kernel,
        grid=(2, blocks),
        in_specs=[
            pl.BlockSpec((block, NODES, 2, padded, ny), lambda a, b: (early(a, b), 0, 0, 0, 0)),
            pl.BlockSpec((block, 2, padded, ny), lambda a, b: (early(a, b), 0, 0, 0)),
            *[full(t.shape) for t in tables],
        ],
        out_specs=pl.BlockSpec((1, NODES, block, nz, ny), lambda a, b: (0, 0, late(a, b), 0, 0)),
        out_shape=jax.ShapeDtypeStruct((1, NODES, count, nz, ny), jnp.float32),
        scratch_shapes=[
            pltpu.VMEM((count, NODES, 2, padded, ny), jnp.float32),
            pltpu.VMEM((NODES, 2, padded, ny), jnp.float32),
        ],
        compiler_params=pltpu.CompilerParams(
            dimension_semantics=("arbitrary", "arbitrary"), vmem_limit_bytes=32 * 1024 * 1024
        ),
    )(c, b, *tables)


def ring_ends(ends, slabs):
    result = [ends]
    for distance in range(slabs - 1, 0, -1):
        if 2 * distance == slabs:
            moved = lax.ppermute(ends, "space", [(i, (i + distance) % slabs) for i in range(slabs)])
        else:
            moved = jnp.stack(
                [
                    lax.ppermute(
                        ends[side], "space", [(i, (i + shift) % slabs) for i in range(slabs)]
                    )
                    for side, shift in enumerate((distance, -distance))
                ]
            )
        result.append(moved)
    return result


def to_modes(q, devices):
    half, _, count, ny = q.shape
    pieces = devices // half
    if pieces > 1:
        q = q.reshape(half, 2 * count, pieces, ny // pieces)
        q = jnp.transpose(q, (0, 2, 1, 3))
    return q.reshape(devices, 2 * count, ny // pieces)


def from_modes(b, half):
    devices, lines, width = b.shape
    pieces = devices // half
    if pieces > 1:
        b = jnp.transpose(b.reshape(half, pieces, lines, width), (0, 2, 1, 3))
    return b.reshape(half, 2, lines // 2, pieces * width)


def shards(iterate, right_side, diffusivity, velocity):
    steps, slabs = lax.axis_size("tm"), lax.axis_size("space")
    devices = steps * slabs
    _, _, count, nz, ny = iterate.shape
    up = [(i, (i + 1) % slabs) for i in range(slabs)]
    down = [(target, source) for source, target in up]
    last, first = iterate[0, :, count - 1], iterate[0, :, 0]
    if slabs == 2:
        halo = lax.ppermute(jnp.stack([last, first]), "space", up)
    else:
        halo = jnp.stack([lax.ppermute(last, "space", up), lax.ppermute(first, "space", down)])
    lines = line_tables(velocity, nz, ny, count, slabs)
    c, ends = forward_stage(iterate, right_side, diffusivity, halo, lines)
    every = ring_ends(ends, slabs)
    plain = plain_stage(iterate, ends)
    step = lax.axis_index("tm")
    mask = jnp.where(step == steps - 1, 1.0, 0.0).astype(jnp.float32)[None]
    q = node_stage(c, plain, mask, every, lines, nz)
    q = lax.all_to_all(to_modes(q, devices), ("tm", "space"), 0, 0, tiled=True)
    width = q.shape[2]
    first_mode = (step * slabs + lax.axis_index("space")) * width
    b = couple_stage(q.reshape(steps, slabs, 2, count, width), velocity, first_mode, nz, ny)
    b = lax.all_to_all(b.reshape(devices, 2 * count, width), ("tm", "space"), 0, 0, tiled=True)
    b, ends = edge_stage(from_modes(b, nz // 2), ends, lines)
    return inverse_stage(c, b, ring_ends(ends, slabs), lines, nz)


def solution(mesh):
    placed = (
        P("tm", None, "space", None, None),
        P("tm", None, "space", None, None),
        P("space", None, None),
        P(),
    )
    return jax.shard_map(
        shards,
        mesh=mesh,
        in_specs=placed,
        out_specs=P("tm", None, "space", None, None),
        check_vma=False,
    )
```
